128 devices in a mesh: tp: 16 (over z, y), dp: 8 (over x, core).
Axes of the slice: x: 4, y: 4, z: 4, core: 2. Of those that a mesh axis runs over, the one named last changes fastest.
Arguments:
- x: bfloat16 [8192, 4096], P(('dp', 'tp'))
- w_gate: bfloat16 [4096, 14336], P('dp', 'tp')
- w_up: bfloat16 [4096, 14336], P('dp', 'tp')
- w_down: bfloat16 [14336, 4096], P('tp', 'dp')
- dy: bfloat16 [8192, 4096], P(('dp', 'tp'))
Outputs:
- output 1: bfloat16 [8192, 4096], P(('dp', 'tp'))
- output 2: bfloat16 [8192, 4096], P(('dp', 'tp'))
- output 3: float32 [4096, 14336], P('dp', 'tp')
- output 4: float32 [4096, 14336], P('dp', 'tp')
- output 5: float32 [14336, 4096], P('tp', 'dp')
All inputs are finite; a program needn't handle non-finite values.
Results may differ from the reference program's by a relative error of at most 0.001.
Values are sent between devices in bfloat16 or wider.
A program may use at most 1 GiB of HBM per device.

```python
import jax
import jax.numpy as jnp
from jax import lax

ROWS = 8192
D = 4096
FF = 14336


def setup_inputs(seed: int = 0) -> dict:
    ks = jax.random.split(jax.random.key(seed), 5)
    x = jax.random.normal(ks[0], (ROWS, D), jnp.float32)
    w_gate = jax.random.normal(ks[1], (D, FF), jnp.float32) * (D ** -0.5)
    w_up = jax.random.normal(ks[2], (D, FF), jnp.float32) * (D ** -0.5)
    w_down = jax.random.normal(ks[3], (FF, D), jnp.float32) * (1.5 * FF ** -0.5)
    dy = jax.random.normal(ks[4], (ROWS, D), jnp.float32)
    return dict(x=x.astype(jnp.bfloat16), w_gate=w_gate.astype(jnp.bfloat16), w_up=w_up.astype(jnp.bfloat16), w_down=w_down.astype(jnp.bfloat16), dy=dy.astype(jnp.bfloat16))


def reference(x, w_gate, w_up, w_down, dy):
    nb = ROWS // 256
    xs = x.reshape(nb, ROWS // nb, D)
    dys = dy.reshape(nb, ROWS // nb, D)

    def body(carry, inp):
        gw, uw, dw = carry
        xb, dyb = inp
        a = jnp.dot(xb, w_gate, preferred_element_type=jnp.float32)
        b = jnp.dot(xb, w_up, preferred_element_type=jnp.float32)
        sig = jax.nn.sigmoid(a)
        sa = a * sig
        h = (sa * b).astype(jnp.bfloat16)
        y = (xb.astype(jnp.float32) + jnp.dot(h, w_down, preferred_element_type=jnp.float32)).astype(jnp.bfloat16)
        g = jnp.dot(dyb, w_down.T, preferred_element_type=jnp.float32)
        da = (g * b * sig * (1.0 + a * (1.0 - sig))).astype(jnp.bfloat16)
        db = (g * sa).astype(jnp.bfloat16)
        dx = (dyb.astype(jnp.float32) + jnp.dot(da, w_gate.T, preferred_element_type=jnp.float32) + jnp.dot(db, w_up.T, preferred_element_type=jnp.float32)).astype(jnp.bfloat16)
        gw = gw + jnp.dot(xb.T, da, preferred_element_type=jnp.float32)
        uw = uw + jnp.dot(xb.T, db, preferred_element_type=jnp.float32)
        dw = dw + jnp.dot(h.T, dyb, preferred_element_type=jnp.float32)
        return (gw, uw, dw), (y, dx)

    init = (jnp.zeros((D, FF), jnp.float32), jnp.zeros((D, FF), jnp.float32), jnp.zeros((FF, D), jnp.float32))
    (gw, uw, dw), (ys, dxs) = lax.scan(body, init, (xs, dys))
    return ys.reshape(ROWS, D), dxs.reshape(ROWS, D), gw, uw, dw
```

```python
import functools
import jax
import jax.numpy as jnp
from jax import lax
from jax.experimental import pallas as pl
from jax.experimental.pallas import tpu as pltpu
from jax.sharding import PartitionSpec as P

MESH = pl.DeviceIdType.MESH
HBM = pl.BlockSpec(memory_space=pltpu.HBM)


def place():
    i = lax.axis_index("dp")
    j = lax.axis_index("tp")
    return i // 2, i % 2, j // 4, j % 4


def gather_kernel(x_ref, dy_ref, wg_ref, wu_ref, wd_ref, xg, dyg, wgf, wuf, wdf,
                  xv, dyv, wgv, wuv, wdv, lsem, osem, ssem, rsem):
    x, c, z, y = place()
    xp = (x + 1) % 4
    xm = (x + 3) % 4
    dev = {
        "xp": {"dp": 2 * xp + c}, "xm": {"dp": 2 * xm + c}, "pc": {"dp": 2 * x + 1 - c},
        "yp": {"tp": 4 * z + (y + 1) % 4}, "ym": {"tp": 4 * z + (y + 3) % 4},
        "zp": {"tp": 4 * ((z + 1) % 4) + y}, "zm": {"tp": 4 * ((z + 3) % 4) + y},
    }
    loads = [pltpu.make_async_copy(s, d, lsem.at[k]) for k, (s, d) in enumerate(
        ((x_ref, xv), (wg_ref, wgv), (wu_ref, wuv), (wd_ref, wdv), (dy_ref, dyv)))]
    for l in loads:
        l.start()
    barrier = pltpu.get_barrier_semaphore()
    for d in dev.values():
        pl.semaphore_signal(barrier, inc=1, device_id=d, device_id_type=MESH)
    pl.semaphore_wait(barrier, len(dev))

    sends = []
    count = [0]

    def send(src, dst, to):
        k = count[0]
        count[0] += 1
        r = pltpu.make_async_remote_copy(src_ref=src, dst_ref=dst, send_sem=ssem.at[k], recv_sem=rsem.at[k],
                                         device_id=dev[to], device_id_type=MESH)
        r.start()
        sends.append(r)
        return r

    def wblk(k, xx, cc, half=None):
        i = 2 * xx + cc
        if k < 2:
            r = (wgf, wuf)[k]
            if half is None:
                return r.at[pl.ds(pl.multiple_of(i * 512, 512), 512), :]
            return r.at[pl.ds(pl.multiple_of(i * 512 + half * 256, 256), 256), :]
        if half is None:
            return wdf.at[i]
        return wdf.at[i, pl.ds(half * 448, 448), :]

    gath = (xg, dyg)

    def rows(a, color, p, s, lo=0, n=32):
        zz, yy = (s, p) if color == 0 else (p, s)
        return gath[a].at[pl.ds(pl.multiple_of((zz * 4 + yy) * 64 + color * 32 + lo, 16), n), :]

    prim = ((y, z), (z, y))
    links = (("yp", "ym", "zp", "zm"), ("zp", "zm", "yp", "ym"))
    own = (xv, dyv)
    A = {}
    B = {}

    def start_own(a):
        for col in range(2):
            p, s = prim[col]
            pp, pm, sp, sm = links[col]
            src = own[a].at[pl.ds(col * 32, 32), :]
            dst = rows(a, col, p, s)
            A[a, col] = (send(src, dst, pp), send(src, dst, pm))
            B[a, col, 0] = (send(src, dst, sp), send(src, dst, sm))

    A2 = {}

    def step_a(a):
        for col in range(2):
            p, s = prim[col]
            pp, pm, sp, sm = links[col]
            fromm, fromp = A[a, col]
            fromm.wait_recv()
            q = (p + 3) % 4
            f1 = send(rows(a, col, q, s, 0, 16), rows(a, col, q, s, 0, 16), pp)
            B[a, col, -1] = (send(rows(a, col, q, s), rows(a, col, q, s), sp), send(rows(a, col, q, s), rows(a, col, q, s), sm))
            fromp.wait_recv()
            q = (p + 1) % 4
            f2 = send(rows(a, col, q, s, 16, 16), rows(a, col, q, s, 16, 16), pm)
            B[a, col, 1] = (send(rows(a, col, q, s), rows(a, col, q, s), sp), send(rows(a, col, q, s), rows(a, col, q, s), sm))
            A2[a, col] = (f1, f2)

    def step_a2(a):
        for col in range(2):
            p, s = prim[col]
            pp, pm, sp, sm = links[col]
            f1, f2 = A2[a, col]
            f1.wait_recv()
            f2.wait_recv()
            q = (p + 2) % 4
            B[a, col, 2] = (send(rows(a, col, q, s), rows(a, col, q, s), sp), send(rows(a, col, q, s), rows(a, col, q, s), sm))

    last = []

    def step_b(a, q):
        for col in range(2):
            p, s = prim[col]
            pp, pm, sp, sm = links[col]
            fromm, fromp = B[a, col, q]
            qq = (p + q + 4) % 4
            fromm.wait_recv()
            r = rows(a, col, qq, (s + 3) % 4, 0, 16)
            last.append(send(r, r, sp))
            fromp.wait_recv()
            r = rows(a, col, qq, (s + 1) % 4, 16, 16)
            last.append(send(r, r, sm))

    W = {}

    def start_w(k):
        src = (wgv, wuv, wdv)[k]
        dst = wblk(k, x, c)
        W[k] = (send(src, dst, "xp"), send(src, dst, "xm"))
        last.append(send(src, dst, "pc"))

    W2 = {}

    def step_w(k):
        fromm, fromp = W[k]
        fromm.wait_recv()
        r = wblk(k, xm, c, 0)
        f1 = send(r, r, "xp")
        r = wblk(k, xm, c)
        last.append(send(r, r, "pc"))
        fromp.wait_recv()
        r = wblk(k, xp, c, 1)
        f2 = send(r, r, "xm")
        r = wblk(k, xp, c)
        last.append(send(r, r, "pc"))
        W2[k] = (f1, f2)

    def step_w2(k):
        f1, f2 = W2[k]
        xo = (x + 2) % 4
        f1.wait_recv()
        r = wblk(k, xo, c, 0)
        last.append(send(r, r, "pc"))
        f2.wait_recv()
        r = wblk(k, xo, c, 1)
        last.append(send(r, r, "pc"))

    outs = []

    def put(src, dst):
        r = pltpu.make_async_copy(src, dst, osem.at[len(outs)])
        r.start()
        outs.append(r)

    loads[0].wait()
    start_own(0)
    for k in range(3):
        loads[1 + k].wait()
        start_w(k)
    loads[4].wait()
    j64 = pl.multiple_of((z * 4 + y) * 64, 64)
    put(xv, xg.at[pl.ds(j64, 64), :])
    put(dyv, dyg.at[pl.ds(j64, 64), :])
    for k in range(3):
        put((wgv, wuv, wdv)[k], wblk(k, x, c))

    step_a(0)
    start_own(1)
    step_a2(0)
    step_b(0, 0)
    step_a(1)
    step_w(0)
    step_b(0, -1)
    step_b(0, 1)
    step_a2(1)
    step_b(0, 2)
    step_w(1)
    step_b(1, 0)
    step_b(1, -1)
    step_w(2)
    step_w2(0)
    step_b(1, 1)
    step_w2(1)
    step_b(1, 2)
    step_w2(2)
    for r in last:
        r.wait_recv()
    for r in sends:
        r.wait_send()
    for r in outs:
        r.wait()


NSEND = 80 + 6 + 6 + 15


def gather(x, dy, wg, wu, wd):
    bf = jnp.bfloat16
    sd = jax.ShapeDtypeStruct
    return pl.pallas_call(
        gather_kernel,
        out_shape=(sd((1024, 4096), bf), sd((1024, 4096), bf), sd((4096, 896), bf), sd((4096, 896), bf), sd((8, 896, 512), bf)),
        in_specs=[HBM] * 5,
        out_specs=(HBM,) * 5,
        scratch_shapes=[
            pltpu.VMEM((64, 4096), bf), pltpu.VMEM((64, 4096), bf), pltpu.VMEM((512, 896), bf), pltpu.VMEM((512, 896), bf),
            pltpu.VMEM((896, 512), bf),
            pltpu.SemaphoreType.DMA((5,)), pltpu.SemaphoreType.DMA((5,)),
            pltpu.SemaphoreType.DMA((NSEND,)), pltpu.SemaphoreType.DMA((NSEND,)),
        ],
        compiler_params=pltpu.CompilerParams(collective_id=1, has_side_effects=True, vmem_limit_bytes=16 * 2**20),
        name="gather",
    )(x, dy, wg, wu, wd)


def solution(mesh):
    rows = P(("dp", "tp"), None)
    wsp = P("dp", "tp")
    dsp = P("tp", "dp")
    f32 = jnp.float32
    bf = jnp.bfloat16

    def local(x, w_gate, w_up, w_down, dy):
        xg, dyg, wg, wu, wd = gather(x, dy, w_gate, w_up, w_down)
        a = jnp.dot(xg, wg, preferred_element_type=f32)
        b = jnp.dot(xg, wu, preferred_element_type=f32)
        sig = jax.nn.sigmoid(a)
        sa = a * sig
        h = (sa * b).astype(bf)
        dyb = dyg.reshape(1024, 8, 512)
        g = lax.dot_general(dyb, wd, (((1, 2), (0, 2)), ((), ())), preferred_element_type=f32)
        da = (g * b * sig * (1.0 + a * (1.0 - sig))).astype(bf)
        db = (g * sa).astype(bf)
        yp = lax.dot_general(h, wd, (((1,), (1,)), ((), ())), preferred_element_type=f32).reshape(1024, 4096)
        yq = lax.psum_scatter(yp, "tp", scatter_dimension=0, tiled=True)
        dwd = lax.psum_scatter(lax.dot_general(h, dyg, (((0,), (0,)), ((), ())), preferred_element_type=f32), "dp", scatter_dimension=1, tiled=True)
        dxp = jnp.dot(da, wg.T, preferred_element_type=f32) + jnp.dot(db, wu.T, preferred_element_type=f32)
        dxq = lax.psum_scatter(dxp, "tp", scatter_dimension=0, tiled=True)
        dwg = lax.psum_scatter(lax.dot_general(xg, da, (((0,), (0,)), ((), ())), preferred_element_type=f32), "dp", scatter_dimension=0, tiled=True)
        dwu = lax.psum_scatter(lax.dot_general(xg, db, (((0,), (0,)), ((), ())), preferred_element_type=f32), "dp", scatter_dimension=0, tiled=True)
        y = (x.astype(f32) + yq).astype(bf)
        dx = (dy.astype(f32) + dxq).astype(bf)
        return y, dx, dwg, dwu, dwd

    return jax.shard_map(local, mesh=mesh, in_specs=(rows, wsp, wsp, dsp, rows), out_specs=(rows, rows, wsp, wsp, dsp), check_vma=False)
```

```python
import jax
import jax.numpy as jnp
from jax import lax
from jax.experimental import pallas as pl
from jax.experimental.pallas import tpu as pltpu
from jax.sharding import PartitionSpec as P

MESH = pl.DeviceIdType.MESH
HBM = pl.BlockSpec(memory_space=pltpu.HBM)


def place():
    i = lax.axis_index("dp")
    j = lax.axis_index("tp")
    return i // 2, i % 2, j // 4, j % 4


def gather_kernel(x_ref, dy_ref, wg_ref, wu_ref, wd_ref, xd, wgf, wuf, wdf,
                  xv, dyv, wgv, wuv, wdv, lsem, osem, ssem, rsem):
    x, c, z, y = place()
    xp = (x + 1) % 4
    xm = (x + 3) % 4
    dev = {
        "xp": {"dp": 2 * xp + c}, "xm": {"dp": 2 * xm + c}, "pc": {"dp": 2 * x + 1 - c},
        "yp": {"tp": 4 * z + (y + 1) % 4}, "ym": {"tp": 4 * z + (y + 3) % 4},
        "zp": {"tp": 4 * ((z + 1) % 4) + y}, "zm": {"tp": 4 * ((z + 3) % 4) + y},
    }
    loads = [pltpu.make_async_copy(s, d, lsem.at[k]) for k, (s, d) in enumerate(
        ((x_ref, xv), (wg_ref, wgv), (wu_ref, wuv), (wd_ref, wdv), (dy_ref, dyv)))]
    for l in loads:
        l.start()
    barrier = pltpu.get_barrier_semaphore()
    for d in dev.values():
        pl.semaphore_signal(barrier, inc=1, device_id=d, device_id_type=MESH)
    pl.semaphore_wait(barrier, len(dev))

    sends = []
    count = [0]

    def send(src, dst, to):
        k = count[0]
        count[0] += 1
        r = pltpu.make_async_remote_copy(src_ref=src, dst_ref=dst, send_sem=ssem.at[k], recv_sem=rsem.at[k],
                                         device_id=dev[to], device_id_type=MESH)
        r.start()
        sends.append(r)
        return r

    def wblk(k, xx, cc, half=None):
        i = 2 * xx + cc
        if k < 2:
            r = (wgf, wuf)[k]
            if half is None:
                return r.at[pl.ds(pl.multiple_of(i * 512, 512), 512), :]
            return r.at[pl.ds(pl.multiple_of(i * 512 + half * 256, 256), 256), :]
        if half is None:
            return wdf.at[i]
        return wdf.at[i, pl.ds(half * 448, 448), :]

    def rows(a, color, p, s, lo=0, n=32):
        zz, yy = (s, p) if color == 0 else (p, s)
        return xd.at[a, pl.ds(pl.multiple_of((zz * 4 + yy) * 64 + color * 32 + lo, 16), n), :]

    prim = ((y, z), (z, y))
    links = (("yp", "ym", "zp", "zm"), ("zp", "zm", "yp", "ym"))
    own = (xv, dyv)
    A = {}
    B = {}

    def start_own(a):
        for col in range(2):
            p, s = prim[col]
            pp, pm, sp, sm = links[col]
            src = own[a].at[pl.ds(col * 32, 32), :]
            dst = rows(a, col, p, s)
            A[a, col] = (send(src, dst, pp), send(src, dst, pm))
            B[a, col, 0] = (send(src, dst, sp), send(src, dst, sm))

    A2 = {}

    def step_a(a):
        for col in range(2):
            p, s = prim[col]
            pp, pm, sp, sm = links[col]
            fromm, fromp = A[a, col]
            fromm.wait_recv()
            q = (p + 3) % 4
            f1 = send(rows(a, col, q, s, 0, 16), rows(a, col, q, s, 0, 16), pp)
            B[a, col, -1] = (send(rows(a, col, q, s), rows(a, col, q, s), sp), send(rows(a, col, q, s), rows(a, col, q, s), sm))
            fromp.wait_recv()
            q = (p + 1) % 4
            f2 = send(rows(a, col, q, s, 16, 16), rows(a, col, q, s, 16, 16), pm)
            B[a, col, 1] = (send(rows(a, col, q, s), rows(a, col, q, s), sp), send(rows(a, col, q, s), rows(a, col, q, s), sm))
            A2[a, col] = (f1, f2)

    def step_a2(a):
        for col in range(2):
            p, s = prim[col]
            pp, pm, sp, sm = links[col]
            f1, f2 = A2[a, col]
            f1.wait_recv()
            f2.wait_recv()
            q = (p + 2) % 4
            B[a, col, 2] = (send(rows(a, col, q, s), rows(a, col, q, s), sp), send(rows(a, col, q, s), rows(a, col, q, s), sm))

    last = []

    def step_b(a, q):
        for col in range(2):
            p, s = prim[col]
            pp, pm, sp, sm = links[col]
            fromm, fromp = B[a, col, q]
            qq = (p + q + 4) % 4
            fromm.wait_recv()
            r = rows(a, col, qq, (s + 3) % 4, 0, 16)
            last.append(send(r, r, sp))
            fromp.wait_recv()
            r = rows(a, col, qq, (s + 1) % 4, 16, 16)
            last.append(send(r, r, sm))

    W = {}

    def start_w(k):
        src = (wgv, wuv, wdv)[k]
        dst = wblk(k, x, c)
        W[k] = (send(src, dst, "xp"), send(src, dst, "xm"))
        last.append(send(src, dst, "pc"))

    W2 = {}

    def step_w(k):
        fromm, fromp = W[k]
        fromm.wait_recv()
        r = wblk(k, xm, c, 0)
        f1 = send(r, r, "xp")
        r = wblk(k, xm, c)
        last.append(send(r, r, "pc"))
        fromp.wait_recv()
        r = wblk(k, xp, c, 1)
        f2 = send(r, r, "xm")
        r = wblk(k, xp, c)
        last.append(send(r, r, "pc"))
        W2[k] = (f1, f2)

    def step_w2(k):
        f1, f2 = W2[k]
        xo = (x + 2) % 4
        f1.wait_recv()
        r = wblk(k, xo, c, 0)
        last.append(send(r, r, "pc"))
        f2.wait_recv()
        r = wblk(k, xo, c, 1)
        last.append(send(r, r, "pc"))

    outs = []

    def put(src, dst):
        r = pltpu.make_async_copy(src, dst, osem.at[len(outs)])
        r.start()
        outs.append(r)

    loads[0].wait()
    start_own(0)
    for k in range(3):
        loads[1 + k].wait()
        start_w(k)
    loads[4].wait()
    j64 = pl.multiple_of((z * 4 + y) * 64, 64)
    put(xv, xd.at[0, pl.ds(j64, 64), :])
    put(dyv, xd.at[1, pl.ds(j64, 64), :])
    for k in range(3):
        put((wgv, wuv, wdv)[k], wblk(k, x, c))

    step_a(0)
    start_own(1)
    step_a2(0)
    step_b(0, 0)
    step_a(1)
    step_w(0)
    step_b(0, -1)
    step_b(0, 1)
    step_a2(1)
    step_b(0, 2)
    step_w(1)
    step_b(1, 0)
    step_b(1, -1)
    step_w(2)
    step_w2(0)
    step_b(1, 1)
    step_w2(1)
    step_b(1, 2)
    step_w2(2)
    for r in last:
        r.wait_recv()
    for r in sends:
        r.wait_send()
    for r in outs:
        r.wait()


NSEND = 80 + 6 + 6 + 15


def gather(x, dy, wg, wu, wd):
    bf = jnp.bfloat16
    sd = jax.ShapeDtypeStruct
    return pl.pallas_call(
        gather_kernel,
        out_shape=(sd((2, 1024, 4096), bf), sd((4096, 896), bf), sd((4096, 896), bf), sd((8, 896, 512), bf)),
        in_specs=[HBM] * 5,
        out_specs=(HBM,) * 4,
        scratch_shapes=[
            pltpu.VMEM((64, 4096), bf), pltpu.VMEM((64, 4096), bf), pltpu.VMEM((512, 896), bf), pltpu.VMEM((512, 896), bf),
            pltpu.VMEM((896, 512), bf),
            pltpu.SemaphoreType.DMA((5,)), pltpu.SemaphoreType.DMA((5,)),
            pltpu.SemaphoreType.DMA((NSEND,)), pltpu.SemaphoreType.DMA((NSEND,)),
        ],
        compiler_params=pltpu.CompilerParams(collective_id=1, has_side_effects=True, vmem_limit_bytes=60 * 2**20),
        name="gather",
    )(x, dy, wg, wu, wd)


NT = (((1,), (1,)), ((), ()))
TN = (((0,), (0,)), ((), ()))
F32 = jnp.float32
BF = jnp.bfloat16


def reduce_kernel(hh, da, db, xd, wg, wu, wd, xo, dyo, dw, yo,
                  XR, ZR, AP, B, A, XB, XS, WD, WX, ZB, ZS, Z2, res, ov,
                  s_ld, s_a, s_ap, r_ap, s_b, r_b, s_xs, r_xs, s_zs, r_zs, s_2, r_2, s_w, s_xst, s_zst, s_xo, s_yo):
    x, c, z, y = place()
    dev = {
        "xp": {"dp": 2 * ((x + 1) % 4) + c}, "xm": {"dp": 2 * ((x + 3) % 4) + c}, "pc": {"dp": 2 * x + 1 - c},
        "yp": {"tp": 4 * z + (y + 1) % 4}, "ym": {"tp": 4 * z + (y + 3) % 4},
        "zp": {"tp": 4 * ((z + 1) % 4) + y}, "zm": {"tp": 4 * ((z + 3) % 4) + y},
    }
    hbm_b = (hh, da, db)

    def remote(src, dst, ss, rs, to):
        return pltpu.make_async_remote_copy(src_ref=src, dst_ref=dst, send_sem=ss, recv_sem=rs, device_id=dev[to], device_id_type=MESH)

    def add(dst, src, n):
        def body(r, _):
            s = pl.ds(pl.multiple_of(r * 32, 32), 32)
            dst[s, :] = dst[s, :] + src[s, :]
            return 0
        lax.fori_loop(0, n // 32, body, 0)

    ld_b = [pltpu.make_async_copy(hbm_b[k], B.at[k, 0], s_ld.at[k]) for k in range(3)]
    ld_r = [pltpu.make_async_copy(xo, res.at[0], s_ld.at[3]), pltpu.make_async_copy(dyo, res.at[1], s_ld.at[4])]

    def load_w(n):
        out = []
        for col in range(2):
            q = 2 * col + n % 2
            if n < 2:
                out.append(pltpu.make_async_copy(wd.at[pl.ds(2 * q, 2)], WD.at[col], s_w.at[col, 0]))
            else:
                out.append(pltpu.make_async_copy(wg.at[pl.ds(1024 * q, 1024), :], WX.at[col, 0], s_w.at[col, 1]))
                out.append(pltpu.make_async_copy(wu.at[pl.ds(1024 * q, 1024), :], WX.at[col, 1], s_w.at[col, 2]))
        for o in out:
            o.start()
        return out

    ld_b[0].start()
    wl = {0: load_w(0)}
    for l in ld_b[1:] + ld_r:
        l.start()
    wl[2] = load_w(2)

    barrier = pltpu.get_barrier_semaphore()
    for d in dev.values():
        pl.semaphore_signal(barrier, inc=1, device_id=d, device_id_type=MESH)
    pl.semaphore_wait(barrier, len(dev))

    def chunk(idx):
        return (x + 6 - idx) % 4

    bp = [remote(hbm_b[k], B.at[k, 1], s_b.at[k], r_b.at[k], "pc") for k in range(3)]

    def ap(arr, idx):
        ch = chunk(idx)
        return remote(xd.at[arr, :, pl.ds(pl.multiple_of(1024 * ch + 512 * (1 - c), 512), 512)], AP.at[arr, idx], s_ap.at[arr, idx], r_ap.at[arr, idx], "pc")

    bp[0].start()
    for idx in range(4):
        ap(1, idx).start()
    bp[1].start()
    for idx in range(4):
        ap(0, idx).start()
    bp[2].start()

    def load_a(arr, idx):
        slot = idx % 2
        ch = chunk(idx)
        return (pltpu.make_async_copy(xd.at[arr, :, pl.ds(pl.multiple_of(1024 * ch + 512 * c, 512), 512)], A.at[slot, 0], s_a.at[slot, 0]),
                pltpu.make_async_copy(AP.at[arr, idx], A.at[slot, 1], s_a.at[slot, 1]))

    def start_a(arr, idx):
        for l in load_a(arr, idx):
            l.start()

    def wait_ap(arr, idx):
        ap(arr, idx).wait_recv()

    def dot_x(k, idx):
        slot = idx % 2
        for l in load_a(0, idx):
            l.wait()

        def body(m, _):
            cols = pl.ds(pl.multiple_of(m * 256, 256), 256)
            XB[idx, m] = (lax.dot_general(A[slot, 0, :, cols], B[k, 0], TN, preferred_element_type=F32)
                          + lax.dot_general(A[slot, 1, :, cols], B[k, 1], TN, preferred_element_type=F32))
            return 0
        lax.fori_loop(0, 2, body, 0)

    def xmsg(k, t):
        src = (XB.at[0, 0], XB.at[0, 1], XB.at[1, 1], XB.at[3, 0], XB.at[1, 0], XB.at[3, 1])[t]
        return remote(src, XR.at[k, t], s_xs.at[t], r_xs.at[k, t], ("xp", "xm")[t % 2])

    def x1(k):
        if k == 0:
            bp[0].wait_recv()
            for idx in range(2):
                wait_ap(1, idx)
                start_a(1, idx)
        else:
            bp[k].wait_recv()
            xmsg(k - 1, 0).wait_send()
            xmsg(k - 1, 1).wait_send()
        dot_x(k, 0)
        xmsg(k, 0).start()
        xmsg(k, 1).start()
        if k < 2:
            wait_ap(1 - min(k, 1), 2)
        start_a(1 - min(k, 1), 2)

    def x2(k):
        if k > 0:
            for t in range(2, 6):
                xmsg(k - 1, t).wait_send()
            xout(k - 1).wait()

        def body(idx, _):
            dot_x(k, idx)
            nxt = (idx + 2) % 4
            carry = (idx + 2) // 4
            if k == 0:
                wait_ap(1 - carry, nxt)
                start_a(1 - carry, nxt)
            elif k == 1:
                @pl.when(idx == 1)
                def _():
                    wait_ap(0, nxt)
                start_a(0, nxt)
            else:
                @pl.when(idx == 1)
                def _():
                    start_a(0, nxt)
            return 0
        lax.fori_loop(1, 4, body, 0)
        xmsg(k, 2).start()
        xmsg(k, 3).start()

    def xstage(k, t, slot):
        return pltpu.make_async_copy(XR.at[k, t], XS.at[slot], s_xst.at[slot])

    def x3(k):
        for t in range(2):
            xmsg(k, t).wait_recv()
            xstage(k, t, t).start()
        for t in range(2):
            xstage(k, t, t).wait()
            add(XB.at[(1, 3)[t], t], XS.at[t], 256)
            xmsg(k, 4 + t).start()

    def xout(k):
        return pltpu.make_async_copy(XB.at[2], dw.at[k], s_xo)

    def xf(k):
        for pair in ((3, 2), (4, 5)):
            for h, t in enumerate(pair):
                xmsg(k, t).wait_recv()
                xstage(k, t, h).start()
            for h, t in enumerate(pair):
                xstage(k, t, h).wait()
                add(XB.at[2, h], XS.at[h], 256)
        xout(k).start()

    pos = ((z, y), (y, z))
    link = (("zp", "zm", "yp", "ym"), ("yp", "ym", "zp", "zm"))

    def dots_z(n, lo, hi):
        m = hi - lo

        def body(i, _):
            col = i // m
            idx = lo + i % m
            p = z + col * (y - z)
            ch = (p + 6 - idx) % 4
            s1 = 256 - 192 * col
            s2 = 64 + 192 * col
            own = (idx // 2) * (1 - idx // 3)
            slot = idx + own * 2 * (n % 2)

            def lhs(k):
                return jnp.concatenate([B[k, 0, pl.ds(pl.multiple_of(ch * s1 + g * s2, 64), 64), :] for g in range(4)], axis=0)

            if n < 2:
                l = lhs(0)
                for h in range(2):
                    ZB[col, slot, h] = jnp.dot(l, WD[col, h], preferred_element_type=F32)
            else:
                l = lhs(1)
                u = lhs(2)
                for h in range(2):
                    r = pl.ds(512 * h, 512)
                    ZB[col, slot, h] = (lax.dot_general(l, WX[col, 0, r, :], NT, preferred_element_type=F32)
                                        + lax.dot_general(u, WX[col, 1, r, :], NT, preferred_element_type=F32))
            return 0
        lax.fori_loop(0, 2 * m, body, 0)

    def zmsg(n, col, t):
        src = ((0, 0), (0, 1), (1, 1), (3, 0), (1, 0), (3, 1))[t]
        return remote(ZB.at[col, src[0], src[1]], ZR.at[col, n, t], s_zs.at[col, t], r_zs.at[col, n, t], link[col][t % 2])

    def own(n, col, h):
        return ZB.at[col, 2 + 2 * (n % 2), h]

    def sub(n, col, h, d):
        s = (pos[col][1] + d) % 4
        return ZB.at[col, 2 + 2 * (n % 2), h, pl.ds(pl.multiple_of(s * 64, 64), 64), :]

    def msg2(n, col, t):
        h, d = ((0, 2), (1, 2), (1, 1), (0, 3), (0, 1), (1, 3))[t]
        return remote(sub(n, col, h, d), Z2.at[col, n, t], s_2.at[col, n % 2, t], r_2.at[col, n, t], link[col][2 + t % 2])

    def p1(n):
        if n == 0:
            ld_b[0].wait()
        for l in wl[n]:
            l.wait()
        if n > 0:
            for col in range(2):
                for t in range(2):
                    zmsg(n - 1, col, t).wait_send()
        dots_z(n, 0, 1)
        for t in range(2):
            for col in range(2):
                zmsg(n, col, t).start()

    def p2(n):
        if n > 0:
            for col in range(2):
                for t in range(2, 6):
                    zmsg(n - 1, col, t).wait_send()
        if n > 1:
            for col in range(2):
                for t in range(6):
                    msg2(n - 2, col, t).wait_send()
        dots_z(n, 1, 4)
        for t in range(2, 4):
            for col in range(2):
                zmsg(n, col, t).start()
        if n % 2 == 0:
            wl[n + 1] = load_w(n + 1)

    def zstage(n, col, t, slot):
        return pltpu.make_async_copy(ZR.at[col, n, t], ZS.at[col, slot], s_zst.at[col, slot])

    def p4(n):
        for t in range(2):
            for col in range(2):
                zmsg(n, col, t).wait_recv()
                zstage(n, col, t, t).start()
        for t in range(2):
            for col in range(2):
                zstage(n, col, t, t).wait()
                add(ZB.at[col, (1, 3)[t], t], ZS.at[col, t], 256)
                zmsg(n, col, 4 + t).start()

    def f(n):
        order = ((3, 0), (2, 1), (4, 0), (5, 1))
        for i, (t, h) in enumerate(order):
            for col in range(2):
                zmsg(n, col, t).wait_recv()
                zstage(n, col, t, i).start()
        for i, (t, h) in enumerate(order):
            for col in range(2):
                zstage(n, col, t, i).wait()
                add(own(n, col, h), ZS.at[col, i], 256)
        for t in range(4):
            for col in range(2):
                msg2(n, col, t).start()

    def hh2(n):
        for t in range(2):
            for col in range(2):
                msg2(n, col, t).wait_recv()
                add(sub(n, col, t, (1, 3)[t]), Z2.at[col, n, t], 64)
                msg2(n, col, 4 + t).start()

    def zf(n):
        a = n // 2
        for col in range(2):
            for h, ts in ((0, (3, 4)), (1, (2, 5))):
                for t in ts:
                    msg2(n, col, t).wait_recv()
                cs = pl.ds(2048 * col + 1024 * (n % 2) + 512 * h, 512)
                v = sub(n, col, h, 0)[...] + Z2[col, n, ts[0]] + Z2[col, n, ts[1]]
                ov[a, :, cs] = (res[a, :, cs].astype(F32) + v).astype(BF)

    p1(0)
    x1(0)
    p2(0)
    x2(0)
    p4(0)
    x3(0)
    for l in ld_b[1:] + ld_r:
        l.wait()
    p1(1)
    x1(1)
    f(0)
    p2(1)
    hh2(0)
    zf(0)
    p4(1)
    xf(0)
    x2(1)
    p1(2)
    f(1)
    p2(2)
    x3(1)
    hh2(1)
    zf(1)
    p4(2)
    x1(2)
    p1(3)
    f(2)
    xf(1)
    x2(2)
    p2(3)
    hh2(2)
    zf(2)
    p4(3)
    x3(2)
    f(3)
    hh2(3)
    zf(3)
    xf(2)
    out = [pltpu.make_async_copy(ov, yo, s_yo)]
    out[0].start()
    for t in range(6):
        xmsg(2, t).wait_send()
        for col in range(2):
            zmsg(3, col, t).wait_send()
            msg2(2, col, t).wait_send()
            msg2(3, col, t).wait_send()
    for k in range(3):
        bp[k].wait_send()
    for arr in range(2):
        for idx in range(4):
            ap(arr, idx).wait_send()
    xout(2).wait()
    out[0].wait()


def reduce(h, da, db, xd, wg, wu, wd, xo, dyo):
    sd = jax.ShapeDtypeStruct
    dma = pltpu.SemaphoreType.DMA
    V = pltpu.VMEM
    return pl.pallas_call(
        reduce_kernel,
        out_shape=(sd((3, 2, 256, 896), F32), sd((2, 64, 4096), BF),
                   sd((3, 6, 256, 896), F32), sd((2, 4, 6, 256, 512), F32), sd((2, 4, 1024, 512), BF)),
        in_specs=[HBM] * 9,
        out_specs=(HBM,) * 5,
        scratch_shapes=[
            V((3, 2, 1024, 896), BF), V((2, 2, 1024, 512), BF), V((4, 2, 256, 896), F32), V((2, 256, 896), F32),
            V((2, 2, 896, 512), BF), V((2, 2, 1024, 896), BF), V((2, 5, 2, 256, 512), F32), V((2, 4, 256, 512), F32),
            V((2, 4, 6, 64, 512), F32), V((2, 64, 4096), BF), V((2, 64, 4096), BF),
            dma((5,)), dma((2, 2)), dma((2, 4)), dma((2, 4)), dma((3,)), dma((3,)), dma((6,)), dma((3, 6)),
            dma((2, 6)), dma((2, 4, 6)), dma((2, 2, 6)), dma((2, 4, 6)), dma((2, 3)), dma((2,)), dma((2, 4)), dma, dma,
        ],
        compiler_params=pltpu.CompilerParams(collective_id=2, has_side_effects=True, vmem_limit_bytes=67043328),
        name="reduce",
    )(h, da, db, xd, wg, wu, wd, xo, dyo)[:2]


def solution(mesh):
    rows = P(("dp", "tp"), None)
    wsp = P("dp", "tp")
    dsp = P("tp", "dp")

    def local(x, w_gate, w_up, w_down, dy):
        xd, wg, wu, wd = gather(x, dy, w_gate, w_up, w_down)
        a = jnp.dot(xd[0], wg, preferred_element_type=F32)
        b = jnp.dot(xd[0], wu, preferred_element_type=F32)
        sig = jax.nn.sigmoid(a)
        sa = a * sig
        h = (sa * b).astype(BF)
        g = lax.dot_general(xd[1].reshape(1024, 8, 512), wd, (((1, 2), (0, 2)), ((), ())), preferred_element_type=F32)
        da = (g * b * sig * (1.0 + a * (1.0 - sig))).astype(BF)
        db = (g * sa).astype(BF)
        dw, yo = reduce(h, da, db, xd, wg, wu, wd, x, dy)
        dw = dw.reshape(3, 512, 896)
        return yo[0], yo[1], dw[1], dw[2], dw[0].T

    return jax.shard_map(local, mesh=mesh, in_specs=(rows, wsp, wsp, dsp, rows), out_specs=(rows, rows, wsp, wsp, dsp), check_vma=False)
```

```python
import jax
import jax.numpy as jnp
from jax import lax
from jax.experimental import pallas as pl
from jax.experimental.pallas import tpu as pltpu
from jax.sharding import PartitionSpec as P

MESH = pl.DeviceIdType.MESH
HBM = pl.BlockSpec(memory_space=pltpu.HBM)
NT = (((1,), (1,)), ((), ()))
TN = (((0,), (0,)), ((), ()))
F32 = jnp.float32
BF = jnp.bfloat16
NSEND = 107


def mlp_kernel(x_ref, dy_ref, wg_ref, wu_ref, wd_ref, dw, yo, xd, wgf, wuf, wdf, UV, XR, ZR, AP,
               B, A, XB, XS, WD, WX, ZB, ZS, Z2, US, res, ov,
               ssem, rsem, s_ld, s_put, s_c, s_a, s_ap, r_ap, s_b, r_b, s_xs, r_xs, s_zs, r_zs, s_2, r_2, s_w, s_xst, s_zst, s_xo, s_yo, s_uv, s_us):
    i = lax.axis_index("dp")
    j = lax.axis_index("tp")
    x, c, z, y = i // 2, i % 2, j // 4, j % 4
    xp, xm, xq, c1 = (x + 1) % 4, (x + 3) % 4, (x + 2) % 4, 1 - c
    dev = {
        "xp": {"dp": 2 * xp + c}, "xm": {"dp": 2 * xm + c}, "pc": {"dp": 2 * x + c1},
        "yp": {"tp": 4 * z + (y + 1) % 4}, "ym": {"tp": 4 * z + (y + 3) % 4},
        "zp": {"tp": 4 * ((z + 1) % 4) + y}, "zm": {"tp": 4 * ((z + 3) % 4) + y},
    }
    pos = ((z, y), (y, z))
    link = (("zp", "zm", "yp", "ym"), ("yp", "ym", "zp", "zm"))

    def remote(src, dst, ss, rs, to):
        return pltpu.make_async_remote_copy(src_ref=src, dst_ref=dst, send_sem=ss, recv_sem=rs, device_id=dev[to], device_id_type=MESH)

    def add(dst, src, n):
        def body(r, _):
            s = pl.ds(pl.multiple_of(r * 32, 32), 32)
            dst[s, :] = dst[s, :] + src[s, :]
            return 0
        lax.fori_loop(0, n // 32, body, 0)

    sends = []

    def send(src, dst, to):
        k = len(sends)
        r = remote(src, dst, ssem.at[k], rsem.at[k], to)
        r.start()
        sends.append(r)
        return r

    def wblk(k, xx, cc, half=None):
        ii = 2 * xx + cc
        if k < 2:
            r = (wgf, wuf)[k]
            if half is None:
                return r.at[pl.ds(pl.multiple_of(ii * 512, 512), 512), :]
            return r.at[pl.ds(pl.multiple_of(ii * 512 + half * 256, 256), 256), :]
        if half is None:
            return wdf.at[ii]
        return wdf.at[ii, pl.ds(half * 448, 448), :]

    def rows(a, col, s, p, lo=0, n=32):
        zz, yy = (p, s) if col == 0 else (s, p)
        return xd.at[a, pl.ds(pl.multiple_of((zz * 4 + yy) * 64 + col * 32 + lo, 16), n), :]

    GA = {}
    GA2 = {}
    GB = {}
    tail = {0: [], 1: []}

    def geo(col):
        sec, prim = pos[col]
        sp, sm, pp, pm = link[col]
        return prim, sec, pp, pm, sp, sm

    def start_own(a):
        for col in range(2):
            p, s, pp, pm, sp, sm = geo(col)
            src = res.at[a, pl.ds(col * 32, 32), :]
            dst = rows(a, col, p, s)
            GA[a, col] = (send(src, dst, pp), send(src, dst, pm))
            GB[a, col, 0] = (send(src, dst, sp), send(src, dst, sm))

    def step_a(a):
        for col in range(2):
            p, s, pp, pm, sp, sm = geo(col)
            out = []
            for fr, d, lo, fw in ((0, 3, 0, pp), (1, 1, 16, pm)):
                GA[a, col][fr].wait_recv()
                q = (p + d) % 4
                r = rows(a, col, q, s, lo, 16)
                out.append(send(r, r, fw))
                r = rows(a, col, q, s)
                GB[a, col, d] = (send(r, r, sp), send(r, r, sm))
            GA2[a, col] = out

    def step_a2(a):
        for col in range(2):
            p, s, pp, pm, sp, sm = geo(col)
            for m in GA2[a, col]:
                m.wait_recv()
            r = rows(a, col, (p + 2) % 4, s)
            GB[a, col, 2] = (send(r, r, sp), send(r, r, sm))

    def step_b(a, d):
        for col in range(2):
            p, s, pp, pm, sp, sm = geo(col)
            q = (p + d) % 4
            for fr, e, lo, fw in ((0, 3, 0, sp), (1, 1, 16, sm)):
                GB[a, col, d][fr].wait_recv()
                r = rows(a, col, q, (s + e) % 4, lo, 16)
                tail[a].append(send(r, r, fw))

    W1 = {}
    W2 = {}
    WP = {}
    w_in = (wg_ref, wu_ref, wd_ref)

    def start_w(k):
        dst = wblk(k, x, c)
        WP[k, 0] = [send(w_in[k], dst, "pc")]
        W1[k] = (send(w_in[k], dst, "xp"), send(w_in[k], dst, "xm"))

    def step_w(k):
        out = []
        for fr, xx, d, half, fw in ((0, xm, 3, 0, "xp"), (1, xp, 1, 1, "xm")):
            W1[k][fr].wait_recv()
            r = wblk(k, xx, c, half)
            out.append(send(r, r, fw))
            r = wblk(k, xx, c)
            WP[k, d] = [send(r, r, "pc")]
        W2[k] = out

    def step_w2(k):
        WP[k, 2] = []
        for half in range(2):
            W2[k][half].wait_recv()
            r = wblk(k, xq, c, half)
            WP[k, 2].append(send(r, r, "pc"))

    def wait_wp(k, d):
        for m in WP[k, d]:
            m.wait_recv()

    xpos = {0: x, 1: xp, 2: xq, 3: xm}
    order = ((0, 0), (0, 1), (3, 0), (1, 0), (3, 1), (1, 1), (2, 0), (2, 1))

    def blk(t):
        d, o = order[t]
        return 2 * xpos[d] + (c if o == 0 else c1)

    def a_slot(t):
        s = t % 4
        return A.at[s // 2, s % 2]

    def ld_ab(t):
        d, o = order[t]
        s = t % 4
        ii = blk(t)
        out = [pltpu.make_async_copy(xd.at[0, :, pl.ds(pl.multiple_of(ii * 512, 512), 512)], a_slot(t), s_c.at[s, 0])]
        for k in range(2):
            src = w_in[k] if t == 0 else wblk(k, xpos[d], c if o == 0 else c1)
            out.append(pltpu.make_async_copy(src, WX.at[s % 2, k, pl.ds((s // 2) * 512, 512), :], s_c.at[s, 1 + k]))
        return out

    def start_ab(t):
        d, o = order[t]
        if o == 1:
            for k in range(2):
                wait_wp(k, d)
        for l in ld_ab(t):
            l.start()

    def ab(t):
        for l in ld_ab(t):
            l.wait()
        s = t % 4

        def body(m, _):
            r = pl.ds(pl.multiple_of(m * 256, 256), 256)
            lhs = A[s // 2, s % 2, r, :]
            for k in range(2):
                v = jnp.dot(lhs, WX[s % 2, k, pl.ds((s // 2) * 512, 512), :], preferred_element_type=F32)
                if t == 0:
                    XB[2 * k + m // 2, m % 2] = v
                else:
                    XB[2 * k + m // 2, m % 2] += v
            return 0
        lax.fori_loop(0, 4, body, 0)

    def h_pass():
        def body(q, _):
            m = q // 8
            r = pl.ds(pl.multiple_of((q % 8) * 32, 32), 32)
            a = XB[m // 2, m % 2, r, :]
            b = XB[2 + m // 2, m % 2, r, :]
            sig = jax.nn.sigmoid(a)
            sa = a * sig
            XB[m // 2, m % 2, r, :] = b * sig * (1.0 + a * (1.0 - sig))
            XB[2 + m // 2, m % 2, r, :] = sa
            B[0, 0, pl.ds(pl.multiple_of(q * 32, 32), 32), :] = (sa * b).astype(BF)
            return 0
        lax.fori_loop(0, 32, body, 0)

    uv_put = pltpu.make_async_copy(XB, UV, s_uv)

    def ld_g(t):
        d, o = order[t]
        s = t % 4
        ii = blk(t)
        src = wd_ref if t == 0 else wdf.at[ii]
        return [pltpu.make_async_copy(xd.at[1, :, pl.ds(pl.multiple_of(ii * 512, 512), 512)], a_slot(t), s_c.at[s, 0]),
                pltpu.make_async_copy(src, WX.at[s % 2, s // 2, pl.ds(0, 896), pl.ds(0, 512)], s_c.at[s, 1])]

    def start_g(t):
        for l in ld_g(t):
            l.start()

    def gg(t):
        for l in ld_g(t):
            l.wait()
        s = t % 4

        def body(m, _):
            r = pl.ds(pl.multiple_of(m * 256, 256), 256)
            v = lax.dot_general(A[s // 2, s % 2, r, :], WX[s % 2, s // 2, pl.ds(0, 896), pl.ds(0, 512)], NT, preferred_element_type=F32)
            if t == 0:
                XS[m] = v
            else:
                XS[m] += v
            return 0
        lax.fori_loop(0, 4, body, 0)

    def us_load(q, k):
        m = q // 2
        return pltpu.make_async_copy(UV.at[2 * k + m // 2, m % 2, pl.ds(pl.multiple_of((q % 2) * 128, 128), 128), :], US.at[q % 2, k], s_us.at[q % 2, k])

    def dadb():
        for k in range(2):
            us_load(0, k).start()

        def body(q, _):
            @pl.when(q < 7)
            def _():
                for k in range(2):
                    us_load(q + 1, k).start()
            for k in range(2):
                us_load(q, k).wait()

            def inner(e, _):
                r = pl.ds(pl.multiple_of(e * 32, 32), 32)
                g = XS[q // 2, pl.ds(pl.multiple_of((q % 2) * 128 + e * 32, 32), 32), :]
                o = pl.ds(pl.multiple_of(q * 128 + e * 32, 32), 32)
                for k in range(2):
                    B[1 + k, 0, o, :] = (g * US[q % 2, k, r, :]).astype(BF)
                return 0
            lax.fori_loop(0, 4, inner, 0)
            return 0
        lax.fori_loop(0, 8, body, 0)

    def chunk(idx):
        return (x + 6 - idx) % 4

    bp = [remote(B.at[k, 0], B.at[k, 1], s_b.at[k], r_b.at[k], "pc") for k in range(3)]

    def ap(arr, idx):
        return remote(xd.at[arr, :, pl.ds(pl.multiple_of(1024 * chunk(idx) + 512 * c1, 512), 512)], AP.at[arr, idx], s_ap.at[arr, idx], r_ap.at[arr, idx], "pc")

    def load_a(arr, idx):
        slot = idx % 2
        return (pltpu.make_async_copy(xd.at[arr, :, pl.ds(pl.multiple_of(1024 * chunk(idx) + 512 * c, 512), 512)], A.at[slot, 0], s_a.at[slot, 0]),
                pltpu.make_async_copy(AP.at[arr, idx], A.at[slot, 1], s_a.at[slot, 1]))

    def start_a(arr, idx):
        for l in load_a(arr, idx):
            l.start()

    def dot_x(k, idx):
        slot = idx % 2
        for l in load_a(0, idx):
            l.wait()

        def body(m, _):
            cols = pl.ds(pl.multiple_of(m * 256, 256), 256)
            XB[idx, m] = (lax.dot_general(A[slot, 0, :, cols], B[k, 0], TN, preferred_element_type=F32)
                          + lax.dot_general(A[slot, 1, :, cols], B[k, 1], TN, preferred_element_type=F32))
            return 0
        lax.fori_loop(0, 2, body, 0)

    def xmsg(k, t):
        src = (XB.at[0, 0], XB.at[0, 1], XB.at[1, 1], XB.at[3, 0], XB.at[1, 0], XB.at[3, 1])[t]
        return remote(src, XR.at[k, t], s_xs.at[t], r_xs.at[k, t], ("xp", "xm")[t % 2])

    def x1(k):
        arr = 1 - min(k, 1)
        if k < 2:
            for idx in range(2):
                ap(arr, idx).wait_recv()
                start_a(arr, idx)
        bp[k].wait_recv()
        if k == 0:
            uv_put.wait()
        else:
            xmsg(k - 1, 0).wait_send()
            xmsg(k - 1, 1).wait_send()
        dot_x(k, 0)
        xmsg(k, 0).start()
        xmsg(k, 1).start()
        if k < 2:
            ap(arr, 2).wait_recv()
        start_a(arr, 2)

    def x2(k):
        arr = 1 - min(k, 1)
        if k > 0:
            for t in range(2, 6):
                xmsg(k - 1, t).wait_send()
            xout(k - 1).wait()

        def body(idx, _):
            dot_x(k, idx)
            if k == 1:
                @pl.when(idx == 1)
                def _():
                    ap(arr, 3).wait_recv()
                start_a(0, (idx + 2) % 4)
            else:
                @pl.when(idx == 1)
                def _():
                    if k == 0:
                        ap(arr, 3).wait_recv()
                    start_a(arr, 3)
            return 0
        lax.fori_loop(1, 4, body, 0)
        xmsg(k, 2).start()
        xmsg(k, 3).start()

    def xstage(k, t, slot):
        return pltpu.make_async_copy(XR.at[k, t], XS.at[slot], s_xst.at[slot])

    def x3(k):
        for t in range(2):
            xmsg(k, t).wait_recv()
            xstage(k, t, t).start()
        for t in range(2):
            xstage(k, t, t).wait()
            add(XB.at[(1, 3)[t], t], XS.at[t], 256)
            xmsg(k, 4 + t).start()

    def xout(k):
        return pltpu.make_async_copy(XB.at[2], dw.at[k], s_xo)

    def xf(k):
        todo = ((3, 0), (2, 1), (4, 0), (5, 1))
        for n, (t, h) in enumerate(todo):
            xmsg(k, t).wait_recv()
            xstage(k, t, n).start()
        for n, (t, h) in enumerate(todo):
            xstage(k, t, n).wait()
            add(XB.at[2, h], XS.at[n], 256)
        xout(k).start()

    def pair(n, col):
        return ((0, 3), (1, 2))[col][n % 2]

    def load_w(n):
        out = []
        for col in range(2):
            d = pair(n, col)
            q = xpos[d]
            if n < 2:
                if d == 0:
                    out.append(pltpu.make_async_copy(wd_ref, WD.at[col, c], s_w.at[col, 0]))
                    out.append(pltpu.make_async_copy(wdf.at[2 * x + c1], WD.at[col, c1], s_w.at[col, 1]))
                else:
                    out.append(pltpu.make_async_copy(wdf.at[pl.ds(2 * q, 2)], WD.at[col], s_w.at[col, 0]))
            else:
                for k in range(2):
                    full = (wgf, wuf)[k]
                    if d == 0:
                        out.append(pltpu.make_async_copy(w_in[k], WX.at[col, k, pl.ds(pl.multiple_of(512 * c, 512), 512), :], s_w.at[col, 2 * k]))
                        out.append(pltpu.make_async_copy(full.at[pl.ds(pl.multiple_of(1024 * x + 512 * c1, 512), 512), :],
                                                         WX.at[col, k, pl.ds(pl.multiple_of(512 * c1, 512), 512), :], s_w.at[col, 2 * k + 1]))
                    else:
                        out.append(pltpu.make_async_copy(full.at[pl.ds(pl.multiple_of(1024 * q, 1024), 1024), :], WX.at[col, k], s_w.at[col, 2 * k]))
        for o in out:
            o.start()
        return out

    wl = {}

    def dots_z(n, lo, hi):
        m = hi - lo

        def body(q, _):
            col = q // m
            idx = lo + q % m
            p = z + col * (y - z)
            ch = (p + 6 - idx) % 4
            s1 = 256 - 192 * col
            s2 = 64 + 192 * col
            own = (idx // 2) * (1 - idx // 3)
            slot = idx + own * 2 * (n % 2)

            def lhs(k):
                return jnp.concatenate([B[k, 0, pl.ds(pl.multiple_of(ch * s1 + g * s2, 64), 64), :] for g in range(4)], axis=0)

            if n < 2:
                l = lhs(0)
                for h in range(2):
                    ZB[col, slot, h] = jnp.dot(l, WD[col, h], preferred_element_type=F32)
            else:
                l = lhs(1)
                u = lhs(2)
                for h in range(2):
                    r = pl.ds(512 * h, 512)
                    ZB[col, slot, h] = (lax.dot_general(l, WX[col, 0, r, :], NT, preferred_element_type=F32)
                                        + lax.dot_general(u, WX[col, 1, r, :], NT, preferred_element_type=F32))
            return 0
        lax.fori_loop(0, 2 * m, body, 0)

    def zmsg(n, col, t):
        src = ((0, 0), (0, 1), (1, 1), (3, 0), (1, 0), (3, 1))[t]
        return remote(ZB.at[col, src[0], src[1]], ZR.at[col, n, t], s_zs.at[col, t], r_zs.at[col, n, t], link[col][t % 2])

    def own(n, col, h):
        return ZB.at[col, 2 + 2 * (n % 2), h]

    def sub(n, col, h, d):
        s = (pos[col][1] + d) % 4
        return ZB.at[col, 2 + 2 * (n % 2), h, pl.ds(pl.multiple_of(s * 64, 64), 64), :]

    def msg2(n, col, t):
        h, d = ((0, 2), (1, 2), (1, 1), (0, 3), (0, 1), (1, 3))[t]
        return remote(sub(n, col, h, d), Z2.at[col, n % 2, t], s_2.at[col, n % 2, t], r_2.at[col, n, t], link[col][2 + t % 2])

    def p1(n):
        for l in wl[n]:
            l.wait()
        if n > 0:
            for col in range(2):
                for t in range(2):
                    zmsg(n - 1, col, t).wait_send()
        dots_z(n, 0, 1)
        for t in range(2):
            for col in range(2):
                zmsg(n, col, t).start()

    def p2(n):
        if n > 0:
            for col in range(2):
                for t in range(2, 6):
                    zmsg(n - 1, col, t).wait_send()
        if n > 1:
            for col in range(2):
                for t in range(6):
                    msg2(n - 2, col, t).wait_send()
        dots_z(n, 1, 4)
        for t in range(2, 4):
            for col in range(2):
                zmsg(n, col, t).start()

    def zstage(n, col, t, slot):
        return pltpu.make_async_copy(ZR.at[col, n, t], ZS.at[col, slot], s_zst.at[col, slot])

    def p4(n):
        for t in range(2):
            for col in range(2):
                zmsg(n, col, t).wait_recv()
                zstage(n, col, t, t).start()
        for t in range(2):
            for col in range(2):
                zstage(n, col, t, t).wait()
                add(ZB.at[col, (1, 3)[t], t], ZS.at[col, t], 256)
                zmsg(n, col, 4 + t).start()

    def f(n):
        todo = ((3, 0), (2, 1), (4, 0), (5, 1))
        for e, (t, h) in enumerate(todo):
            for col in range(2):
                zmsg(n, col, t).wait_recv()
                zstage(n, col, t, e).start()
        for e, (t, h) in enumerate(todo):
            for col in range(2):
                zstage(n, col, t, e).wait()
                add(own(n, col, h), ZS.at[col, e], 256)
        for t in range(4):
            for col in range(2):
                msg2(n, col, t).start()

    def hh2(n):
        for t in range(2):
            for col in range(2):
                msg2(n, col, t).wait_recv()
                add(sub(n, col, t, (1, 3)[t]), Z2.at[col, n % 2, t], 64)
                msg2(n, col, 4 + t).start()

    def zf(n):
        a = n // 2
        for col in range(2):
            q = xpos[pair(n, col)]
            for h, ts in ((0, (3, 4)), (1, (2, 5))):
                for t in ts:
                    msg2(n, col, t).wait_recv()
                cs = pl.ds(pl.multiple_of(1024 * q + 512 * h, 512), 512)
                v = sub(n, col, h, 0)[...] + Z2[col, n % 2, ts[0]] + Z2[col, n % 2, ts[1]]
                ov[a, :, cs] = (res[a, :, cs].astype(F32) + v).astype(BF)

    own_ld = [pltpu.make_async_copy(r, res.at[k], s_ld.at[k]) for k, r in enumerate((x_ref, dy_ref))]
    for l in own_ld:
        l.start()
    barrier = pltpu.get_barrier_semaphore()
    for d in dev.values():
        pl.semaphore_signal(barrier, inc=1, device_id=d, device_id_type=MESH)
    pl.semaphore_wait(barrier, len(dev))
    own_ld[0].wait()
    start_own(0)
    start_w(0)
    start_w(1)
    own_ld[1].wait()
    put = pltpu.make_async_copy(res, xd.at[:, pl.ds(pl.multiple_of(j * 64, 64), 64), :], s_put)
    put.start()
    step_a(0)
    step_b(0, 0)
    step_a2(0)
    step_w(0)
    step_b(0, 3)
    start_own(1)
    step_b(0, 1)
    step_b(0, 2)
    step_w(1)
    start_w(2)
    put.wait()
    for m in tail[0]:
        m.wait_recv()
    for idx in range(4):
        ap(0, idx).start()
    start_ab(0)
    start_ab(1)
    ab(0)
    step_a(1)
    start_ab(2)
    ab(1)
    step_b(1, 0)
    step_w2(0)
    start_ab(3)
    ab(2)
    step_a2(1)
    start_ab(4)
    ab(3)
    step_b(1, 3)
    start_ab(5)
    ab(4)
    step_w2(1)
    start_ab(6)
    ab(5)
    step_b(1, 1)
    start_ab(7)
    ab(6)
    ab(7)
    step_b(1, 2)
    h_pass()
    bp[0].start()
    uv_put.start()
    step_w(2)
    wait_wp(2, 0)
    wait_wp(2, 1)
    wl[0] = load_w(0)
    p1(0)
    for m in tail[1]:
        m.wait_recv()
    for idx in range(4):
        ap(1, idx).start()
    x1(0)
    step_w2(2)
    p2(0)
    wait_wp(2, 3)
    wait_wp(2, 2)
    wl[1] = load_w(1)
    p4(0)
    x2(0)
    for t in range(3):
        start_g(t)
    for t in range(8):
        gg(t)
        if t + 3 < 8:
            start_g(t + 3)
        if t == 3:
            p1(1)
    f(0)
    dadb()
    bp[1].start()
    bp[2].start()
    wl[2] = load_w(2)
    x3(0)
    p2(1)
    x1(1)
    hh2(0)
    zf(0)
    p4(1)
    xf(0)
    x2(1)
    p1(2)
    f(1)
    p2(2)
    wl[3] = load_w(3)
    x3(1)
    hh2(1)
    zf(1)
    p4(2)
    x1(2)
    p1(3)
    f(2)
    xf(1)
    x2(2)
    p2(3)
    hh2(2)
    zf(2)
    p4(3)
    x3(2)
    f(3)
    hh2(3)
    zf(3)
    out = pltpu.make_async_copy(ov, yo, s_yo)
    out.start()
    xf(2)
    for r in sends:
        r.wait_send()
    for t in range(6):
        xmsg(2, t).wait_send()
        for col in range(2):
            zmsg(3, col, t).wait_send()
            msg2(2, col, t).wait_send()
            msg2(3, col, t).wait_send()
    for k in range(3):
        bp[k].wait_send()
    for arr in range(2):
        for idx in range(4):
            ap(arr, idx).wait_send()
    xout(2).wait()
    out.wait()


def mlp(x, dy, wg, wu, wd):
    sd = jax.ShapeDtypeStruct
    dma = pltpu.SemaphoreType.DMA
    V = pltpu.VMEM
    return pl.pallas_call(
        mlp_kernel,
        out_shape=(sd((3, 2, 256, 896), F32), sd((2, 64, 4096), BF),
                   sd((2, 1024, 4096), BF), sd((4096, 896), BF), sd((4096, 896), BF), sd((8, 896, 512), BF), sd((4, 2, 256, 896), F32),
                   sd((3, 6, 256, 896), F32), sd((2, 4, 6, 256, 512), F32), sd((2, 4, 1024, 512), BF)),
        in_specs=[HBM] * 5,
        out_specs=(HBM,) * 10,
        scratch_shapes=[
            V((3, 2, 1024, 896), BF), V((2, 2, 1024, 512), BF), V((4, 2, 256, 896), F32), V((4, 256, 896), F32),
            V((2, 2, 896, 512), BF), V((2, 2, 1024, 896), BF), V((2, 5, 2, 256, 512), F32), V((2, 4, 256, 512), F32),
            V((2, 2, 6, 64, 512), F32), V((2, 2, 128, 896), F32), V((2, 64, 4096), BF), V((2, 64, 4096), BF),
            dma((NSEND,)), dma((NSEND,)), dma((2,)), dma, dma((4, 3)),
            dma((2, 2)), dma((2, 4)), dma((2, 4)), dma((3,)), dma((3,)), dma((6,)), dma((3, 6)),
            dma((2, 6)), dma((2, 4, 6)), dma((2, 2, 6)), dma((2, 4, 6)), dma((2, 4)), dma((4,)), dma((2, 4)), dma, dma, dma, dma((2, 2)),
        ],
        compiler_params=pltpu.CompilerParams(collective_id=1, has_side_effects=True, vmem_limit_bytes=67043328),
        name="mlp",
    )(x, dy, wg, wu, wd)[:2]


def solution(mesh):
    rows = P(("dp", "tp"), None)
    wsp = P("dp", "tp")
    dsp = P("tp", "dp")

    def local(x, w_gate, w_up, w_down, dy):
        dw, yo = mlp(x, dy, w_gate, w_up, w_down)
        dw = dw.reshape(3, 512, 896)
        return yo[0], yo[1], dw[1], dw[2], dw[0].T

    return jax.shard_map(local, mesh=mesh, in_specs=(rows, wsp, wsp, dsp, rows), out_specs=(rows, rows, wsp, wsp, dsp), check_vma=False)
```

```python
import jax
import jax.numpy as jnp
from jax import lax
from jax.experimental import pallas as pl
from jax.experimental.pallas import tpu as pltpu
from jax.sharding import PartitionSpec as P

MESH = pl.DeviceIdType.MESH
HBM = pl.BlockSpec(memory_space=pltpu.HBM)
NT = (((1,), (1,)), ((), ()))
TN = (((0,), (0,)), ((), ()))
F32 = jnp.float32
BF = jnp.bfloat16
NSEND = 107


def mlp_kernel(x_ref, dy_ref, wg_ref, wu_ref, wd_ref, dw, yo, xd, wgf, wuf, wdf, UV, XR, ZR, AP,
               B, A, XB, XS, WD, WX, ZB, ZS, Z2, US, res, ov,
               ssem, rsem, s_ld, s_put, s_c, s_a, s_ap, r_ap, s_b, r_b, s_xs, r_xs, s_zs, r_zs, s_2, r_2, s_w, s_xst, s_zst, s_xo, s_yo, s_uv, s_us):
    i = lax.axis_index("dp")
    j = lax.axis_index("tp")
    x, c, z, y = i // 2, i % 2, j // 4, j % 4
    xp, xm, xq, c1 = (x + 1) % 4, (x + 3) % 4, (x + 2) % 4, 1 - c
    dev = {
        "xp": {"dp": 2 * xp + c}, "xm": {"dp": 2 * xm + c}, "pc": {"dp": 2 * x + c1},
        "yp": {"tp": 4 * z + (y + 1) % 4}, "ym": {"tp": 4 * z + (y + 3) % 4},
        "zp": {"tp": 4 * ((z + 1) % 4) + y}, "zm": {"tp": 4 * ((z + 3) % 4) + y},
    }
    pos = ((z, y), (y, z))
    link = (("zp", "zm", "yp", "ym"), ("yp", "ym", "zp", "zm"))

    def remote(src, dst, ss, rs, to):
        return pltpu.make_async_remote_copy(src_ref=src, dst_ref=dst, send_sem=ss, recv_sem=rs, device_id=dev[to], device_id_type=MESH)

    def add(dst, src, n):
        def body(r, _):
            s = pl.ds(pl.multiple_of(r * 32, 32), 32)
            dst[s, :] = dst[s, :] + src[s, :]
            return 0
        lax.fori_loop(0, n // 32, body, 0)

    sends = []

    def send(src, dst, to):
        k = len(sends)
        r = remote(src, dst, ssem.at[k], rsem.at[k], to)
        r.start()
        sends.append(r)
        return r

    def wblk(k, xx, cc, half=None):
        ii = 2 * xx + cc
        if k < 2:
            r = (wgf, wuf)[k]
            if half is None:
                return r.at[pl.ds(pl.multiple_of(ii * 512, 512), 512), :]
            return r.at[pl.ds(pl.multiple_of(ii * 512 + half * 256, 256), 256), :]
        if half is None:
            return wdf.at[ii]
        return wdf.at[ii, pl.ds(half * 448, 448), :]

    def rows(a, col, s, p, lo=0, n=32):
        zz, yy = (p, s) if col == 0 else (s, p)
        return xd.at[a, pl.ds(pl.multiple_of((zz * 4 + yy) * 64 + col * 32 + lo, 16), n), :]

    GA = {}
    GA2 = {}
    GB = {}
    tail = {0: [], 1: []}

    def geo(col):
        sec, prim = pos[col]
        sp, sm, pp, pm = link[col]
        return prim, sec, pp, pm, sp, sm

    seen = set()

    def once(m):
        if id(m) not in seen:
            seen.add(id(m))
            m.wait_recv()

    def ga(a):
        for col in range(2):
            p, s, pp, pm, sp, sm = geo(col)
            src = res.at[a, pl.ds(col * 32, 32), :]
            GA[a, col] = [send(src, rows(a, col, p, s), to) for to in (pp, pm)]

    def gb0(a):
        for col in range(2):
            p, s, pp, pm, sp, sm = geo(col)
            src = res.at[a, pl.ds(col * 32, 32), :]
            GB[a, col, 0] = [send(src, rows(a, col, p, s), to) for to in (sp, sm)]

    def ga2(a):
        for col in range(2):
            p, s, pp, pm, sp, sm = geo(col)
            GA2[a, col] = []
            for fr, d, lo, fw in ((0, 3, 0, pp), (1, 1, 16, pm)):
                once(GA[a, col][fr])
                r = rows(a, col, (p + d) % 4, s, lo, 16)
                GA2[a, col].append(send(r, r, fw))

    def gb31(a):
        for col in range(2):
            p, s, pp, pm, sp, sm = geo(col)
            for d in (3, 1):
                r = rows(a, col, (p + d) % 4, s)
                GB[a, col, d] = [send(r, r, to) for to in (sp, sm)]

    def gb2(a):
        for col in range(2):
            p, s, pp, pm, sp, sm = geo(col)
            for m in GA2[a, col]:
                once(m)
            r = rows(a, col, (p + 2) % 4, s)
            GB[a, col, 2] = [send(r, r, to) for to in (sp, sm)]

    def gf(a, d):
        for col in range(2):
            p, s, pp, pm, sp, sm = geo(col)
            q = (p + d) % 4
            for fr, e, lo, fw in ((0, 3, 0, sp), (1, 1, 16, sm)):
                once(GB[a, col, d][fr])
                r = rows(a, col, q, (s + e) % 4, lo, 16)
                tail[a].append(send(r, r, fw))

    def gend(a):
        if a == 0:
            put.wait()
        for m in tail[a]:
            once(m)
        for idx in range(4):
            ap(a, idx).start()

    W1 = {}
    W2 = {}
    WP = {}
    w_in = (wg_ref, wu_ref, wd_ref)

    def wpc(k):
        WP[k, 0] = [send(w_in[k], wblk(k, x, c), "pc")]

    def wown(k):
        W1[k] = [send(w_in[k], wblk(k, x, c), to) for to in ("xp", "xm")]

    def wf(k):
        W2[k] = []
        for fr, xx, d, half, fw in ((0, xm, 3, 0, "xp"), (1, xp, 1, 1, "xm")):
            once(W1[k][fr])
            r = wblk(k, xx, c, half)
            W2[k].append(send(r, r, fw))
            r = wblk(k, xx, c)
            WP[k, d] = [send(r, r, "pc")]

    def wf2(k):
        WP[k, 2] = []
        for half in range(2):
            once(W2[k][half])
            r = wblk(k, xq, c, half)
            WP[k, 2].append(send(r, r, "pc"))

    def have(k, d, o):
        if o == 1:
            for m in WP[k, d]:
                once(m)
        elif d == 2:
            for m in W2[k]:
                once(m)
        elif d:
            once(W1[k][0 if d == 3 else 1])

    xpos = {0: x, 1: xp, 2: xq, 3: xm}
    order = ((0, 0), (0, 1), (3, 0), (1, 0), (3, 1), (1, 1), (2, 0), (2, 1))

    def blk(t):
        d, o = order[t]
        return 2 * xpos[d] + (c if o == 0 else c1)

    def a_slot(t):
        s = t % 4
        return A.at[s // 2, s % 2]

    def ld_ab(t):
        d, o = order[t]
        s = t % 4
        ii = blk(t)
        out = [pltpu.make_async_copy(xd.at[0, :, pl.ds(pl.multiple_of(ii * 512, 512), 512)], a_slot(t), s_c.at[s, 0])]
        for k in range(2):
            src = w_in[k] if t == 0 else wblk(k, xpos[d], c if o == 0 else c1)
            out.append(pltpu.make_async_copy(src, WX.at[s % 2, k, pl.ds((s // 2) * 512, 512), :], s_c.at[s, 1 + k]))
        return out

    def sab(t):
        for k in range(2):
            have(k, *order[t])
        for l in ld_ab(t):
            l.start()

    def ab(t):
        for l in ld_ab(t):
            l.wait()
        s = t % 4

        def body(m, _):
            r = pl.ds(pl.multiple_of(m * 256, 256), 256)
            lhs = A[s // 2, s % 2, r, :]
            for k in range(2):
                v = jnp.dot(lhs, WX[s % 2, k, pl.ds((s // 2) * 512, 512), :], preferred_element_type=F32)
                if t == 0:
                    XB[2 * k + m // 2, m % 2] = v
                else:
                    XB[2 * k + m // 2, m % 2] += v
            return 0
        lax.fori_loop(0, 4, body, 0)

    def hp():
        def body(q, _):
            m = q // 8
            r = pl.ds(pl.multiple_of((q % 8) * 32, 32), 32)
            a = XB[m // 2, m % 2, r, :]
            b = XB[2 + m // 2, m % 2, r, :]
            sig = jax.nn.sigmoid(a)
            sa = a * sig
            XB[m // 2, m % 2, r, :] = b * sig * (1.0 + a * (1.0 - sig))
            XB[2 + m // 2, m % 2, r, :] = sa
            B[0, 0, pl.ds(pl.multiple_of(q * 32, 32), 32), :] = (sa * b).astype(BF)
            return 0
        lax.fori_loop(0, 32, body, 0)
        bp[0].start()
        uv_put.start()

    uv_put = pltpu.make_async_copy(XB, UV, s_uv)

    def ld_g(t):
        d, o = order[t]
        s = t % 4
        ii = blk(t)
        src = wd_ref if t == 0 else wdf.at[ii]
        return [pltpu.make_async_copy(xd.at[1, :, pl.ds(pl.multiple_of(ii * 512, 512), 512)], a_slot(t), s_c.at[s, 0]),
                pltpu.make_async_copy(src, WX.at[s % 2, s // 2, pl.ds(0, 896), pl.ds(0, 512)], s_c.at[s, 1])]

    def sg(t):
        have(2, *order[t])
        for l in ld_g(t):
            l.start()

    def gg(t):
        for l in ld_g(t):
            l.wait()
        s = t % 4

        def body(m, _):
            r = pl.ds(pl.multiple_of(m * 256, 256), 256)
            v = lax.dot_general(A[s // 2, s % 2, r, :], WX[s % 2, s // 2, pl.ds(0, 896), pl.ds(0, 512)], NT, preferred_element_type=F32)
            if t == 0:
                XS[m] = v
            else:
                XS[m] += v
            return 0
        lax.fori_loop(0, 4, body, 0)

    def us_load(q, k):
        m = q // 2
        return pltpu.make_async_copy(UV.at[2 * k + m // 2, m % 2, pl.ds(pl.multiple_of((q % 2) * 128, 128), 128), :], US.at[q % 2, k], s_us.at[q % 2, k])

    def dadb():
        for k in range(2):
            us_load(0, k).start()

        def body(q, _):
            @pl.when(q < 7)
            def _():
                for k in range(2):
                    us_load(q + 1, k).start()
            for k in range(2):
                us_load(q, k).wait()

            def inner(e, _):
                r = pl.ds(pl.multiple_of(e * 32, 32), 32)
                g = XS[q // 2, pl.ds(pl.multiple_of((q % 2) * 128 + e * 32, 32), 32), :]
                o = pl.ds(pl.multiple_of(q * 128 + e * 32, 32), 32)
                for k in range(2):
                    B[1 + k, 0, o, :] = (g * US[q % 2, k, r, :]).astype(BF)
                return 0
            lax.fori_loop(0, 4, inner, 0)
            return 0
        lax.fori_loop(0, 8, body, 0)
        bp[1].start()
        bp[2].start()

    def chunk(idx):
        return (x + 6 - idx) % 4

    bp = [remote(B.at[k, 0], B.at[k, 1], s_b.at[k], r_b.at[k], "pc") for k in range(3)]

    APM = {}

    def ap(arr, idx):
        if (arr, idx) not in APM:
            APM[arr, idx] = ap_(arr, idx)
        return APM[arr, idx]

    def ap_(arr, idx):
        return remote(xd.at[arr, :, pl.ds(pl.multiple_of(1024 * chunk(idx) + 512 * c1, 512), 512)], AP.at[arr, idx], s_ap.at[arr, idx], r_ap.at[arr, idx], "pc")

    seq = (0, 1, 3, 2)

    def load_a(k, n):
        arr = 1 - min(k, 1)
        idx = seq[n]
        return (pltpu.make_async_copy(xd.at[arr, :, pl.ds(pl.multiple_of(1024 * chunk(idx) + 512 * c, 512), 512)], A.at[n % 2, 0], s_a.at[n % 2, 0]),
                pltpu.make_async_copy(AP.at[arr, idx], A.at[n % 2, 1], s_a.at[n % 2, 1]))

    def start_a(k, n):
        once(ap(1 - min(k, 1), seq[n]))
        for l in load_a(k, n):
            l.start()

    def dot_x(k, n):
        slot = n % 2
        for l in load_a(k, n):
            l.wait()

        def body(m, _):
            cols = pl.ds(pl.multiple_of(m * 256, 256), 256)
            XB[seq[n], m] = (lax.dot_general(A[slot, 0, :, cols], B[k, 0], TN, preferred_element_type=F32)
                             + lax.dot_general(A[slot, 1, :, cols], B[k, 1], TN, preferred_element_type=F32))
            return 0
        lax.fori_loop(0, 2, body, 0)

    def xmsg(k, t):
        src = (XB.at[0, 0], XB.at[0, 1], XB.at[1, 1], XB.at[3, 0], XB.at[1, 0], XB.at[3, 1])[t]
        return remote(src, XR.at[k, t], s_xs.at[t], r_xs.at[k, t], ("xp", "xm")[t % 2])

    def xl0(k):
        start_a(k, 0)
        start_a(k, 1)

    def x1(k):
        bp[k].wait_recv()
        if k == 0:
            uv_put.wait()
        else:
            xmsg(k - 1, 0).wait_send()
            xmsg(k - 1, 1).wait_send()
        dot_x(k, 0)
        xmsg(k, 0).start()
        xmsg(k, 1).start()
        start_a(k, 2)

    def x2(k):
        if k > 0:
            for t in range(2, 6):
                xmsg(k - 1, t).wait_send()
        dot_x(k, 1)
        start_a(k, 3)
        xmsg(k, 2).start()
        dot_x(k, 2)
        if k == 1:
            start_a(2, 0)
        xmsg(k, 3).start()

    def x2o(k):
        if k > 0:
            xout(k - 1).wait()
        dot_x(k, 3)
        if k == 1:
            start_a(2, 1)

    def xstage(k, t, slot):
        return pltpu.make_async_copy(XR.at[k, t], XS.at[slot], s_xst.at[slot])

    def x3(k):
        for t in range(2):
            xmsg(k, t).wait_recv()
            xstage(k, t, t).start()
        for t in range(2):
            xstage(k, t, t).wait()
            add(XB.at[(1, 3)[t], t], XS.at[t], 256)
            xmsg(k, 4 + t).start()

    def xout(k):
        return pltpu.make_async_copy(XB.at[2], dw.at[k], s_xo)

    def xf(k):
        todo = ((3, 0), (2, 1), (4, 0), (5, 1))
        for n, (t, h) in enumerate(todo):
            xmsg(k, t).wait_recv()
            xstage(k, t, n).start()
        for n, (t, h) in enumerate(todo):
            xstage(k, t, n).wait()
            add(XB.at[2, h], XS.at[n], 256)
        xout(k).start()

    def pair(n, col):
        return ((0, 3), (1, 2))[col][n % 2]

    def lw(n):
        if n < 2:
            for col in range(2):
                have(2, pair(n, col), 0)
                have(2, pair(n, col), 1)
        out = []
        for col in range(2):
            d = pair(n, col)
            q = xpos[d]
            if n < 2:
                if d == 0:
                    out.append(pltpu.make_async_copy(wd_ref, WD.at[col, c], s_w.at[col, 0]))
                    out.append(pltpu.make_async_copy(wdf.at[2 * x + c1], WD.at[col, c1], s_w.at[col, 1]))
                else:
                    out.append(pltpu.make_async_copy(wdf.at[pl.ds(2 * q, 2)], WD.at[col], s_w.at[col, 0]))
            else:
                for k in range(2):
                    full = (wgf, wuf)[k]
                    if d == 0:
                        out.append(pltpu.make_async_copy(w_in[k], WX.at[col, k, pl.ds(pl.multiple_of(512 * c, 512), 512), :], s_w.at[col, 2 * k]))
                        out.append(pltpu.make_async_copy(full.at[pl.ds(pl.multiple_of(1024 * x + 512 * c1, 512), 512), :],
                                                         WX.at[col, k, pl.ds(pl.multiple_of(512 * c1, 512), 512), :], s_w.at[col, 2 * k + 1]))
                    else:
                        out.append(pltpu.make_async_copy(full.at[pl.ds(pl.multiple_of(1024 * q, 1024), 1024), :], WX.at[col, k], s_w.at[col, 2 * k]))
        for o in out:
            o.start()
        wl[n] = out

    wl = {}

    def dots_z(n, lo, m):

        def body(q, _):
            col = q // m
            idx = lo + 2 * (q % m)
            p = z + col * (y - z)
            ch = (p + 6 - idx) % 4
            s1 = 256 - 192 * col
            s2 = 64 + 192 * col
            own = (idx // 2) * (1 - idx // 3)
            slot = idx + own * 2 * (n % 2)

            def lhs(k):
                return jnp.concatenate([B[k, 0, pl.ds(pl.multiple_of(ch * s1 + g * s2, 64), 64), :] for g in range(4)], axis=0)

            if n < 2:
                l = lhs(0)
                for h in range(2):
                    ZB[col, slot, h] = jnp.dot(l, WD[col, h], preferred_element_type=F32)
            else:
                l = lhs(1)
                u = lhs(2)
                for h in range(2):
                    r = pl.ds(512 * h, 512)
                    ZB[col, slot, h] = (lax.dot_general(l, WX[col, 0, r, :], NT, preferred_element_type=F32)
                                        + lax.dot_general(u, WX[col, 1, r, :], NT, preferred_element_type=F32))
            return 0
        lax.fori_loop(0, 2 * m, body, 0)

    def zmsg(n, col, t):
        src = ((0, 0), (0, 1), (1, 1), (3, 0), (1, 0), (3, 1))[t]
        return remote(ZB.at[col, src[0], src[1]], ZR.at[col, n, t], s_zs.at[col, t], r_zs.at[col, n, t], link[col][t % 2])

    def own(n, col, h):
        return ZB.at[col, 2 + 2 * (n % 2), h]

    def sub(n, col, h, d):
        s = (pos[col][1] + d) % 4
        return ZB.at[col, 2 + 2 * (n % 2), h, pl.ds(pl.multiple_of(s * 64, 64), 64), :]

    def msg2(n, col, t):
        h, d = ((0, 2), (1, 2), (1, 1), (0, 3), (0, 1), (1, 3))[t]
        return remote(sub(n, col, h, d), Z2.at[col, n, t], s_2.at[col, n % 2, t], r_2.at[col, n, t], link[col][2 + t % 2])

    def p1(n):
        for l in wl[n]:
            l.wait()
        if n > 0:
            for col in range(2):
                for t in range(2):
                    zmsg(n - 1, col, t).wait_send()
        dots_z(n, 0, 1)
        for t in range(2):
            for col in range(2):
                zmsg(n, col, t).start()

    def p2(n):
        if n > 0:
            for col in range(2):
                for t in range(2, 6):
                    zmsg(n - 1, col, t).wait_send()
        dots_z(n, 1, 2)
        for t in range(2, 4):
            for col in range(2):
                zmsg(n, col, t).start()

    def p2o(n):
        if n > 1:
            for col in range(2):
                for t in range(6):
                    msg2(n - 2, col, t).wait_send()
        dots_z(n, 2, 1)

    def zstage(n, col, t, slot):
        return pltpu.make_async_copy(ZR.at[col, n, t], ZS.at[col, slot], s_zst.at[col, slot])

    def p4(n):
        for t in range(2):
            for col in range(2):
                zmsg(n, col, t).wait_recv()
                zstage(n, col, t, t).start()
        for t in range(2):
            for col in range(2):
                zstage(n, col, t, t).wait()
                add(ZB.at[col, (1, 3)[t], t], ZS.at[col, t], 256)
                zmsg(n, col, 4 + t).start()

    def f(n):
        todo = ((3, 0), (2, 1), (4, 0), (5, 1))
        for e, (t, h) in enumerate(todo):
            for col in range(2):
                zmsg(n, col, t).wait_recv()
                zstage(n, col, t, e).start()
        for e, (t, h) in enumerate(todo):
            for col in range(2):
                zstage(n, col, t, e).wait()
                add(own(n, col, h), ZS.at[col, e], 256)
        for t in range(4):
            for col in range(2):
                msg2(n, col, t).start()

    def hh(n):
        for t in range(2):
            for col in range(2):
                msg2(n, col, t).wait_recv()
                add(sub(n, col, t, (1, 3)[t]), Z2.at[col, n, t], 64)
                msg2(n, col, 4 + t).start()

    def zf(n):
        a = n // 2
        for col in range(2):
            q = xpos[pair(n, col)]
            for h, ts in ((0, (3, 4)), (1, (2, 5))):
                for t in ts:
                    msg2(n, col, t).wait_recv()
                cs = pl.ds(pl.multiple_of(1024 * q + 512 * h, 512), 512)
                v = sub(n, col, h, 0)[...] + Z2[col, n, ts[0]] + Z2[col, n, ts[1]]
                ov[a, :, cs] = (res[a, :, cs].astype(F32) + v).astype(BF)
        if n == 3:
            out.start()

    own_ld = [pltpu.make_async_copy(r, res.at[k], s_ld.at[k]) for k, r in enumerate((x_ref, dy_ref))]
    for l in own_ld:
        l.start()
    barrier = pltpu.get_barrier_semaphore()
    for d in dev.values():
        pl.semaphore_signal(barrier, inc=1, device_id=d, device_id_type=MESH)
    pl.semaphore_wait(barrier, len(dev))
    own_ld[0].wait()
    own_ld[1].wait()
    put = pltpu.make_async_copy(res, xd.at[:, pl.ds(pl.multiple_of(j * 64, 64), 64), :], s_put)
    put.start()
    out = pltpu.make_async_copy(ov, yo, s_yo)
    wpc(0)
    wown(0)
    ga(1)
    wpc(2)
    ga(0)
    wown(1)
    wpc(1)
    gb0(0)
    ga2(1)
    ga2(0)
    gb31(0)
    gb2(0)
    gf(0, 0)
    wf(0)
    gf(0, 3)
    gf(0, 2)
    wf(1)
    gf(0, 1)
    gb2(1)
    gend(0)
    wown(2)
    sab(3)
    wf2(0)
    sab(0)
    sab(2)
    sab(1)
    gb0(1)
    ab(0)
    ab(1)
    gb31(1)
    ab(2)
    wf2(1)
    sab(4)
    ab(3)
    sab(6)
    sab(5)
    gf(1, 2)
    gf(1, 0)
    ab(4)
    sab(7)
    ab(5)
    ab(6)
    gf(1, 1)
    ab(7)
    gf(1, 3)
    wf(2)
    hp()
    gend(1)
    lw(0)
    p1(0)
    xl0(0)
    x1(0)
    wf2(2)
    x2(0)
    p2(0)
    x2o(0)
    sg(1)
    sg(2)
    sg(0)
    gg(0)
    gg(1)
    sg(3)
    gg(2)
    sg(4)
    sg(6)
    gg(3)
    sg(5)
    gg(4)
    gg(5)
    gg(6)
    p2o(0)
    lw(1)
    sg(7)
    p4(0)
    gg(7)
    p1(1)
    xl0(1)
    dadb()
    x3(0)
    p2(1)
    f(0)
    p4(1)
    p2o(1)
    x1(1)
    hh(0)
    x2(1)
    f(1)
    lw(2)
    x3(1)
    xf(0)
    zf(0)
    p1(2)
    p2(2)
    hh(1)
    x1(2)
    p2o(2)
    lw(3)
    p4(2)
    zf(1)
    x2o(1)
    p1(3)
    xf(1)
    p2(3)
    x2(2)
    x3(2)
    p2o(3)
    f(2)
    p4(3)
    hh(2)
    f(3)
    x2o(2)
    hh(3)
    zf(2)
    xf(2)
    zf(3)
    for r in sends:
        r.wait_send()
    for t in range(6):
        xmsg(2, t).wait_send()
        for col in range(2):
            zmsg(3, col, t).wait_send()
            msg2(2, col, t).wait_send()
            msg2(3, col, t).wait_send()
    for k in range(3):
        bp[k].wait_send()
    for arr in range(2):
        for idx in range(4):
            ap(arr, idx).wait_send()
    xout(2).wait()
    out.wait()


def mlp(x, dy, wg, wu, wd):
    sd = jax.ShapeDtypeStruct
    dma = pltpu.SemaphoreType.DMA
    V = pltpu.VMEM
    return pl.pallas_call(
        mlp_kernel,
        out_shape=(sd((3, 2, 256, 896), F32), sd((2, 64, 4096), BF),
                   sd((2, 1024, 4096), BF), sd((4096, 896), BF), sd((4096, 896), BF), sd((8, 896, 512), BF), sd((4, 2, 256, 896), F32),
                   sd((3, 6, 256, 896), F32), sd((2, 4, 6, 256, 512), F32), sd((2, 4, 1024, 512), BF)),
        in_specs=[HBM] * 5,
        out_specs=(HBM,) * 10,
        scratch_shapes=[
            V((3, 2, 1024, 896), BF), V((2, 2, 1024, 512), BF), V((4, 2, 256, 896), F32), V((4, 256, 896), F32),
            V((2, 2, 896, 512), BF), V((2, 2, 1024, 896), BF), V((2, 5, 2, 256, 512), F32), V((2, 4, 256, 512), F32),
            V((2, 4, 6, 64, 512), F32), V((2, 2, 128, 896), F32), V((2, 64, 4096), BF), V((2, 64, 4096), BF),
            dma((NSEND,)), dma((NSEND,)), dma((2,)), dma, dma((4, 3)),
            dma((2, 2)), dma((2, 4)), dma((2, 4)), dma((3,)), dma((3,)), dma((6,)), dma((3, 6)),
            dma((2, 6)), dma((2, 4, 6)), dma((2, 2, 6)), dma((2, 4, 6)), dma((2, 4)), dma((4,)), dma((2, 4)), dma, dma, dma, dma((2, 2)),
        ],
        compiler_params=pltpu.CompilerParams(collective_id=1, has_side_effects=True, vmem_limit_bytes=67043328),
        name="mlp",
    )(x, dy, wg, wu, wd)[:2]


def place_kernel(dw, yo, y, dx, dg, du, dd, bw, by, bt, s_in, s_out):
    w_in = [pltpu.make_async_copy(dw.at[k], bw.at[k], s_in.at[k]) for k in range(3)]
    y_in = [pltpu.make_async_copy(yo.at[k], by.at[k], s_in.at[3 + k]) for k in range(2)]
    for l in w_in + y_in:
        l.start()
    outs = [pltpu.make_async_copy(bw.at[1], dg, s_out.at[1]), pltpu.make_async_copy(bw.at[2], du, s_out.at[2]),
            pltpu.make_async_copy(by.at[0], y, s_out.at[3]), pltpu.make_async_copy(by.at[1], dx, s_out.at[4])]
    w_in[0].wait()
    for h in range(2):
        bt[:, pl.ds(256 * h, 256)] = bw[0, pl.ds(256 * h, 256), :].T
    o = pltpu.make_async_copy(bt, dd, s_out.at[0])
    o.start()
    for l, e in zip(w_in[1:] + y_in, outs):
        l.wait()
        e.start()
    for e in [o] + outs:
        e.wait()


def place(dw, yo):
    sd = jax.ShapeDtypeStruct
    V = pltpu.VMEM
    return pl.pallas_call(
        place_kernel,
        out_shape=(sd((64, 4096), BF), sd((64, 4096), BF), sd((512, 896), F32), sd((512, 896), F32), sd((896, 512), F32)),
        in_specs=[HBM] * 2,
        out_specs=(HBM,) * 5,
        scratch_shapes=[V((3, 512, 896), F32), V((2, 64, 4096), BF), V((896, 512), F32),
                        pltpu.SemaphoreType.DMA((5,)), pltpu.SemaphoreType.DMA((5,))],
        compiler_params=pltpu.CompilerParams(vmem_limit_bytes=60 * 2**20),
        name="place",
    )(dw.reshape(3, 512, 896), yo)


def solution(mesh):
    rows = P(("dp", "tp"), None)
    wsp = P("dp", "tp")
    dsp = P("tp", "dp")

    def local(x, w_gate, w_up, w_down, dy):
        return place(*mlp(x, dy, w_gate, w_up, w_down))

    return jax.shard_map(local, mesh=mesh, in_specs=(rows, wsp, wsp, dsp, rows), out_specs=(rows, rows, wsp, wsp, dsp), check_vma=False)
```

```python
import jax
import jax.numpy as jnp
from jax import lax
from jax.experimental import pallas as pl
from jax.experimental.pallas import tpu as pltpu
from jax.sharding import PartitionSpec as P

MESH = pl.DeviceIdType.MESH
HBM = pl.BlockSpec(memory_space=pltpu.HBM)
NT = (((1,), (1,)), ((), ()))
TN = (((0,), (0,)), ((), ()))
F32 = jnp.float32
BF = jnp.bfloat16
TWO = range(2)
NSEND = 109
RING = 4
PAIR = 2
DM, TG, FB, CB, QB, RW, RH = 4096, 1024, 896, 512, 256, 64, 32
AX, AD = TWO
OWN, NEXT, OPP, PREV = range(4)
WG, WU, WL = range(3)
DOWN, GATE, UP = range(3)
Y0, Y1, X0, X1 = range(4)
B0, B1, B2, B3, B4, B5, B6, B7 = range(8)


def mlp_kernel(x_ref, dy_ref, wg_ref, wu_ref, wd_ref, dw, yo, xd, wgf, wuf, wdf, UV, XR, ZR, AP,
               B, A, XB, XS, WD, WX, ZB, ZS, Z2, US, res, ov,
               ssem, rsem, s_ld, s_put, s_c, s_a, s_ap, r_ap, s_b, r_b, s_xs, r_xs, s_zs, r_zs, s_2, r_2, s_w, s_xst, s_zst, s_xo, s_yo, s_uv, s_us):
    i = lax.axis_index("dp")
    j = lax.axis_index("tp")
    x, c, z, y = i // PAIR, i % PAIR, j // 4, j % RING
    xp, xm, xq, c1 = (x + 1) % RING, (x + 3) % RING, (x + 2) % RING, 1 - c
    dev = {
        "xp": {"dp": 2 * xp + c}, "xm": {"dp": 2 * xm + c}, "pc": {"dp": 2 * x + c1},
        "yp": {"tp": 4 * z + (y + 1) % RING}, "ym": {"tp": 4 * z + (y + 3) % RING},
        "zp": {"tp": 4 * ((z + 1) % RING) + y}, "zm": {"tp": 4 * ((z + 3) % RING) + y},
    }
    pos = ((z, y), (y, z))
    link = (("zp", "zm", "yp", "ym"), ("yp", "ym", "zp", "zm"))

    def remote(src, dst, ss, rs, to):
        return pltpu.make_async_remote_copy(src_ref=src, dst_ref=dst, send_sem=ss, recv_sem=rs, device_id=dev[to], device_id_type=MESH)

    def add(dst, src, n):
        def body(r, _):
            s = pl.ds(pl.multiple_of(r * RH, RH), RH)
            dst[s, :] = dst[s, :] + src[s, :]
            return 0
        lax.fori_loop(0, n // RH, body, 0)

    sends = []

    def send(src, dst, to):
        k = len(sends)
        r = remote(src, dst, ssem.at[k], rsem.at[k], to)
        r.start()
        sends.append(r)
        return r

    def wblk(k, xx, cc, half=None):
        ii = 2 * xx + cc
        if k < 2:
            r = (wgf, wuf)[k]
            if half is None:
                return r.at[pl.ds(pl.multiple_of(ii * CB, CB), CB), :]
            return r.at[pl.ds(pl.multiple_of(ii * CB + half * QB, QB), QB), :]
        if half is None:
            return wdf.at[ii]
        return wdf.at[ii, pl.ds(half * 448, 448), :]

    def rows(a, col, s, p, lo=0, n=RH):
        zz, yy = (p, s) if col == 0 else (s, p)
        return xd.at[a, pl.ds(pl.multiple_of((zz * 4 + yy) * RW + col * RH + lo, 16), n), :]

    GA = {}
    GA2 = {}
    GB = {}
    tail = {0: [], 1: []}

    def geo(col):
        sec, prim = pos[col]
        sp, sm, pp, pm = link[col]
        return prim, sec, pp, pm, sp, sm

    seen = set()

    def once(m):
        if id(m) not in seen:
            seen.add(id(m))
            m.wait_recv()

    def ga(a):
        for col in TWO:
            p, s, pp, pm, sp, sm = geo(col)
            src = res.at[a, pl.ds(col * RH, RH), :]
            GA[a, col] = [send(src, rows(a, col, p, s), to) for to in (pp, pm)]

    def gb0(a):
        for col in TWO:
            p, s, pp, pm, sp, sm = geo(col)
            src = res.at[a, pl.ds(col * RH, RH), :]
            GB[a, col, 0] = [send(src, rows(a, col, p, s), to) for to in (sp, sm)]

    def ga2(a):
        for col in TWO:
            p, s, pp, pm, sp, sm = geo(col)
            GA2[a, col] = []
            for fr, d, lo, fw in ((0, 3, 0, pp), (1, 1, 16, pm)):
                once(GA[a, col][fr])
                r = rows(a, col, (p + d) % RING, s, lo, 16)
                GA2[a, col].append(send(r, r, fw))

    def gb31(a):
        for col in TWO:
            p, s, pp, pm, sp, sm = geo(col)
            for d in (3, 1):
                r = rows(a, col, (p + d) % RING, s)
                GB[a, col, d] = [send(r, r, to) for to in (sp, sm)]

    def gb2(a):
        for col in TWO:
            p, s, pp, pm, sp, sm = geo(col)
            for m in GA2[a, col]:
                once(m)
            r = rows(a, col, (p + 2) % RING, s)
            GB[a, col, 2] = [send(r, r, to) for to in (sp, sm)]

    def gf(a, d):
        for col in TWO:
            p, s, pp, pm, sp, sm = geo(col)
            q = (p + d) % RING
            for fr, e, lo, fw in ((0, 3, 0, sp), (1, 1, 16, sm)):
                once(GB[a, col, d][fr])
                r = rows(a, col, q, (s + e) % RING, lo, 16)
                tail[a].append(send(r, r, fw))

    def gend(a):
        if a == 0:
            put.wait()
        for m in tail[a]:
            once(m)
        for idx in range(4):
            ap(a, idx).start()

    W1 = {}
    W2 = {}
    WP = {}
    w_in = (wg_ref, wu_ref, wd_ref)

    def wpc(k):
        WP[k, 0] = [send(w_in[k], wblk(k, x, c), "pc")]

    def wown(k):
        if k < WL:
            W1[k] = [[send(w_in[k], wblk(k, x, c), to)] for to in ("xp", "xm")]
        else:
            W1[k] = [[], []]
            for first in TWO:
                for fr, to in enumerate(("xp", "xm")):
                    half = (fr + first) % PAIR
                    W1[k][fr].append(send(wd_ref.at[pl.ds(half * 448, 448), :], wblk(k, x, c, half), to))

    def wf(k):
        W2[k] = []
        for fr, xx, d, half, fw in ((0, xm, 3, 0, "xp"), (1, xp, 1, 1, "xm")):
            once(W1[k][fr][0])
            r = wblk(k, xx, c, half)
            W2[k].append(send(r, r, fw))
            if k < 2:
                r = wblk(k, xx, c)
                WP[k, d] = [send(r, r, "pc")]

    def wfp():
        for fr, xx, d in ((0, xm, 3), (1, xp, 1)):
            once(W1[2][fr][1])
            r = wblk(2, xx, c)
            WP[2, d] = [send(r, r, "pc")]

    def wf2(k):
        WP[k, 2] = []
        for half in TWO:
            once(W2[k][half])
            r = wblk(k, xq, c, half)
            WP[k, 2].append(send(r, r, "pc"))

    def have(k, d, o):
        if o == 1:
            for m in WP[k, d]:
                once(m)
        elif d == 2:
            for m in W2[k]:
                once(m)
        elif d:
            for m in W1[k][d == NEXT]:
                once(m)

    xpos = {0: x, 1: xp, 2: xq, 3: xm}
    order = ((0, 0), (0, 1), (3, 0), (1, 0), (3, 1), (1, 1), (2, 0), (2, 1))

    def blk(t):
        d, o = order[t]
        return 2 * xpos[d] + (c if o == 0 else c1)

    def a_slot(t):
        s = t % RING
        return A.at[s // PAIR, s % PAIR]

    def ld_ab(t):
        d, o = order[t]
        s = t % RING
        ii = blk(t)
        out = [pltpu.make_async_copy(xd.at[0, :, pl.ds(pl.multiple_of(ii * CB, CB), CB)], a_slot(t), s_c.at[s, 0])]
        for k in TWO:
            src = w_in[k] if t == 0 else wblk(k, xpos[d], c if o == 0 else c1)
            out.append(pltpu.make_async_copy(src, WX.at[s % PAIR, k, pl.ds((s // PAIR) * CB, CB), :], s_c.at[s, 1 + k]))
        return out

    def sab(t):
        for k in TWO:
            have(k, *order[t])
        for l in ld_ab(t):
            l.start()

    def ab(t):
        for l in ld_ab(t):
            l.wait()
        s = t % RING

        def body(m, _):
            r = pl.ds(pl.multiple_of(m * QB, QB), QB)
            lhs = A[s // PAIR, s % PAIR, r, :]
            for k in TWO:
                v = jnp.dot(lhs, WX[s % PAIR, k, pl.ds((s // PAIR) * CB, CB), :], preferred_element_type=F32)
                if t == 0:
                    XB[2 * k + m // PAIR, m % PAIR] = v
                else:
                    XB[2 * k + m // PAIR, m % PAIR] += v
            return 0
        lax.fori_loop(0, 4, body, 0)

    def hp():
        def body(q, _):
            m = q // 8
            r = pl.ds(pl.multiple_of((q % 8) * RH, RH), RH)
            a = XB[m // PAIR, m % PAIR, r, :]
            b = XB[2 + m // PAIR, m % PAIR, r, :]
            sig = jax.nn.sigmoid(a)
            sa = a * sig
            XB[m // PAIR, m % PAIR, r, :] = b * sig * (1.0 + a * (1.0 - sig))
            XB[2 + m // PAIR, m % PAIR, r, :] = sa
            B[0, 0, pl.ds(pl.multiple_of(q * RH, RH), RH), :] = (sa * b).astype(BF)
            return 0
        lax.fori_loop(0, RH, body, 0)
        bp[0].start()
        uv_put.start()

    uv_put = pltpu.make_async_copy(XB, UV, s_uv)

    def ld_g(t):
        d, o = order[t]
        s = t % RING
        ii = blk(t)
        src = wd_ref if t == 0 else wdf.at[ii]
        return [pltpu.make_async_copy(xd.at[1, :, pl.ds(pl.multiple_of(ii * CB, CB), CB)], a_slot(t), s_c.at[s, 0]),
                pltpu.make_async_copy(src, WX.at[s % PAIR, s // PAIR, pl.ds(0, FB), pl.ds(0, CB)], s_c.at[s, 1])]

    def sg(t):
        have(2, *order[t])
        for l in ld_g(t):
            l.start()

    def gg(t):
        for l in ld_g(t):
            l.wait()
        s = t % RING

        def body(m, _):
            r = pl.ds(pl.multiple_of(m * QB, QB), QB)
            v = lax.dot_general(A[s // PAIR, s % PAIR, r, :], WX[s % PAIR, s // PAIR, pl.ds(0, FB), pl.ds(0, CB)], NT, preferred_element_type=F32)
            if t == 0:
                XS[m] = v
            else:
                XS[m] += v
            return 0
        lax.fori_loop(0, 4, body, 0)

    def us_load(q, k):
        m = q // PAIR
        return pltpu.make_async_copy(UV.at[2 * k + m // PAIR, m % PAIR, pl.ds(pl.multiple_of((q % PAIR) * 128, 128), 128), :], US.at[q % PAIR, k], s_us.at[q % PAIR, k])

    def dadb():
        for k in TWO:
            us_load(0, k).start()

        def body(q, _):
            @pl.when(q < 7)
            def _():
                for k in TWO:
                    us_load(q + 1, k).start()
            for k in TWO:
                us_load(q, k).wait()

            def inner(e, _):
                r = pl.ds(pl.multiple_of(e * RH, RH), RH)
                g = XS[q // PAIR, pl.ds(pl.multiple_of((q % PAIR) * 128 + e * RH, RH), RH), :]
                o = pl.ds(pl.multiple_of(q * 128 + e * RH, RH), RH)
                for k in TWO:
                    B[1 + k, 0, o, :] = (g * US[q % PAIR, k, r, :]).astype(BF)
                return 0
            lax.fori_loop(0, 4, inner, 0)
            return 0
        lax.fori_loop(0, 8, body, 0)
        bp[1].start()
        bp[2].start()

    def chunk(idx):
        return (x + 6 - idx) % RING

    bp = [remote(B.at[k, 0], B.at[k, 1], s_b.at[k], r_b.at[k], "pc") for k in range(3)]

    APM = {}

    def ap(arr, idx):
        if (arr, idx) not in APM:
            APM[arr, idx] = ap_(arr, idx)
        return APM[arr, idx]

    def ap_(arr, idx):
        return remote(xd.at[arr, :, pl.ds(pl.multiple_of(TG * chunk(idx) + CB * c1, CB), CB)], AP.at[arr, idx], s_ap.at[arr, idx], r_ap.at[arr, idx], "pc")

    seq = (0, 1, 3, 2)

    def load_a(k, n):
        arr = 1 - min(k, 1)
        idx = seq[n]
        return (pltpu.make_async_copy(xd.at[arr, :, pl.ds(pl.multiple_of(TG * chunk(idx) + CB * c, CB), CB)], A.at[n % PAIR, 0], s_a.at[n % PAIR, 0]),
                pltpu.make_async_copy(AP.at[arr, idx], A.at[n % PAIR, 1], s_a.at[n % PAIR, 1]))

    def start_a(k, n):
        once(ap(1 - min(k, 1), seq[n]))
        for l in load_a(k, n):
            l.start()

    def dot_x(k, n, split=False):
        slot = n % PAIR
        for l in load_a(k, n):
            l.wait()

        def body(m, _):
            cols = pl.ds(pl.multiple_of(m * QB, QB), QB)
            XB[seq[n], m] = (lax.dot_general(A[slot, 0, :, cols], B[k, 0], TN, preferred_element_type=F32)
                             + lax.dot_general(A[slot, 1, :, cols], B[k, 1], TN, preferred_element_type=F32))
            return 0

        if split:
            for m in TWO:
                body(m, 0)
                xmsg(k, m).start()
        else:
            lax.fori_loop(0, 2, body, 0)

    def xmsg(k, t):
        src = (XB.at[0, 0], XB.at[0, 1], XB.at[1, 1], XB.at[3, 0], XB.at[1, 0], XB.at[3, 1])[t]
        return remote(src, XR.at[k, t], s_xs.at[t], r_xs.at[k, t], ("xp", "xm")[t % PAIR])

    def xl0(k):
        start_a(k, 0)
        start_a(k, 1)

    def x1(k):
        bp[k].wait_recv()
        if k == 0:
            uv_put.wait()
        else:
            xmsg(k - 1, 0).wait_send()
            xmsg(k - 1, 1).wait_send()
        dot_x(k, 0, True)
        start_a(k, 2)

    def x2(k):
        if k > 0:
            for t in range(2, 6):
                xmsg(k - 1, t).wait_send()
        dot_x(k, 1)
        start_a(k, 3)
        xmsg(k, 2).start()
        dot_x(k, 2)
        if k == 1:
            start_a(2, 0)
        xmsg(k, 3).start()

    def x2o(k):
        if k > 0:
            xout(k - 1).wait()
        dot_x(k, 3)
        if k == 1:
            start_a(2, 1)

    def xstage(k, t, slot):
        return pltpu.make_async_copy(XR.at[k, t], XS.at[4 + slot], s_xst.at[slot])

    def x3(k):
        for t in TWO:
            xmsg(k, t).wait_recv()
            xstage(k, t, t).start()
        for t in TWO:
            xstage(k, t, t).wait()
            add(XB.at[(1, 3)[t], t], XS.at[4 + t], QB)
            xmsg(k, 4 + t).start()

    def xout(k):
        return pltpu.make_async_copy(XB.at[2], dw.at[k], s_xo)

    def xadd(k, ts):
        for h, t in enumerate(ts):
            xmsg(k, t).wait_recv()
            xstage(k, t, h).start()
        for h, t in enumerate(ts):
            xstage(k, t, h).wait()
            add(XB.at[2, h], XS.at[4 + h], QB)

    def xfa(k):
        xadd(k, (3, 2))
        if k == 2:
            xout(k).start()

    def xfb(k):
        xadd(k, (4, 5))
        xout(k).start()

    def pair(n, col):
        return ((0, 3), (1, 2))[col][n % PAIR]

    def lw(n):
        if n < 2:
            for col in TWO:
                have(2, pair(n, col), 0)
                have(2, pair(n, col), 1)
        out = []
        for col in TWO:
            d = pair(n, col)
            q = xpos[d]
            if n < 2:
                if d == 0:
                    out.append(pltpu.make_async_copy(wd_ref, WD.at[col, c], s_w.at[col, 0]))
                    out.append(pltpu.make_async_copy(wdf.at[2 * x + c1], WD.at[col, c1], s_w.at[col, 1]))
                else:
                    out.append(pltpu.make_async_copy(wdf.at[pl.ds(2 * q, 2)], WD.at[col], s_w.at[col, 0]))
            else:
                for k in TWO:
                    full = (wgf, wuf)[k]
                    if d == 0:
                        out.append(pltpu.make_async_copy(w_in[k], WX.at[col, k, pl.ds(pl.multiple_of(CB * c, CB), CB), :], s_w.at[col, 2 * k]))
                        out.append(pltpu.make_async_copy(full.at[pl.ds(pl.multiple_of(TG * x + CB * c1, CB), CB), :],
                                                         WX.at[col, k, pl.ds(pl.multiple_of(CB * c1, CB), CB), :], s_w.at[col, 2 * k + 1]))
                    else:
                        out.append(pltpu.make_async_copy(full.at[pl.ds(pl.multiple_of(TG * q, TG), TG), :], WX.at[col, k], s_w.at[col, 2 * k]))
        for o in out:
            o.start()
        wl[n] = out

    wl = {}

    def dots_z(n, lo, m):

        def body(q, _):
            col = q // m
            idx = lo + 2 * (q % m)
            p = z + col * (y - z)
            ch = (p + 6 - idx) % RING
            s1 = QB - 192 * col
            s2 = RW + 192 * col
            own = (idx // PAIR) * (1 - idx // 3)
            slot = idx + own * 2 * (n % PAIR)

            def lhs(k):
                return jnp.concatenate([B[k, 0, pl.ds(pl.multiple_of(ch * s1 + g * s2, RW), RW), :] for g in range(4)], axis=0)

            if n < 2:
                l = lhs(0)
                for h in TWO:
                    ZB[col, slot, h] = jnp.dot(l, WD[col, h], preferred_element_type=F32)
            else:
                l = lhs(1)
                u = lhs(2)
                for h in TWO:
                    r = pl.ds(CB * h, CB)
                    ZB[col, slot, h] = (lax.dot_general(l, WX[col, 0, r, :], NT, preferred_element_type=F32)
                                        + lax.dot_general(u, WX[col, 1, r, :], NT, preferred_element_type=F32))
            return 0
        lax.fori_loop(0, 2 * m, body, 0)

    def zmsg(n, col, t):
        src = ((0, 0), (0, 1), (1, 1), (3, 0), (1, 0), (3, 1))[t]
        return remote(ZB.at[col, src[0], src[1]], ZR.at[col, n, t], s_zs.at[col, t], r_zs.at[col, n, t], link[col][t % PAIR])

    def own(n, col, h):
        return ZB.at[col, 2 + 2 * (n % PAIR), h]

    def sub(n, col, h, d):
        s = (pos[col][1] + d) % RING
        return ZB.at[col, 2 + 2 * (n % PAIR), h, pl.ds(pl.multiple_of(s * RW, RW), RW), :]

    def msg2(n, col, t):
        h, d = ((0, 2), (1, 2), (1, 1), (0, 3), (0, 1), (1, 3))[t]
        return remote(sub(n, col, h, d), Z2.at[col, n, t], s_2.at[col, n % PAIR, t], r_2.at[col, n, t], link[col][2 + t % PAIR])

    def p1(n):
        for l in wl[n]:
            l.wait()
        if n > 0:
            for col in TWO:
                for t in TWO:
                    zmsg(n - 1, col, t).wait_send()
        dots_z(n, 0, 1)
        for t in TWO:
            for col in TWO:
                zmsg(n, col, t).start()

    def p2(n):
        if n > 0:
            for col in TWO:
                for t in range(2, 6):
                    zmsg(n - 1, col, t).wait_send()
        dots_z(n, 1, 2)
        for t in range(2, 4):
            for col in TWO:
                zmsg(n, col, t).start()

    def p2o(n):
        if n > 1:
            for col in TWO:
                for t in range(6):
                    msg2(n - 2, col, t).wait_send()
        dots_z(n, 2, 1)

    def zstage(n, col, t, slot):
        return pltpu.make_async_copy(ZR.at[col, n, t], ZS.at[col, slot], s_zst.at[col, slot])

    def p4(n):
        for t in TWO:
            for col in TWO:
                zmsg(n, col, t).wait_recv()
                zstage(n, col, t, t).start()
        for t in TWO:
            for col in TWO:
                zstage(n, col, t, t).wait()
                add(ZB.at[col, (1, 3)[t], t], ZS.at[col, t], QB)
                zmsg(n, col, 4 + t).start()

    def zadd(n, ts):
        for h, t in enumerate(ts):
            for col in TWO:
                zmsg(n, col, t).wait_recv()
                zstage(n, col, t, h).start()
        for h, t in enumerate(ts):
            for col in TWO:
                zstage(n, col, t, h).wait()
                add(own(n, col, h), ZS.at[col, h], QB)

    def fa(n):
        zadd(n, (3, 2))

    def fb(n):
        zadd(n, (4, 5))
        for t in range(4):
            for col in TWO:
                msg2(n, col, t).start()

    def hh(n):
        for t in TWO:
            for col in TWO:
                msg2(n, col, t).wait_recv()
                add(sub(n, col, t, (1, 3)[t]), Z2.at[col, n, t], RW)
                msg2(n, col, 4 + t).start()

    def zf(n):
        a = n // PAIR
        for col in TWO:
            q = xpos[pair(n, col)]
            for h, ts in ((0, (3, 4)), (1, (2, 5))):
                for t in ts:
                    msg2(n, col, t).wait_recv()
                cs = pl.ds(pl.multiple_of(TG * q + CB * h, CB), CB)
                v = sub(n, col, h, 0)[...] + Z2[col, n, ts[0]] + Z2[col, n, ts[1]]
                ov[a, :, cs] = (res[a, :, cs].astype(F32) + v).astype(BF)
        if n == 3:
            out.start()

    own_ld = [pltpu.make_async_copy(r, res.at[k], s_ld.at[k]) for k, r in enumerate((x_ref, dy_ref))]
    for l in own_ld:
        l.start()
    barrier = pltpu.get_barrier_semaphore()
    for d in dev.values():
        pl.semaphore_signal(barrier, inc=1, device_id=d, device_id_type=MESH)
    pl.semaphore_wait(barrier, len(dev))
    own_ld[0].wait()
    own_ld[1].wait()
    put = pltpu.make_async_copy(res, xd.at[:, pl.ds(pl.multiple_of(j * RW, RW), RW), :], s_put)
    put.start()
    out = pltpu.make_async_copy(ov, yo, s_yo)
    gb0(AX)
    ga(AX)
    wown(WU)
    wpc(WG)
    gf(AX, OWN)
    ga2(AX)
    gb31(AX)
    wown(WG)
    gb2(AX)
    gf(AX, PREV)
    gf(AX, NEXT)
    gf(AX, OPP)
    ga(AD)
    wf(WU)
    gb0(AD)
    wpc(WU)
    gend(AX)
    wf(WG)
    sab(B0)
    sab(B1)
    sab(B3)
    ga2(AD)
    ab(B0)
    gb31(AD)
    gf(AD, OWN)
    wf2(WU)
    sab(B2)
    ab(B1)
    gb2(AD)
    wown(WL)
    sab(B4)
    ab(B2)
    sab(B5)
    ab(B3)
    wf2(WG)
    ab(B4)
    sab(B6)
    ab(B5)
    gf(AD, NEXT)
    gf(AD, PREV)
    sab(B7)
    ab(B6)
    wpc(WL)
    ab(B7)
    hp()
    wf(WL)
    gf(AD, OPP)
    wfp()
    gend(AD)
    xl0(DOWN)
    lw(Y0)
    x1(DOWN)
    x2(DOWN)
    p1(Y0)
    p2(Y0)
    x2o(DOWN)
    wf2(WL)
    sg(B3)
    sg(B2)
    sg(B1)
    sg(B0)
    p2o(Y0)
    lw(Y1)
    gg(B0)
    gg(B1)
    p4(Y0)
    sg(B5)
    gg(B2)
    sg(B6)
    gg(B3)
    sg(B4)
    sg(B7)
    x3(DOWN)
    gg(B4)
    gg(B5)
    gg(B6)
    gg(B7)
    p1(Y1)
    dadb()
    xl0(GATE)
    p2(Y1)
    x1(GATE)
    fa(Y0)
    p2o(Y1)
    lw(X0)
    p4(Y1)
    fb(Y0)
    p1(X0)
    x2(GATE)
    fa(Y1)
    xfa(DOWN)
    x3(GATE)
    hh(Y0)
    fb(Y1)
    xfb(DOWN)
    p2(X0)
    zf(Y0)
    hh(Y1)
    x2o(GATE)
    p2o(X0)
    p4(X0)
    lw(X1)
    xfa(GATE)
    x1(UP)
    zf(Y1)
    p1(X1)
    fa(X0)
    x2(UP)
    p2(X1)
    xfb(GATE)
    p4(X1)
    fb(X0)
    p2o(X1)
    x3(UP)
    x2o(UP)
    fa(X1)
    fb(X1)
    hh(X0)
    hh(X1)
    xfa(UP)
    zf(X0)
    zf(X1)
    for r in sends:
        r.wait_send()
    for t in range(4, 6):
        xmsg(2, t).wait_recv()
    for t in range(6):
        xmsg(2, t).wait_send()
        for col in TWO:
            zmsg(3, col, t).wait_send()
            msg2(2, col, t).wait_send()
            msg2(3, col, t).wait_send()
    for k in range(3):
        bp[k].wait_send()
    for arr in TWO:
        for idx in range(4):
            ap(arr, idx).wait_send()
    xout(2).wait()
    out.wait()


def mlp(x, dy, wg, wu, wd):
    sd = jax.ShapeDtypeStruct
    dma = pltpu.SemaphoreType.DMA
    V = pltpu.VMEM
    o = pl.pallas_call(
        mlp_kernel,
        out_shape=(sd((3, 2, QB, FB), F32), sd((2, RW, DM), BF),
                   sd((2, TG, DM), BF), sd((DM, FB), BF), sd((DM, FB), BF), sd((8, FB, CB), BF), sd((4, 2, QB, FB), F32),
                   sd((3, 6, QB, FB), F32), sd((2, 4, 6, QB, CB), F32), sd((2, 4, TG, CB), BF)),
        in_specs=[HBM] * 5,
        out_specs=(HBM,) * 10,
        scratch_shapes=[
            V((3, 2, TG, FB), BF), V((2, 2, TG, CB), BF), V((4, 2, QB, FB), F32), V((6, QB, FB), F32),
            V((2, 2, FB, CB), BF), V((2, 2, TG, FB), BF), V((2, 5, 2, QB, CB), F32), V((2, 2, QB, CB), F32),
            V((2, 4, 6, RW, CB), F32), V((2, 2, 128, FB), F32), V((2, RW, DM), BF), V((2, RW, DM), BF),
            dma((NSEND,)), dma((NSEND,)), dma((2,)), dma, dma((4, 3)),
            dma((2, 2)), dma((2, 4)), dma((2, 4)), dma((3,)), dma((3,)), dma((6,)), dma((3, 6)),
            dma((2, 6)), dma((2, 4, 6)), dma((2, 2, 6)), dma((2, 4, 6)), dma((2, 4)), dma((4,)), dma((2, 4)), dma, dma, dma, dma((2, 2)),
        ],
        compiler_params=pltpu.CompilerParams(collective_id=1, has_side_effects=True, vmem_limit_bytes=67043328),
        name="mlp",
    )(x, dy, wg, wu, wd)
    return o[0], o[1], o[7]


def place_kernel(dw, yo, xr, y, dx, dg, du, dd, bw, by, bt, br, s_in, s_out):
    w_in = [pltpu.make_async_copy(dw.at[k], bw.at[k], s_in.at[k]) for k in range(3)]
    y_in = [pltpu.make_async_copy(yo.at[k], by.at[k], s_in.at[3 + k]) for k in TWO]
    r_in = pltpu.make_async_copy(xr.at[2, pl.ds(4, 2)], br, s_in.at[5])
    for l in w_in + [r_in] + y_in:
        l.start()
    w_out = [pltpu.make_async_copy(bt, dd, s_out.at[0]), pltpu.make_async_copy(bw.at[1], dg, s_out.at[1]), pltpu.make_async_copy(bw.at[2], du, s_out.at[2])]
    y_out = [pltpu.make_async_copy(by.at[0], y, s_out.at[3]), pltpu.make_async_copy(by.at[1], dx, s_out.at[4])]
    w_in[0].wait()
    for h in TWO:
        bt[:, pl.ds(QB * h, QB)] = bw[0, pl.ds(QB * h, QB), :].T
    w_out[0].start()
    w_in[1].wait()
    w_out[1].start()
    w_in[2].wait()
    r_in.wait()
    for h in TWO:
        bw[2, pl.ds(QB * h, QB), :] += br[h]
    w_out[2].start()
    for l, e in zip(y_in, y_out):
        l.wait()
        e.start()
    for e in w_out + y_out:
        e.wait()


def place(dw, yo, xr):
    sd = jax.ShapeDtypeStruct
    V = pltpu.VMEM
    return pl.pallas_call(
        place_kernel,
        out_shape=(sd((RW, DM), BF), sd((RW, DM), BF), sd((CB, FB), F32), sd((CB, FB), F32), sd((FB, CB), F32)),
        in_specs=[HBM] * 3,
        out_specs=(HBM,) * 5,
        scratch_shapes=[V((3, CB, FB), F32), V((2, RW, DM), BF), V((FB, CB), F32), V((2, QB, FB), F32),
                        pltpu.SemaphoreType.DMA((6,)), pltpu.SemaphoreType.DMA((5,))],
        compiler_params=pltpu.CompilerParams(vmem_limit_bytes=60 * 2**20),
        name="place",
    )(dw.reshape(3, CB, FB), yo, xr)


def solution(mesh):
    rows = P(("dp", "tp"), None)
    wsp = P("dp", "tp")
    dsp = P("tp", "dp")

    def local(x, w_gate, w_up, w_down, dy):
        return place(*mlp(x, dy, w_gate, w_up, w_down))

    return jax.shard_map(local, mesh=mesh, in_specs=(rows, wsp, wsp, dsp, rows), out_specs=(rows, rows, wsp, wsp, dsp), check_vma=False)
```

```python
import jax
import jax.numpy as jnp
from jax import lax
from jax.experimental import pallas as pl
from jax.experimental.pallas import tpu as pltpu
from jax.sharding import PartitionSpec as P

MESH = pl.DeviceIdType.MESH
HBM = pl.BlockSpec(memory_space=pltpu.HBM)
NT = (((1,), (1,)), ((), ()))
TN = (((0,), (0,)), ((), ()))
F32 = jnp.float32
BF = jnp.bfloat16
TWO = range(2)
NSEND = 149
RING = 4
PAIR = 2
DM, TG, FB, CB, QB, RW, RH = 4096, 1024, 896, 512, 256, 64, 32
AX, AD, AE = range(3)
OWN, NEXT, OPP, PREV = range(4)
WG, WU, WL = range(3)
DOWN, GATE, UP = range(3)
Y0, Y1, X0, X1 = range(4)
B0, B1, B2, B3, B4, B5, B6, B7 = range(8)


def mlp_kernel(x_ref, dy_ref, wg_ref, wu_ref, wd_ref, dw, yo, xd, wgf, wuf, wdf, UV, XR, ZR, AP,
               B, A, XB, XS, WD, WX, ZB, ZS, Z2, US, res, ov,
               ssem, rsem, s_ld, s_put, s_c, s_a, s_ap, r_ap, s_b, r_b, s_xs, r_xs, s_zs, r_zs, s_2, r_2, s_w, s_xst, s_zst, s_xo, s_yo, s_uv, s_us):
    i = lax.axis_index("dp")
    j = lax.axis_index("tp")
    x, c, z, y = i // PAIR, i % PAIR, j // 4, j % RING
    xp, xm, xq, c1 = (x + 1) % RING, (x + 3) % RING, (x + 2) % RING, 1 - c
    dev = {
        "xp": {"dp": 2 * xp + c}, "xm": {"dp": 2 * xm + c}, "pc": {"dp": 2 * x + c1},
        "yp": {"tp": 4 * z + (y + 1) % RING}, "ym": {"tp": 4 * z + (y + 3) % RING},
        "zp": {"tp": 4 * ((z + 1) % RING) + y}, "zm": {"tp": 4 * ((z + 3) % RING) + y},
    }
    pos = ((z, y), (y, z))
    link = (("zp", "zm", "yp", "ym"), ("yp", "ym", "zp", "zm"))

    def remote(src, dst, ss, rs, to):
        return pltpu.make_async_remote_copy(src_ref=src, dst_ref=dst, send_sem=ss, recv_sem=rs, device_id=dev[to], device_id_type=MESH)

    def add(dst, src, n):
        def body(r, _):
            s = pl.ds(pl.multiple_of(r * RH, RH), RH)
            dst[s, :] = dst[s, :] + src[s, :]
            return 0
        lax.fori_loop(0, n // RH, body, 0)

    sends = []

    def send(src, dst, to):
        k = len(sends)
        r = remote(src, dst, ssem.at[k], rsem.at[k], to)
        r.start()
        sends.append(r)
        return r

    def wblk(k, xx, cc, half=None):
        ii = 2 * xx + cc
        if k < 2:
            r = (wgf, wuf)[k]
            if half is None:
                return r.at[pl.ds(pl.multiple_of(ii * CB, CB), CB), :]
            return r.at[pl.ds(pl.multiple_of(ii * CB + half * QB, QB), QB), :]
        if half is None:
            return wdf.at[ii]
        return wdf.at[ii, pl.ds(half * 448, 448), :]

    ahead = xq // PAIR

    def cols(a):
        if a == AX:
            return slice(None)
        h = ahead if a == AD else 1 - ahead
        return pl.ds(pl.multiple_of(h * (DM // PAIR), DM // PAIR), DM // PAIR)

    def rows(a, col, s, p, lo=0, n=RH):
        zz, yy = (p, s) if col == 0 else (s, p)
        return xd.at[min(a, AD), pl.ds(pl.multiple_of((zz * 4 + yy) * RW + col * RH + lo, 16), n), cols(a)]

    GA = {}
    GA2 = {}
    GB = {}
    tail = ([], [], [])

    def geo(col):
        sec, prim = pos[col]
        sp, sm, pp, pm = link[col]
        return prim, sec, pp, pm, sp, sm

    seen = set()

    def once(m):
        if id(m) not in seen:
            seen.add(id(m))
            m.wait_recv()

    def ga(a):
        for col in TWO:
            p, s, pp, pm, sp, sm = geo(col)
            src = res.at[min(a, AD), pl.ds(col * RH, RH), cols(a)]
            GA[a, col] = [send(src, rows(a, col, p, s), to) for to in (pp, pm)]

    def gb0(a):
        for col in TWO:
            p, s, pp, pm, sp, sm = geo(col)
            src = res.at[min(a, AD), pl.ds(col * RH, RH), cols(a)]
            GB[a, col, 0] = [send(src, rows(a, col, p, s), to) for to in (sp, sm)]

    def ga2(a):
        for col in TWO:
            p, s, pp, pm, sp, sm = geo(col)
            GA2[a, col] = []
            for fr, d, lo, fw in ((0, 3, 0, pp), (1, 1, 16, pm)):
                once(GA[a, col][fr])
                r = rows(a, col, (p + d) % RING, s, lo, 16)
                GA2[a, col].append(send(r, r, fw))

    def gb31(a):
        for col in TWO:
            p, s, pp, pm, sp, sm = geo(col)
            for d in (3, 1):
                r = rows(a, col, (p + d) % RING, s)
                GB[a, col, d] = [send(r, r, to) for to in (sp, sm)]

    def gb2(a):
        for col in TWO:
            p, s, pp, pm, sp, sm = geo(col)
            for m in GA2[a, col]:
                once(m)
            r = rows(a, col, (p + 2) % RING, s)
            GB[a, col, 2] = [send(r, r, to) for to in (sp, sm)]

    def gf(a, d):
        for col in TWO:
            p, s, pp, pm, sp, sm = geo(col)
            q = (p + d) % RING
            for fr, e, lo, fw in ((0, 3, 0, sp), (1, 1, 16, sm)):
                once(GB[a, col, d][fr])
                r = rows(a, col, q, (s + e) % RING, lo, 16)
                tail[a].append(send(r, r, fw))

    def gend(a):
        if a == 0:
            put.wait()
        for m in tail[a]:
            once(m)
        for arr, idx in (((AX, 0), (AX, 1), (AX, 3), (AX, 2)), ((AD, 0),), ((AD, 1), (AD, 3), (AD, 2)))[a]:
            ap(arr, idx).start()

    W1 = {}
    W2 = {}
    WP = {}
    w_in = (wg_ref, wu_ref, wd_ref)

    def wpc(k):
        WP[k, 0] = [send(w_in[k], wblk(k, x, c), "pc")]

    def wown(k):
        if k < WL:
            W1[k] = [[send(w_in[k], wblk(k, x, c), to)] for to in ("xp", "xm")]
        else:
            W1[k] = [[], []]
            for first in TWO:
                for fr, to in enumerate(("xp", "xm")):
                    half = (fr + first) % PAIR
                    W1[k][fr].append(send(wd_ref.at[pl.ds(half * 448, 448), :], wblk(k, x, c, half), to))

    def wf(k):
        W2[k] = []
        for fr, xx, d, half, fw in ((0, xm, 3, 0, "xp"), (1, xp, 1, 1, "xm")):
            once(W1[k][fr][0])
            r = wblk(k, xx, c, half)
            W2[k].append(send(r, r, fw))
            if k < 2:
                r = wblk(k, xx, c)
                WP[k, d] = [send(r, r, "pc")]

    def wfp():
        for fr, xx, d in ((0, xm, 3), (1, xp, 1)):
            once(W1[2][fr][1])
            r = wblk(2, xx, c)
            WP[2, d] = [send(r, r, "pc")]

    def wf2(k):
        WP[k, 2] = []
        for half in TWO:
            once(W2[k][half])
            r = wblk(k, xq, c, half)
            WP[k, 2].append(send(r, r, "pc"))

    def have(k, d, o):
        if o == 1:
            for m in WP[k, d]:
                once(m)
        elif d == 2:
            for m in W2[k]:
                once(m)
        elif d:
            for m in W1[k][d == NEXT]:
                once(m)

    xpos = {0: x, 1: xp, 2: xq, 3: xm}
    order = ((0, 0), (0, 1), (3, 0), (1, 0), (3, 1), (1, 1), (2, 0), (2, 1))

    def blk(t):
        d, o = order[t]
        return 2 * xpos[d] + (c if o == 0 else c1)

    def a_slot(t):
        s = t % RING
        return A.at[s // PAIR, s % PAIR]

    def ld_ab(t):
        d, o = order[t]
        s = t % RING
        ii = blk(t)
        out = [pltpu.make_async_copy(xd.at[0, :, pl.ds(pl.multiple_of(ii * CB, CB), CB)], a_slot(t), s_c.at[s, 0])]
        for k in TWO:
            src = w_in[k] if t == 0 else wblk(k, xpos[d], c if o == 0 else c1)
            out.append(pltpu.make_async_copy(src, WX.at[s % PAIR, k, pl.ds((s // PAIR) * CB, CB), :], s_c.at[s, 1 + k]))
        return out

    def sab(t):
        for k in TWO:
            have(k, *order[t])
        for l in ld_ab(t):
            l.start()

    def ab(t):
        for l in ld_ab(t):
            l.wait()
        s = t % RING

        def body(m, _):
            r = pl.ds(pl.multiple_of(m * QB, QB), QB)
            lhs = A[s // PAIR, s % PAIR, r, :]
            for k in TWO:
                v = jnp.dot(lhs, WX[s % PAIR, k, pl.ds((s // PAIR) * CB, CB), :], preferred_element_type=F32)
                if t == 0:
                    XB[2 * k + m // PAIR, m % PAIR] = v
                else:
                    XB[2 * k + m // PAIR, m % PAIR] += v
            return 0
        lax.fori_loop(0, 4, body, 0)

    def hp():
        def body(q, _):
            m = q // 8
            r = pl.ds(pl.multiple_of((q % 8) * RH, RH), RH)
            a = XB[m // PAIR, m % PAIR, r, :]
            b = XB[2 + m // PAIR, m % PAIR, r, :]
            sig = jax.nn.sigmoid(a)
            sa = a * sig
            XB[m // PAIR, m % PAIR, r, :] = b * sig * (1.0 + a * (1.0 - sig))
            XB[2 + m // PAIR, m % PAIR, r, :] = sa
            B[0, 0, pl.ds(pl.multiple_of(q * RH, RH), RH), :] = (sa * b).astype(BF)
            return 0
        lax.fori_loop(0, RH, body, 0)
        bp[0].start()
        uv_put.start()

    uv_put = pltpu.make_async_copy(XB, UV, s_uv)

    def ld_g(t):
        d, o = order[t]
        s = t % RING
        ii = blk(t)
        src = wd_ref if t == 0 else wdf.at[ii]
        return [pltpu.make_async_copy(xd.at[1, :, pl.ds(pl.multiple_of(ii * CB, CB), CB)], a_slot(t), s_c.at[s, 0]),
                pltpu.make_async_copy(src, WX.at[s % PAIR, s // PAIR, pl.ds(0, FB), pl.ds(0, CB)], s_c.at[s, 1])]

    def sg(t):
        have(2, *order[t])
        for l in ld_g(t):
            l.start()

    def gg(t):
        for l in ld_g(t):
            l.wait()
        s = t % RING

        def body(m, _):
            r = pl.ds(pl.multiple_of(m * QB, QB), QB)
            v = lax.dot_general(A[s // PAIR, s % PAIR, r, :], WX[s % PAIR, s // PAIR, pl.ds(0, FB), pl.ds(0, CB)], NT, preferred_element_type=F32)
            if t == 0:
                XS[m] = v
            else:
                XS[m] += v
            return 0
        lax.fori_loop(0, 4, body, 0)

    def us_load(q, k):
        m = q // PAIR
        return pltpu.make_async_copy(UV.at[2 * k + m // PAIR, m % PAIR, pl.ds(pl.multiple_of((q % PAIR) * 128, 128), 128), :], US.at[q % PAIR, k], s_us.at[q % PAIR, k])

    def dadb():
        for k in TWO:
            us_load(0, k).start()

        def body(q, _):
            @pl.when(q < 7)
            def _():
                for k in TWO:
                    us_load(q + 1, k).start()
            for k in TWO:
                us_load(q, k).wait()

            def inner(e, _):
                r = pl.ds(pl.multiple_of(e * RH, RH), RH)
                g = XS[q // PAIR, pl.ds(pl.multiple_of((q % PAIR) * 128 + e * RH, RH), RH), :]
                o = pl.ds(pl.multiple_of(q * 128 + e * RH, RH), RH)
                for k in TWO:
                    B[1 + k, 0, o, :] = (g * US[q % PAIR, k, r, :]).astype(BF)
                return 0
            lax.fori_loop(0, 4, inner, 0)
            return 0
        lax.fori_loop(0, 8, body, 0)
        bp[1].start()
        bp[2].start()

    def chunk(idx):
        return (x + 6 - idx) % RING

    bp = [remote(B.at[k, 0], B.at[k, 1], s_b.at[k], r_b.at[k], "pc") for k in range(3)]

    APM = {}

    def ap(arr, idx):
        if (arr, idx) not in APM:
            APM[arr, idx] = ap_(arr, idx)
        return APM[arr, idx]

    def ap_(arr, idx):
        return remote(xd.at[arr, :, pl.ds(pl.multiple_of(TG * chunk(idx) + CB * c1, CB), CB)], AP.at[arr, idx], s_ap.at[arr, idx], r_ap.at[arr, idx], "pc")

    seq = (0, 1, 3, 2)

    def load_a(k, n):
        arr = 1 - min(k, 1)
        idx = seq[n]
        return (pltpu.make_async_copy(xd.at[arr, :, pl.ds(pl.multiple_of(TG * chunk(idx) + CB * c, CB), CB)], A.at[n % PAIR, 0], s_a.at[n % PAIR, 0]),
                pltpu.make_async_copy(AP.at[arr, idx], A.at[n % PAIR, 1], s_a.at[n % PAIR, 1]))

    def start_a(k, n):
        once(ap(1 - min(k, 1), seq[n]))
        for l in load_a(k, n):
            l.start()

    def dot_x(k, n, split=False):
        slot = n % PAIR
        for l in load_a(k, n):
            l.wait()

        def body(m, _):
            cols = pl.ds(pl.multiple_of(m * QB, QB), QB)
            XB[seq[n], m] = (lax.dot_general(A[slot, 0, :, cols], B[k, 0], TN, preferred_element_type=F32)
                             + lax.dot_general(A[slot, 1, :, cols], B[k, 1], TN, preferred_element_type=F32))
            return 0

        if split:
            for m in TWO:
                body(m, 0)
                xmsg(k, m).start()
        else:
            lax.fori_loop(0, 2, body, 0)

    def xmsg(k, t):
        src = (XB.at[0, 0], XB.at[0, 1], XB.at[1, 1], XB.at[3, 0], XB.at[1, 0], XB.at[3, 1])[t]
        return remote(src, XR.at[k, t], s_xs.at[t], r_xs.at[k, t], ("xp", "xm")[t % PAIR])

    def xl(k, n):
        start_a(k, n)

    def x1(k):
        bp[k].wait_recv()
        if k == 0:
            uv_put.wait()
        else:
            xmsg(k - 1, 0).wait_send()
            xmsg(k - 1, 1).wait_send()
        dot_x(k, 0, True)
        start_a(k, 2)

    def x2(k):
        if k > 0:
            for t in range(2, 6):
                xmsg(k - 1, t).wait_send()
        dot_x(k, 1)
        start_a(k, 3)
        xmsg(k, 2).start()
        dot_x(k, 2)
        if k == 1:
            start_a(2, 0)
        xmsg(k, 3).start()

    def x2o(k):
        if k > 0:
            xout(k - 1).wait()
        dot_x(k, 3)
        if k == 1:
            start_a(2, 1)

    def xstage(k, t, slot):
        return pltpu.make_async_copy(XR.at[k, t], XS.at[4 + slot], s_xst.at[slot])

    def x3(k):
        for t in TWO:
            xmsg(k, t).wait_recv()
            xstage(k, t, t).start()
        for t in TWO:
            xstage(k, t, t).wait()
            add(XB.at[(1, 3)[t], t], XS.at[4 + t], QB)
            xmsg(k, 4 + t).start()

    def xout(k):
        return pltpu.make_async_copy(XB.at[2], dw.at[k], s_xo)

    def xadd(k, ts):
        for h, t in enumerate(ts):
            xmsg(k, t).wait_recv()
            xstage(k, t, h).start()
        for h, t in enumerate(ts):
            xstage(k, t, h).wait()
            add(XB.at[2, h], XS.at[4 + h], QB)

    def xfa(k):
        xadd(k, (3, 2))
        if k == 2:
            xout(k).start()

    def xfb(k):
        xadd(k, (4, 5))
        xout(k).start()

    def pair(n, col):
        return ((0, 3), (1, 2))[col][n % PAIR]

    def lw(n):
        if n < 2:
            for col in TWO:
                have(2, pair(n, col), 0)
                have(2, pair(n, col), 1)
        out = []
        for col in TWO:
            d = pair(n, col)
            q = xpos[d]
            if n < 2:
                if d == 0:
                    out.append(pltpu.make_async_copy(wd_ref, WD.at[col, c], s_w.at[col, 0]))
                    out.append(pltpu.make_async_copy(wdf.at[2 * x + c1], WD.at[col, c1], s_w.at[col, 1]))
                else:
                    out.append(pltpu.make_async_copy(wdf.at[pl.ds(2 * q, 2)], WD.at[col], s_w.at[col, 0]))
            else:
                for k in TWO:
                    full = (wgf, wuf)[k]
                    if d == 0:
                        out.append(pltpu.make_async_copy(w_in[k], WX.at[col, k, pl.ds(pl.multiple_of(CB * c, CB), CB), :], s_w.at[col, 2 * k]))
                        out.append(pltpu.make_async_copy(full.at[pl.ds(pl.multiple_of(TG * x + CB * c1, CB), CB), :],
                                                         WX.at[col, k, pl.ds(pl.multiple_of(CB * c1, CB), CB), :], s_w.at[col, 2 * k + 1]))
                    else:
                        out.append(pltpu.make_async_copy(full.at[pl.ds(pl.multiple_of(TG * q, TG), TG), :], WX.at[col, k], s_w.at[col, 2 * k]))
        for o in out:
            o.start()
        wl[n] = out

    wl = {}

    def dots_z(n, lo, m):

        def body(q, _):
            col = q // m
            idx = lo + 2 * (q % m)
            p = z + col * (y - z)
            ch = (p + 6 - idx) % RING
            s1 = QB - 192 * col
            s2 = RW + 192 * col
            own = (idx // PAIR) * (1 - idx // 3)
            slot = idx + own * 2 * (n % PAIR)

            def lhs(k):
                return jnp.concatenate([B[k, 0, pl.ds(pl.multiple_of(ch * s1 + g * s2, RW), RW), :] for g in range(4)], axis=0)

            if n < 2:
                l = lhs(0)
                for h in TWO:
                    ZB[col, slot, h] = jnp.dot(l, WD[col, h], preferred_element_type=F32)
            else:
                l = lhs(1)
                u = lhs(2)
                for h in TWO:
                    r = pl.ds(CB * h, CB)
                    ZB[col, slot, h] = (lax.dot_general(l, WX[col, 0, r, :], NT, preferred_element_type=F32)
                                        + lax.dot_general(u, WX[col, 1, r, :], NT, preferred_element_type=F32))
            return 0
        lax.fori_loop(0, 2 * m, body, 0)

    def zmsg(n, col, t):
        src = ((0, 0), (0, 1), (1, 1), (3, 0), (1, 0), (3, 1))[t]
        return remote(ZB.at[col, src[0], src[1]], ZR.at[col, n, t], s_zs.at[col, t], r_zs.at[col, n, t], link[col][t % PAIR])

    def own(n, col, h):
        return ZB.at[col, 2 + 2 * (n % PAIR), h]

    def sub(n, col, h, d):
        s = (pos[col][1] + d) % RING
        return ZB.at[col, 2 + 2 * (n % PAIR), h, pl.ds(pl.multiple_of(s * RW, RW), RW), :]

    def msg2(n, col, t):
        h, d = ((0, 2), (1, 2), (1, 1), (0, 3), (0, 1), (1, 3))[t]
        return remote(sub(n, col, h, d), Z2.at[col, n, t], s_2.at[col, n % PAIR, t], r_2.at[col, n, t], link[col][2 + t % PAIR])

    def p1(n):
        for l in wl[n]:
            l.wait()
        if n > 0:
            for col in TWO:
                for t in TWO:
                    zmsg(n - 1, col, t).wait_send()
        dots_z(n, 0, 1)
        for t in TWO:
            for col in TWO:
                zmsg(n, col, t).start()

    def p2(n):
        if n > 0:
            for col in TWO:
                for t in range(2, 6):
                    zmsg(n - 1, col, t).wait_send()
        dots_z(n, 1, 2)
        for t in range(2, 4):
            for col in TWO:
                zmsg(n, col, t).start()

    def p2o(n):
        if n > 1:
            for col in TWO:
                for t in range(6):
                    msg2(n - 2, col, t).wait_send()
        dots_z(n, 2, 1)

    def zstage(n, col, t, slot):
        return pltpu.make_async_copy(ZR.at[col, n, t], ZS.at[col, slot], s_zst.at[col, slot])

    def p4(n):
        for t in TWO:
            for col in TWO:
                zmsg(n, col, t).wait_recv()
                zstage(n, col, t, t).start()
        for t in TWO:
            for col in TWO:
                zstage(n, col, t, t).wait()
                add(ZB.at[col, (1, 3)[t], t], ZS.at[col, t], QB)
                zmsg(n, col, 4 + t).start()

    def zadd(n, ts):
        for h, t in enumerate(ts):
            for col in TWO:
                zmsg(n, col, t).wait_recv()
                zstage(n, col, t, h).start()
        for h, t in enumerate(ts):
            for col in TWO:
                zstage(n, col, t, h).wait()
                add(own(n, col, h), ZS.at[col, h], QB)

    def fa(n):
        zadd(n, (3, 2))

    def fb(n):
        zadd(n, (4, 5))
        for t in range(4):
            for col in TWO:
                msg2(n, col, t).start()

    def hh(n):
        for t in TWO:
            for col in TWO:
                msg2(n, col, t).wait_recv()
                add(sub(n, col, t, (1, 3)[t]), Z2.at[col, n, t], RW)
                msg2(n, col, 4 + t).start()

    def zf(n):
        a = n // PAIR
        for col in TWO:
            q = xpos[pair(n, col)]
            for h, ts in ((0, (3, 4)), (1, (2, 5))):
                for t in ts:
                    msg2(n, col, t).wait_recv()
                cs = pl.ds(pl.multiple_of(TG * q + CB * h, CB), CB)
                v = sub(n, col, h, 0)[...] + Z2[col, n, ts[0]] + Z2[col, n, ts[1]]
                ov[a, :, cs] = (res[a, :, cs].astype(F32) + v).astype(BF)
        done.append(n)
        if len(done) == RING:
            out.start()

    def enter():
        for d in dev.values():
            pl.semaphore_signal(barrier, inc=1, device_id=d, device_id_type=MESH)
        pl.semaphore_wait(barrier, len(dev))

    own_ld = [pltpu.make_async_copy(r, res.at[k], s_ld.at[k]) for k, r in enumerate((x_ref, dy_ref))]
    for l in own_ld:
        l.start()
    barrier = pltpu.get_barrier_semaphore()
    enter()
    own_ld[0].wait()
    own_ld[1].wait()
    put = pltpu.make_async_copy(res, xd.at[:, pl.ds(pl.multiple_of(j * RW, RW), RW), :], s_put)
    put.start()
    out = pltpu.make_async_copy(ov, yo, s_yo)
    done = []
    wpc(WG)
    ga(AX)
    wown(WU)
    gb0(AX)
    ga(AD)
    ga2(AX)
    gb31(AX)
    wown(WG)
    gb2(AX)
    ga2(AD)
    gf(AX, OWN)
    gf(AX, OPP)
    gf(AX, NEXT)
    gf(AX, PREV)
    wf(WU)
    wpc(WU)
    wpc(WL)
    wf(WG)
    ga(AE)
    gb31(AD)
    gend(AX)
    sab(B1)
    sab(B2)
    gb2(AD)
    sab(B0)
    ab(B0)
    sab(B3)
    wown(WL)
    wf2(WU)
    gb0(AE)
    ab(B1)
    gb0(AD)
    gf(AD, NEXT)
    sab(B5)
    ab(B2)
    ga2(AE)
    gf(AD, OPP)
    sab(B4)
    ab(B3)
    wf2(WG)
    ab(B4)
    sab(B7)
    sab(B6)
    gf(AD, PREV)
    gf(AD, OWN)
    ab(B5)
    gb31(AE)
    ab(B6)
    gend(AD)
    gb2(AE)
    gf(AE, OWN)
    wf(WL)
    ab(B7)
    hp()
    gf(AE, PREV)
    gf(AE, NEXT)
    xl(DOWN, 0)
    wfp()
    gf(AE, OPP)
    gend(AE)
    lw(Y0)
    x1(DOWN)
    xl(DOWN, 1)
    p1(Y0)
    x2(DOWN)
    x2o(DOWN)
    sg(B3)
    sg(B1)
    wf2(WL)
    sg(B0)
    p2(Y0)
    gg(B0)
    sg(B2)
    gg(B1)
    p4(Y0)
    p2o(Y0)
    lw(Y1)
    sg(B4)
    sg(B5)
    gg(B2)
    gg(B3)
    p1(Y1)
    sg(B6)
    sg(B7)
    gg(B4)
    x3(DOWN)
    gg(B5)
    gg(B6)
    gg(B7)
    xl(GATE, 0)
    lw(X0)
    dadb()
    xl(GATE, 1)
    p2(Y1)
    fa(Y0)
    x1(GATE)
    fb(Y0)
    p2o(Y1)
    hh(Y0)
    p4(Y1)
    x2(GATE)
    p1(X0)
    fa(Y1)
    fb(Y1)
    x3(GATE)
    p2(X0)
    hh(Y1)
    zf(Y0)
    p2o(X0)
    x1(UP)
    p4(X0)
    xfa(DOWN)
    xfb(DOWN)
    lw(X1)
    x2o(GATE)
    xfa(GATE)
    p1(X1)
    p2(X1)
    x2(UP)
    zf(Y1)
    fa(X0)
    p4(X1)
    x3(UP)
    fb(X0)
    p2o(X1)
    fa(X1)
    fb(X1)
    xfb(GATE)
    hh(X0)
    x2o(UP)
    hh(X1)
    xfa(UP)
    zf(X1)
    zf(X0)
    for r in sends:
        r.wait_send()
    for t in range(4, 6):
        xmsg(2, t).wait_recv()
    for t in range(6):
        xmsg(2, t).wait_send()
        for col in TWO:
            zmsg(3, col, t).wait_send()
            msg2(2, col, t).wait_send()
            msg2(3, col, t).wait_send()
    for k in range(3):
        bp[k].wait_send()
    for arr in TWO:
        for idx in range(4):
            ap(arr, idx).wait_send()
    xout(2).wait()
    out.wait()


def mlp(x, dy, wg, wu, wd):
    sd = jax.ShapeDtypeStruct
    dma = pltpu.SemaphoreType.DMA
    V = pltpu.VMEM
    o = pl.pallas_call(
        mlp_kernel,
        out_shape=(sd((3, 2, QB, FB), F32), sd((2, RW, DM), BF),
                   sd((2, TG, DM), BF), sd((DM, FB), BF), sd((DM, FB), BF), sd((8, FB, CB), BF), sd((4, 2, QB, FB), F32),
                   sd((3, 6, QB, FB), F32), sd((2, 4, 6, QB, CB), F32), sd((2, 4, TG, CB), BF)),
        in_specs=[HBM] * 5,
        out_specs=(HBM,) * 10,
        scratch_shapes=[
            V((3, 2, TG, FB), BF), V((2, 2, TG, CB), BF), V((4, 2, QB, FB), F32), V((6, QB, FB), F32),
            V((2, 2, FB, CB), BF), V((2, 2, TG, FB), BF), V((2, 5, 2, QB, CB), F32), V((2, 2, QB, CB), F32),
            V((2, 4, 6, RW, CB), F32), V((2, 2, 128, FB), F32), V((2, RW, DM), BF), V((2, RW, DM), BF),
            dma((NSEND,)), dma((NSEND,)), dma((2,)), dma, dma((4, 3)),
            dma((2, 2)), dma((2, 4)), dma((2, 4)), dma((3,)), dma((3,)), dma((6,)), dma((3, 6)),
            dma((2, 6)), dma((2, 4, 6)), dma((2, 2, 6)), dma((2, 4, 6)), dma((2, 4)), dma((4,)), dma((2, 4)), dma, dma, dma, dma((2, 2)),
        ],
        compiler_params=pltpu.CompilerParams(collective_id=1, has_side_effects=True, vmem_limit_bytes=67043328),
        name="mlp",
    )(x, dy, wg, wu, wd)
    return o[0], o[1], o[7]


def place_kernel(dw, yo, xr, y, dx, dg, du, dd, bw, by, bt, br, s_in, s_out):
    w_in = [pltpu.make_async_copy(dw.at[k], bw.at[k], s_in.at[k]) for k in range(3)]
    y_in = [pltpu.make_async_copy(yo.at[k], by.at[k], s_in.at[3 + k]) for k in TWO]
    r_in = pltpu.make_async_copy(xr.at[2, pl.ds(4, 2)], br, s_in.at[5])
    for l in w_in + [r_in] + y_in:
        l.start()
    w_out = [pltpu.make_async_copy(bt, dd, s_out.at[0]), pltpu.make_async_copy(bw.at[1], dg, s_out.at[1]), pltpu.make_async_copy(bw.at[2], du, s_out.at[2])]
    y_out = [pltpu.make_async_copy(by.at[0], y, s_out.at[3]), pltpu.make_async_copy(by.at[1], dx, s_out.at[4])]
    w_in[0].wait()
    for h in TWO:
        bt[:, pl.ds(QB * h, QB)] = bw[0, pl.ds(QB * h, QB), :].T
    w_out[0].start()
    w_in[1].wait()
    w_out[1].start()
    w_in[2].wait()
    r_in.wait()
    for h in TWO:
        bw[2, pl.ds(QB * h, QB), :] += br[h]
    w_out[2].start()
    for l, e in zip(y_in, y_out):
        l.wait()
        e.start()
    for e in w_out + y_out:
        e.wait()


def place(dw, yo, xr):
    sd = jax.ShapeDtypeStruct
    V = pltpu.VMEM
    return pl.pallas_call(
        place_kernel,
        out_shape=(sd((RW, DM), BF), sd((RW, DM), BF), sd((CB, FB), F32), sd((CB, FB), F32), sd((FB, CB), F32)),
        in_specs=[HBM] * 3,
        out_specs=(HBM,) * 5,
        scratch_shapes=[V((3, CB, FB), F32), V((2, RW, DM), BF), V((FB, CB), F32), V((2, QB, FB), F32),
                        pltpu.SemaphoreType.DMA((6,)), pltpu.SemaphoreType.DMA((5,))],
        compiler_params=pltpu.CompilerParams(vmem_limit_bytes=60 * 2**20),
        name="place",
    )(dw.reshape(3, CB, FB), yo, xr)


def solution(mesh):
    rows = P(("dp", "tp"), None)
    wsp = P("dp", "tp")
    dsp = P("tp", "dp")

    def local(x, w_gate, w_up, w_down, dy):
        return place(*mlp(x, dy, w_gate, w_up, w_down))

    return jax.shard_map(local, mesh=mesh, in_specs=(rows, wsp, wsp, dsp, rows), out_specs=(rows, rows, wsp, wsp, dsp), check_vma=False)
```

```python
import jax
import jax.numpy as jnp
from jax import lax
from jax.experimental import pallas as pl
from jax.experimental.pallas import tpu as pltpu
from jax.sharding import PartitionSpec as P

MESH = pl.DeviceIdType.MESH
HBM = pl.BlockSpec(memory_space=pltpu.HBM)
NT = (((1,), (1,)), ((), ()))
TN = (((0,), (0,)), ((), ()))
F32 = jnp.float32
BF = jnp.bfloat16
TWO = range(2)
RING = 4
PAIR = 2
HB = 448
FOUR = 128
DM, TG, FB, CB, QB, RW, RH = 4096, 1024, 896, 512, 256, 64, 32
AX, AD, AE = range(3)
OWN, NEXT, OPP, PREV = range(4)
WG, WU, WL = range(3)
DOWN, GATE, UP = range(3)
Y0, Y1, X0, X1 = range(4)
A0, A1, A2 = range(3)
B0, B1, B2, B3, B4, B5, B6, B7 = range(8)


def mlp_kernel(x_ref, dy_ref, wg_ref, wu_ref, wd_ref, dw, yo, xd, wgf, wuf, wdf, UV, XR, ZR, AP,
               B, A, XB, XS, WD, WX, ZB, ZS, Z2, res, ov,
               s_g, r_g, s_v, r_v, s_ap, r_ap, s_b, r_b, s_xs, r_xs, s_zs, r_zs, s_2, r_2, s_c, s_a, s_w, s_us, s_one):
    i = lax.axis_index("dp")
    j = lax.axis_index("tp")
    x, c, z, y = i // PAIR, i % PAIR, j // 4, j % RING
    xp, xm, xq, c1 = (x + 1) % RING, (x + 3) % RING, (x + 2) % RING, 1 - c
    dev = {
        "xp": {"dp": 2 * xp + c}, "xm": {"dp": 2 * xm + c}, "pc": {"dp": 2 * x + c1},
        "yp": {"tp": 4 * z + (y + 1) % RING}, "ym": {"tp": 4 * z + (y + 3) % RING},
        "zp": {"tp": 4 * ((z + 1) % RING) + y}, "zm": {"tp": 4 * ((z + 3) % RING) + y},
    }
    pos = ((z, y), (y, z))
    link = (("zp", "zm", "yp", "ym"), ("yp", "ym", "zp", "zm"))

    def remote(src, dst, ss, rs, to):
        return pltpu.make_async_remote_copy(src_ref=src, dst_ref=dst, send_sem=ss, recv_sem=rs, device_id=dev[to], device_id_type=MESH)

    def wait(ref, sem):
        pltpu.make_async_copy(ref, ref, sem).wait()

    def add(dst, src, n):
        def body(r, _):
            s = pl.ds(pl.multiple_of(r * RH, RH), RH)
            dst[s, :] = dst[s, :] + src[s, :]
            return 0
        lax.fori_loop(0, n // RH, body, 0)

    def send(src, dst, to, ss, rs):
        remote(src, dst, ss, rs, to).start()

    def wblk(k, xx, cc, half=None):
        ii = 2 * xx + cc
        if k < 2:
            r = (wgf, wuf)[k]
            if half is None:
                return r.at[pl.ds(pl.multiple_of(ii * CB, CB), CB), :]
            return r.at[pl.ds(pl.multiple_of(ii * CB + half * QB, QB), QB), :]
        if half is None:
            return wdf.at[ii]
        return wdf.at[ii, pl.ds(half * HB, HB), :]

    ahead = xq // PAIR

    def cols(a):
        if a == AX:
            return slice(None)
        h = ahead if a == AD else 1 - ahead
        return pl.ds(pl.multiple_of(h * (DM // PAIR), DM // PAIR), DM // PAIR)

    def rows(a, col, s, p, lo=0, n=RH):
        zz, yy = (p, s) if col == 0 else (s, p)
        return xd.at[min(a, AD), pl.ds(pl.multiple_of((zz * 4 + yy) * RW + col * RH + lo, 16), n), cols(a)]

    def geo(col):
        sec, prim = pos[col]
        sp, sm, pp, pm = link[col]
        return prim, sec, pp, pm, sp, sm

    def some(a, n):
        return xd.at[min(a, AD), pl.ds(0, n), cols(a)]

    FIRST, ON, LAST = range(4, 7)

    def ga(a):
        for col in TWO:
            p, s, pp, pm, sp, sm = geo(col)
            src = res.at[min(a, AD), pl.ds(col * RH, RH), cols(a)]
            for to in (pp, pm):
                send(src, rows(a, col, p, s), to, s_g.at[a], r_g.at[a, FIRST])

    def gb0(a):
        for col in TWO:
            p, s, pp, pm, sp, sm = geo(col)
            src = res.at[min(a, AD), pl.ds(col * RH, RH), cols(a)]
            for to in (sp, sm):
                send(src, rows(a, col, p, s), to, s_g.at[a], r_g.at[a, OWN])

    def ga2(a):
        wait(some(a, FOUR), r_g.at[a, FIRST])
        for col in TWO:
            p, s, pp, pm, sp, sm = geo(col)
            for d, lo, to in ((PREV, 0, pp), (NEXT, 16, pm)):
                r = rows(a, col, (p + d) % RING, s, lo, 16)
                send(r, r, to, s_g.at[a], r_g.at[a, ON])

    def gb31(a):
        for col in TWO:
            p, s, pp, pm, sp, sm = geo(col)
            for d in (PREV, NEXT):
                r = rows(a, col, (p + d) % RING, s)
                for to in (sp, sm):
                    send(r, r, to, s_g.at[a], r_g.at[a, d])

    def gb2(a):
        wait(some(a, RW), r_g.at[a, ON])
        for col in TWO:
            p, s, pp, pm, sp, sm = geo(col)
            r = rows(a, col, (p + OPP) % RING, s)
            for to in (sp, sm):
                send(r, r, to, s_g.at[a], r_g.at[a, OPP])

    def gf(a, d):
        wait(some(a, FOUR), r_g.at[a, d])
        for col in TWO:
            p, s, pp, pm, sp, sm = geo(col)
            for e, lo, to in ((PREV, 0, sp), (NEXT, 16, sm)):
                r = rows(a, col, (p + d) % RING, (s + e) % RING, lo, 16)
                send(r, r, to, s_g.at[a], r_g.at[a, LAST])

    def gend(a):
        if a == AX:
            put.wait()
        wait(some(a, QB), r_g.at[a, LAST])
        for arr, idx in (((AX, 0), (AX, 1), (AX, 3), (AX, 2)), ((AD, 0),), ((AD, 1), (AD, 3), (AD, 2)))[a]:
            ap(arr, idx).start()

    w_in = (wg_ref, wu_ref, wd_ref)
    LATE = 6
    seen = set()

    def blocks(k, n):
        return wdf.at[pl.ds(0, n)] if k == WL else (wgf, wuf)[k].at[pl.ds(0, n * CB), :]

    def once(k, g, n):
        if (k, g) not in seen:
            seen.add((k, g))
            wait(blocks(k, n), r_v.at[k, g])

    def wpc(k):
        send(w_in[k], wblk(k, x, c), "pc", s_v.at[k], r_v.at[k, OWN])

    def wown(k):
        for fr, to in enumerate(("xp", "xm")):
            if k < WL:
                send(w_in[k], wblk(k, x, c), to, s_v.at[k], r_v.at[k, FIRST])
            else:
                send(wd_ref.at[pl.ds(fr * HB, HB), :], wblk(k, x, c, fr), to, s_v.at[k], r_v.at[k, FIRST])
        if k == WL:
            for fr, to in enumerate(("xp", "xm")):
                send(wd_ref.at[pl.ds((1 - fr) * HB, HB), :], wblk(k, x, c, 1 - fr), to, s_v.at[k], r_v.at[k, LATE])

    def wf(k):
        once(k, FIRST, 1 if k == WL else 2)
        for xx, d, half, to in ((xm, PREV, 0, "xp"), (xp, NEXT, 1, "xm")):
            r = wblk(k, xx, c, half)
            send(r, r, to, s_v.at[k], r_v.at[k, ON])
            if k < WL:
                r = wblk(k, xx, c)
                send(r, r, "pc", s_v.at[k], r_v.at[k, d])

    def wfp():
        once(WL, LATE, 1)
        for xx, d in ((xm, PREV), (xp, NEXT)):
            r = wblk(WL, xx, c)
            send(r, r, "pc", s_v.at[WL], r_v.at[WL, d])

    def wf2(k):
        once(k, ON, 1)
        for half in TWO:
            r = wblk(k, xq, c, half)
            send(r, r, "pc", s_v.at[k], r_v.at[k, OPP])

    def have(k, d, o):
        if o == 1:
            once(k, d, 1)
        elif d == OPP:
            once(k, ON, 1)
        elif d:
            once(k, FIRST, 1 if k == WL else 2)
            if k == WL:
                once(k, LATE, 1)

    xpos = {0: x, 1: xp, 2: xq, 3: xm}
    order = ((0, 0), (0, 1), (3, 0), (1, 0), (3, 1), (1, 1), (2, 0), (2, 1))

    def blk(t):
        d, o = order[t]
        return 2 * xpos[d] + (c if o == 0 else c1)

    def a_slot(t):
        s = t % RING
        return A.at[s // PAIR, s % PAIR]

    def ld_ab(t):
        d, o = order[t]
        s = t % RING
        ii = blk(t)
        out = [pltpu.make_async_copy(xd.at[0, :, pl.ds(pl.multiple_of(ii * CB, CB), CB)], a_slot(t), s_c.at[s, 0])]
        for k in TWO:
            src = w_in[k] if t == 0 else wblk(k, xpos[d], c if o == 0 else c1)
            out.append(pltpu.make_async_copy(src, WX.at[s % PAIR, k, pl.ds((s // PAIR) * CB, CB), :], s_c.at[s, 1]))
        return out

    def sab(t):
        for k in TWO:
            have(k, *order[t])
        for l in ld_ab(t):
            l.start()

    def ab(t):
        s = t % RING
        wait(a_slot(t), s_c.at[s, 0])
        wait(WX.at[s % PAIR, :, pl.ds((s // PAIR) * CB, CB), :], s_c.at[s, 1])

        def body(m, _):
            r = pl.ds(pl.multiple_of(m * QB, QB), QB)
            lhs = A[s // PAIR, s % PAIR, r, :]
            for k in TWO:
                v = jnp.dot(lhs, WX[s % PAIR, k, pl.ds((s // PAIR) * CB, CB), :], preferred_element_type=F32)
                if t == 0:
                    XB[2 * k + m // PAIR, m % PAIR] = v
                else:
                    XB[2 * k + m // PAIR, m % PAIR] += v
            return 0
        lax.fori_loop(0, 4, body, 0)

    def hp():
        def body(q, _):
            m = q // 8
            r = pl.ds(pl.multiple_of((q % 8) * RH, RH), RH)
            a = XB[m // PAIR, m % PAIR, r, :]
            b = XB[2 + m // PAIR, m % PAIR, r, :]
            sig = jax.nn.sigmoid(a)
            sa = a * sig
            XB[m // PAIR, m % PAIR, r, :] = b * sig * (1.0 + a * (1.0 - sig))
            XB[2 + m // PAIR, m % PAIR, r, :] = sa
            B[0, 0, pl.ds(pl.multiple_of(q * RH, RH), RH), :] = (sa * b).astype(BF)
            return 0
        lax.fori_loop(0, RH, body, 0)
        bp[0].start()
        uv_put.start()

    uv_put = pltpu.make_async_copy(XB, UV, s_one.at[0])

    def ld_g(t):
        d, o = order[t]
        s = t % RING
        ii = blk(t)
        src = wd_ref if t == 0 else wdf.at[ii]
        return [pltpu.make_async_copy(xd.at[1, :, pl.ds(pl.multiple_of(ii * CB, CB), CB)], a_slot(t), s_c.at[s, 0]),
                pltpu.make_async_copy(src, WX.at[s % PAIR, s // PAIR, pl.ds(0, FB), pl.ds(0, CB)], s_c.at[s, 1])]

    def sg(t):
        have(2, *order[t])
        for l in ld_g(t):
            l.start()

    def gg(t):
        for l in ld_g(t):
            l.wait()
        s = t % RING

        def body(m, _):
            r = pl.ds(pl.multiple_of(m * QB, QB), QB)
            v = lax.dot_general(A[s // PAIR, s % PAIR, r, :], WX[s % PAIR, s // PAIR, pl.ds(0, FB), pl.ds(0, CB)], NT, preferred_element_type=F32)
            if t == 0:
                XS[m] = v
            else:
                XS[m] += v
            return 0
        lax.fori_loop(0, 4, body, 0)

    def us_load(q, k):
        m = q // PAIR
        return pltpu.make_async_copy(UV.at[2 * k + m // PAIR, m % PAIR, pl.ds(pl.multiple_of((q % PAIR) * FOUR, FOUR), FOUR), :], XS.at[4 + q % PAIR, pl.ds(FOUR * k, FOUR), :], s_us.at[q % PAIR])

    def dadb():
        for k in TWO:
            us_load(0, k).start()

        def body(q, _):
            @pl.when(q < 7)
            def _():
                for k in TWO:
                    us_load(q + 1, k).start()
            wait(XS.at[4 + q % PAIR], s_us.at[q % PAIR])

            def inner(e, _):
                g = XS[q // PAIR, pl.ds(pl.multiple_of((q % PAIR) * FOUR + e * RH, RH), RH), :]
                o = pl.ds(pl.multiple_of(q * FOUR + e * RH, RH), RH)
                for k in TWO:
                    B[1 + k, 0, o, :] = (g * XS[4 + q % PAIR, pl.ds(pl.multiple_of(FOUR * k + e * RH, RH), RH), :]).astype(BF)
                return 0
            lax.fori_loop(0, 4, inner, 0)
            return 0
        lax.fori_loop(0, 8, body, 0)
        bp[1].start()
        bp[2].start()

    def chunk(idx):
        return (x + 6 - idx) % RING

    bp = [remote(B.at[k, 0], B.at[k, 1], s_b, r_b.at[k], "pc") for k in range(3)]

    def ap(arr, idx):
        return remote(xd.at[arr, :, pl.ds(pl.multiple_of(TG * chunk(idx) + CB * c1, CB), CB)], AP.at[arr, idx], s_ap, r_ap.at[arr, idx], "pc")

    seq = (0, 1, 3, 2)

    def load_a(k, n):
        arr = 1 - min(k, 1)
        idx = seq[n]
        return (pltpu.make_async_copy(xd.at[arr, :, pl.ds(pl.multiple_of(TG * chunk(idx) + CB * c, CB), CB)], A.at[n % PAIR, 0], s_a.at[n % PAIR]),
                pltpu.make_async_copy(AP.at[arr, idx], A.at[n % PAIR, 1], s_a.at[n % PAIR]))

    def start_a(k, n):
        if k < UP:
            ap(1 - k, seq[n]).wait_recv()
        for l in load_a(k, n):
            l.start()

    def dot_x(k, n, split=False):
        slot = n % PAIR
        wait(A.at[slot], s_a.at[slot])

        def body(m, _):
            cols = pl.ds(pl.multiple_of(m * QB, QB), QB)
            XB[seq[n], m] = (lax.dot_general(A[slot, 0, :, cols], B[k, 0], TN, preferred_element_type=F32)
                             + lax.dot_general(A[slot, 1, :, cols], B[k, 1], TN, preferred_element_type=F32))
            return 0

        if split:
            for m in TWO:
                body(m, 0)
                xmsg(k, m).start()
        else:
            lax.fori_loop(0, 2, body, 0)

    def xmsg(k, t):
        src = (XB.at[0, 0], XB.at[0, 1], XB.at[1, 1], XB.at[3, 0], XB.at[1, 0], XB.at[3, 1])[t]
        return remote(src, XR.at[k, t], s_xs.at[min(t // PAIR, 1)], r_xs.at[k, t // PAIR], ("xp", "xm")[t % PAIR])

    def xl(k, n):
        start_a(k, n)

    def x1(k):
        bp[k].wait_recv()
        if k == 0:
            uv_put.wait()
        else:
            wait(XB.at[0], s_xs.at[0])
        dot_x(k, 0, True)

    def x2(k):
        if k > 0:
            wait(XB.at[pl.ds(0, 2)], s_xs.at[1])
        dot_x(k, 1)
        start_a(k, 3)
        xmsg(k, 2).start()
        dot_x(k, 2)
        if k == 1:
            start_a(2, 0)
        xmsg(k, 3).start()

    def x2o(k):
        if k > 0:
            xout(k - 1).wait()
        dot_x(k, 3)
        if k == 1:
            start_a(2, 1)

    def xstage(k, t, slot):
        return pltpu.make_async_copy(XR.at[k, t], XS.at[4 + slot], s_one.at[1])

    def x3(k):
        wait(XS.at[pl.ds(4, 2)], r_xs.at[k, 0])
        for t in TWO:
            xstage(k, t, t).start()
        wait(XS.at[pl.ds(4, 2)], s_one.at[1])
        for t in TWO:
            add(XB.at[(1, 3)[t], t], XS.at[4 + t], QB)
            xmsg(k, 4 + t).start()

    def xout(k):
        return pltpu.make_async_copy(XB.at[2], dw.at[k], s_one.at[2])

    def xadd(k, ts):
        wait(XS.at[pl.ds(4, 2)], r_xs.at[k, ts[0] // PAIR])
        for h, t in enumerate(ts):
            xstage(k, t, h).start()
        wait(XS.at[pl.ds(4, 2)], s_one.at[1])
        for h, t in enumerate(ts):
            add(XB.at[2, h], XS.at[4 + h], QB)

    def xfa(k):
        xadd(k, (3, 2))
        if k == 2:
            xout(k).start()

    def xfb(k):
        xadd(k, (4, 5))
        xout(k).start()

    def pair(n, col):
        return ((0, 3), (1, 2))[col][n % PAIR]

    def lw(n):
        if n < 2:
            for col in TWO:
                have(2, pair(n, col), 0)
                have(2, pair(n, col), 1)
        out = []
        for col in TWO:
            d = pair(n, col)
            q = xpos[d]
            if n < 2:
                if d == 0:
                    out.append(pltpu.make_async_copy(wd_ref, WD.at[col, c], s_w.at[n // PAIR]))
                    out.append(pltpu.make_async_copy(wdf.at[2 * x + c1], WD.at[col, c1], s_w.at[n // PAIR]))
                else:
                    out.append(pltpu.make_async_copy(wdf.at[pl.ds(2 * q, 2)], WD.at[col], s_w.at[n // PAIR]))
            else:
                for k in TWO:
                    full = (wgf, wuf)[k]
                    if d == 0:
                        out.append(pltpu.make_async_copy(w_in[k], WX.at[col, k, pl.ds(pl.multiple_of(CB * c, CB), CB), :], s_w.at[n // PAIR]))
                        out.append(pltpu.make_async_copy(full.at[pl.ds(pl.multiple_of(TG * x + CB * c1, CB), CB), :],
                                                         WX.at[col, k, pl.ds(pl.multiple_of(CB * c1, CB), CB), :], s_w.at[n // PAIR]))
                    else:
                        out.append(pltpu.make_async_copy(full.at[pl.ds(pl.multiple_of(TG * q, TG), TG), :], WX.at[col, k], s_w.at[n // PAIR]))
        for o in out:
            o.start()

    def dots_z(n, lo, m):

        def body(q, _):
            col = q // m
            idx = lo + 2 * (q % m)
            p = z + col * (y - z)
            ch = (p + 6 - idx) % RING
            s1 = QB - 192 * col
            s2 = RW + 192 * col
            own = (idx // PAIR) * (1 - idx // 3)
            slot = idx + own * 2 * (n % PAIR)

            def lhs(k):
                return jnp.concatenate([B[k, 0, pl.ds(pl.multiple_of(ch * s1 + g * s2, RW), RW), :] for g in range(4)], axis=0)

            if n < 2:
                l = lhs(0)
                for h in TWO:
                    ZB[col, slot, h] = jnp.dot(l, WD[col, h], preferred_element_type=F32)
            else:
                l = lhs(1)
                u = lhs(2)
                for h in TWO:
                    r = pl.ds(CB * h, CB)
                    ZB[col, slot, h] = (lax.dot_general(l, WX[col, 0, r, :], NT, preferred_element_type=F32)
                                        + lax.dot_general(u, WX[col, 1, r, :], NT, preferred_element_type=F32))
            return 0
        lax.fori_loop(0, 2 * m, body, 0)

    def zmsg(n, col, t):
        src = ((0, 0), (0, 1), (1, 1), (3, 0), (1, 0), (3, 1))[t]
        return remote(ZB.at[col, src[0], src[1]], ZR.at[col, n, t], s_zs.at[min(t // PAIR, 1)], r_zs.at[n, t // PAIR], link[col][t % PAIR])

    def own(n, col, h):
        return ZB.at[col, 2 + 2 * (n % PAIR), h]

    def sub(n, col, h, d):
        s = (pos[col][1] + d) % RING
        return ZB.at[col, 2 + 2 * (n % PAIR), h, pl.ds(pl.multiple_of(s * RW, RW), RW), :]

    def msg2(n, col, t):
        h, d = ((0, 2), (1, 2), (1, 1), (0, 3), (0, 1), (1, 3))[t]
        return remote(sub(n, col, h, d), Z2.at[col, n, t], s_2.at[n % PAIR], r_2.at[n, min(t // PAIR, 1)], link[col][2 + t % PAIR])

    def p1(n):
        wait((WD, WX)[n // PAIR], s_w.at[n // PAIR])
        if n > 0:
            wait(ZB.at[0, pl.ds(0, 2)], s_zs.at[0])
        dots_z(n, 0, 1)
        for t in TWO:
            for col in TWO:
                zmsg(n, col, t).start()

    def p2(n):
        if n > 0:
            wait(ZB.at[0, pl.ds(0, 4)], s_zs.at[1])
        dots_z(n, 1, 2)
        for t in range(2, 4):
            for col in TWO:
                zmsg(n, col, t).start()

    def p2o(n):
        if n > 1:
            wait(Z2.at[0, pl.ds(0, 2)], s_2.at[n % PAIR])
        dots_z(n, 2, 1)

    def zstage(n, col, t, slot):
        return pltpu.make_async_copy(ZR.at[col, n, t], ZS.at[col, slot], s_one.at[3])

    def stage(n, ts):
        wait(ZS, r_zs.at[n, ts[0] // PAIR])
        for h, t in enumerate(ts):
            for col in TWO:
                zstage(n, col, t, h).start()
        wait(ZS, s_one.at[3])

    def p4(n):
        stage(n, (0, 1))
        for t in TWO:
            for col in TWO:
                add(ZB.at[col, (1, 3)[t], t], ZS.at[col, t], QB)
                zmsg(n, col, 4 + t).start()

    def zadd(n, ts):
        stage(n, ts)
        for h in TWO:
            for col in TWO:
                add(own(n, col, h), ZS.at[col, h], QB)

    def fa(n):
        zadd(n, (3, 2))

    def fb(n):
        zadd(n, (4, 5))
        for t in range(4):
            for col in TWO:
                msg2(n, col, t).start()

    def hh(n):
        wait(Z2.at[0, 0, pl.ds(0, 4)], r_2.at[n, 0])
        for t in TWO:
            for col in TWO:
                add(sub(n, col, t, (1, 3)[t]), Z2.at[col, n, t], RW)
                msg2(n, col, 4 + t).start()

    def zf(n):
        a = n // PAIR
        wait(Z2.at[:, 0, pl.ds(0, 4)], r_2.at[n, 1])
        for col in TWO:
            q = xpos[pair(n, col)]
            for h, ts in ((0, (3, 4)), (1, (2, 5))):
                cs = pl.ds(pl.multiple_of(TG * q + CB * h, CB), CB)
                v = sub(n, col, h, 0)[...] + Z2[col, n, ts[0]] + Z2[col, n, ts[1]]
                ov[a, :, cs] = (res[a, :, cs].astype(F32) + v).astype(BF)
        done.append(n)
        if len(done) == RING:
            out.start()

    def enter():
        for d in dev.values():
            pl.semaphore_signal(barrier, inc=1, device_id=d, device_id_type=MESH)
        pl.semaphore_wait(barrier, len(dev))

    own_ld = [pltpu.make_async_copy(r, res.at[k], s_one.at[4]) for k, r in enumerate((x_ref, dy_ref))]
    for l in own_ld:
        l.start()
    barrier = pltpu.get_barrier_semaphore()
    enter()
    wait(res, s_one.at[4])
    put = pltpu.make_async_copy(res, xd.at[:, pl.ds(pl.multiple_of(j * RW, RW), RW), :], s_one.at[5])
    put.start()
    out = pltpu.make_async_copy(ov, yo, s_one.at[6])
    done = []
    ga(AX)
    gb0(AX)
    ga(AD)
    wpc(WL)
    wpc(WU)
    wpc(WG)
    wown(WG)
    ga2(AX)
    gf(AX, OWN)
    gb31(AX)
    wown(WU)
    ga2(AD)
    gb2(AX)
    wf(WG)
    gf(AX, PREV)
    gf(AX, NEXT)
    gf(AX, OPP)
    ga(AE)
    gb31(AD)
    wf(WU)
    gb0(AD)
    gend(AX)
    sab(B2)
    sab(B1)
    sab(B0)
    ab(B0)
    wown(WL)
    ab(B1)
    gb2(AD)
    sab(B3)
    gf(AD, PREV)
    sab(B4)
    ga2(AE)
    wf2(WG)
    ab(B2)
    gb0(AE)
    wf2(WU)
    gf(AD, OWN)
    ab(B3)
    sab(B6)
    gf(AD, NEXT)
    gf(AD, OPP)
    sab(B5)
    ab(B4)
    sab(B7)
    gb2(AE)
    ab(B5)
    gb31(AE)
    gf(AE, OWN)
    ab(B6)
    wf(WL)
    ab(B7)
    gend(AD)
    hp()
    xl(DOWN, A0)
    gf(AE, PREV)
    wfp()
    gf(AE, NEXT)
    gf(AE, OPP)
    x1(DOWN)
    lw(Y0)
    gend(AE)
    p1(Y0)
    xl(DOWN, A2)
    xl(DOWN, A1)
    wf2(WL)
    p2(Y0)
    x2(DOWN)
    x2o(DOWN)
    sg(B1)
    sg(B0)
    p2o(Y0)
    lw(Y1)
    gg(B0)
    sg(B4)
    sg(B3)
    gg(B1)
    sg(B2)
    p4(Y0)
    gg(B2)
    gg(B3)
    gg(B4)
    sg(B5)
    p1(Y1)
    x3(DOWN)
    sg(B6)
    gg(B5)
    gg(B6)
    sg(B7)
    p2(Y1)
    gg(B7)
    xl(GATE, A0)
    lw(X0)
    dadb()
    xfa(DOWN)
    p2o(Y1)
    xl(GATE, A1)
    x1(GATE)
    p4(Y1)
    fa(Y0)
    p1(X0)
    xl(GATE, A2)
    x2(GATE)
    fb(Y0)
    xfb(DOWN)
    x3(GATE)
    fa(Y1)
    x1(UP)
    fb(Y1)
    hh(Y0)
    x2o(GATE)
    p2(X0)
    zf(Y0)
    xl(UP, A2)
    p4(X0)
    p2o(X0)
    lw(X1)
    hh(Y1)
    p1(X1)
    xfa(GATE)
    x2(UP)
    fa(X0)
    p2(X1)
    p4(X1)
    xfb(GATE)
    x3(UP)
    zf(Y1)
    fb(X0)
    p2o(X1)
    x2o(UP)
    fa(X1)
    fb(X1)
    hh(X0)
    xfa(UP)
    hh(X1)
    zf(X0)
    zf(X1)
    def end():
        for a in (AX, AD, AE):
            wait(some(a, 960), s_g.at[a])
        for k in (WG, WU, WL):
            wait(blocks(k, 7), s_v.at[k])
        wait(AP, s_ap)
        wait(B.at[:, 0], s_b)
        for q in TWO:
            wait(Z2.at[0, pl.ds(0, 2)], s_2.at[q])
            wait(ZB.at[0, pl.ds(0, 2 + 2 * q)], s_zs.at[q])
        xout(2).wait()
        out.wait()
        wait(XB.at[0], s_xs.at[0])
        wait(XB.at[pl.ds(0, 2)], s_xs.at[1])
        wait(XS.at[pl.ds(4, 2)], r_xs.at[2, 2])

    end()


def mlp(x, dy, wg, wu, wd):
    sd = jax.ShapeDtypeStruct
    dma = pltpu.SemaphoreType.DMA
    V = pltpu.VMEM
    o = pl.pallas_call(
        mlp_kernel,
        out_shape=(sd((3, 2, QB, FB), F32), sd((2, RW, DM), BF),
                   sd((2, TG, DM), BF), sd((DM, FB), BF), sd((DM, FB), BF), sd((8, FB, CB), BF), sd((4, 2, QB, FB), F32),
                   sd((3, 6, QB, FB), F32), sd((2, 4, 6, QB, CB), F32), sd((2, 4, TG, CB), BF)),
        in_specs=[HBM] * 5,
        out_specs=(HBM,) * 10,
        scratch_shapes=[
            V((3, 2, TG, FB), BF), V((2, 2, TG, CB), BF), V((4, 2, QB, FB), F32), V((6, QB, FB), F32),
            V((2, 2, FB, CB), BF), V((2, 2, TG, FB), BF), V((2, 5, 2, QB, CB), F32), V((2, 2, QB, CB), F32),
            V((2, 4, 6, RW, CB), F32), V((2, RW, DM), BF), V((2, RW, DM), BF),
            dma((3,)), dma((3, 7)), dma((3,)), dma((3, 7)), dma, dma((2, 4)), dma, dma((3,)), dma((2,)), dma((3, 3)),
            dma((2,)), dma((4, 3)), dma((2,)), dma((4, 2)), dma((4, 2)), dma((2,)), dma((2,)), dma((2,)), dma((7,)),
        ],
        compiler_params=pltpu.CompilerParams(collective_id=1, has_side_effects=True, vmem_limit_bytes=67043328),
        name="mlp",
    )(x, dy, wg, wu, wd)
    return o[0], o[1], o[7]


def place_kernel(dw, yo, xr, y, dx, dg, du, dd, bw, by, bt, br, s_in, s_out):
    w_in = [pltpu.make_async_copy(dw.at[k], bw.at[k], s_in.at[k]) for k in range(3)]
    y_in = [pltpu.make_async_copy(yo.at[k], by.at[k], s_in.at[3 + k]) for k in TWO]
    r_in = pltpu.make_async_copy(xr.at[2, pl.ds(4, 2)], br, s_in.at[5])
    for l in w_in + [r_in] + y_in:
        l.start()
    w_out = [pltpu.make_async_copy(bt, dd, s_out.at[0]), pltpu.make_async_copy(bw.at[1], dg, s_out.at[1]), pltpu.make_async_copy(bw.at[2], du, s_out.at[2])]
    y_out = [pltpu.make_async_copy(by.at[0], y, s_out.at[3]), pltpu.make_async_copy(by.at[1], dx, s_out.at[4])]
    w_in[0].wait()
    for h in TWO:
        bt[:, pl.ds(QB * h, QB)] = bw[0, pl.ds(QB * h, QB), :].T
    w_out[0].start()
    w_in[1].wait()
    w_out[1].start()
    w_in[2].wait()
    r_in.wait()
    for h in TWO:
        bw[2, pl.ds(QB * h, QB), :] += br[h]
    w_out[2].start()
    for l, e in zip(y_in, y_out):
        l.wait()
        e.start()
    for e in w_out + y_out:
        e.wait()


def place(dw, yo, xr):
    sd = jax.ShapeDtypeStruct
    V = pltpu.VMEM
    return pl.pallas_call(
        place_kernel,
        out_shape=(sd((RW, DM), BF), sd((RW, DM), BF), sd((CB, FB), F32), sd((CB, FB), F32), sd((FB, CB), F32)),
        in_specs=[HBM] * 3,
        out_specs=(HBM,) * 5,
        scratch_shapes=[V((3, CB, FB), F32), V((2, RW, DM), BF), V((FB, CB), F32), V((2, QB, FB), F32),
                        pltpu.SemaphoreType.DMA((6,)), pltpu.SemaphoreType.DMA((5,))],
        compiler_params=pltpu.CompilerParams(vmem_limit_bytes=60 * 2**20),
        name="place",
    )(dw.reshape(3, CB, FB), yo, xr)


def solution(mesh):
    rows = P(("dp", "tp"), None)
    wsp = P("dp", "tp")
    dsp = P("tp", "dp")

    def local(x, w_gate, w_up, w_down, dy):
        return place(*mlp(x, dy, w_gate, w_up, w_down))

    return jax.shard_map(local, mesh=mesh, in_specs=(rows, wsp, wsp, dsp, rows), out_specs=(rows, rows, wsp, wsp, dsp), check_vma=False)
```

```python
import jax
import jax.numpy as jnp
from jax import lax
from jax.experimental import pallas as pl
from jax.experimental.pallas import tpu as pltpu
from jax.sharding import PartitionSpec as P

MESH = pl.DeviceIdType.MESH
HBM = pl.BlockSpec(memory_space=pltpu.HBM)
VMEM = pl.BlockSpec(memory_space=pltpu.VMEM)
NT = (((1,), (1,)), ((), ()))
TN = (((0,), (0,)), ((), ()))
F32 = jnp.float32
BF = jnp.bfloat16
TWO = range(2)
RING = 4
PAIR = 2
HB = 448
FOUR = 128
DM, TG, FB, CB, QB, RW, RH = 4096, 1024, 896, 512, 256, 64, 32
AX, AD, AE = range(3)
OWN, NEXT, OPP, PREV = range(4)
WG, WU, WL = range(3)
DOWN, GATE, UP = range(3)
Y0, Y1, X0, X1 = range(4)
A0, A1, A2 = range(3)
B0, B1, B2, B3, B4, B5, B6, B7 = range(8)


def mlp_kernel(x_ref, dy_ref, wg_ref, wu_ref, wd_ref, dw, yo, du, xd, wgf, wuf, wdf, U, V, XR, ZR, AP,
               B, A, XB, XS, WD, WX, ZB, ZS, Z2,
               s_g, r_g, s_v, r_v, s_ap, r_ap, s_b, r_b, s_xs, r_xs, s_zs, r_zs, s_2, r_2, s_c, s_a, s_w, s_us, s_one):
    i = lax.axis_index("dp")
    j = lax.axis_index("tp")
    x, c, z, y = i // PAIR, i % PAIR, j // 4, j % RING
    xp, xm, xq, c1 = (x + 1) % RING, (x + 3) % RING, (x + 2) % RING, 1 - c
    dev = {
        "xp": {"dp": 2 * xp + c}, "xm": {"dp": 2 * xm + c}, "pc": {"dp": 2 * x + c1},
        "yp": {"tp": 4 * z + (y + 1) % RING}, "ym": {"tp": 4 * z + (y + 3) % RING},
        "zp": {"tp": 4 * ((z + 1) % RING) + y}, "zm": {"tp": 4 * ((z + 3) % RING) + y},
    }
    pos = ((z, y), (y, z))
    link = (("zp", "zm", "yp", "ym"), ("yp", "ym", "zp", "zm"))

    def remote(src, dst, ss, rs, to):
        return pltpu.make_async_remote_copy(src_ref=src, dst_ref=dst, send_sem=ss, recv_sem=rs, device_id=dev[to], device_id_type=MESH)

    def wait(ref, sem):
        pltpu.make_async_copy(ref, ref, sem).wait()

    def add(dst, src, n):
        def body(r, _):
            s = pl.ds(pl.multiple_of(r * RH, RH), RH)
            dst[s, :] = dst[s, :] + src[s, :]
            return 0
        lax.fori_loop(0, n // RH, body, 0)

    def send(src, dst, to, ss, rs):
        remote(src, dst, ss, rs, to).start()

    def wblk(k, xx, cc, half=None):
        ii = 2 * xx + cc
        if k < 2:
            r = (wgf, wuf)[k]
            if half is None:
                return r.at[pl.ds(pl.multiple_of(ii * CB, CB), CB), :]
            return r.at[pl.ds(pl.multiple_of(ii * CB + half * QB, QB), QB), :]
        if half is None:
            return wdf.at[ii]
        return wdf.at[ii, pl.ds(half * HB, HB), :]

    ahead = xq // PAIR

    def cols(a):
        if a == AX:
            return slice(None)
        h = ahead if a == AD else 1 - ahead
        return pl.ds(pl.multiple_of(h * (DM // PAIR), DM // PAIR), DM // PAIR)

    def rows(a, col, s, p, lo=0, n=RH):
        zz, yy = (p, s) if col == 0 else (s, p)
        return xd.at[min(a, AD), pl.ds(pl.multiple_of((zz * 4 + yy) * RW + col * RH + lo, 16), n), cols(a)]

    def geo(col):
        sec, prim = pos[col]
        sp, sm, pp, pm = link[col]
        return prim, sec, pp, pm, sp, sm

    def some(a, n):
        return xd.at[min(a, AD), pl.ds(0, n), cols(a)]

    FIRST, ON, LAST = range(4, 7)

    def ga(a):
        for col in TWO:
            p, s, pp, pm, sp, sm = geo(col)
            src = yo.at[min(a, AD), pl.ds(col * RH, RH), cols(a)]
            for to in (pp, pm):
                send(src, rows(a, col, p, s), to, s_g.at[a], r_g.at[a, FIRST])

    def gb0(a):
        for col in TWO:
            p, s, pp, pm, sp, sm = geo(col)
            src = yo.at[min(a, AD), pl.ds(col * RH, RH), cols(a)]
            for to in (sp, sm):
                send(src, rows(a, col, p, s), to, s_g.at[a], r_g.at[a, OWN])

    def ga2(a):
        wait(some(a, FOUR), r_g.at[a, FIRST])
        for col in TWO:
            p, s, pp, pm, sp, sm = geo(col)
            for d, lo, to in ((PREV, 0, pp), (NEXT, 16, pm)):
                r = rows(a, col, (p + d) % RING, s, lo, 16)
                send(r, r, to, s_g.at[a], r_g.at[a, ON])

    def gb31(a):
        for col in TWO:
            p, s, pp, pm, sp, sm = geo(col)
            for d in (PREV, NEXT):
                r = rows(a, col, (p + d) % RING, s)
                for to in (sp, sm):
                    send(r, r, to, s_g.at[a], r_g.at[a, d])

    def gb2(a):
        wait(some(a, RW), r_g.at[a, ON])
        for col in TWO:
            p, s, pp, pm, sp, sm = geo(col)
            r = rows(a, col, (p + OPP) % RING, s)
            for to in (sp, sm):
                send(r, r, to, s_g.at[a], r_g.at[a, OPP])

    def gf(a, d):
        wait(some(a, FOUR), r_g.at[a, d])
        for col in TWO:
            p, s, pp, pm, sp, sm = geo(col)
            for e, lo, to in ((PREV, 0, sp), (NEXT, 16, sm)):
                r = rows(a, col, (p + d) % RING, (s + e) % RING, lo, 16)
                send(r, r, to, s_g.at[a], r_g.at[a, LAST])

    def gend(a):
        if a == AX:
            put.wait()
        wait(some(a, QB), r_g.at[a, LAST])
        for arr, idx in (((AX, 0), (AX, 1), (AX, 3), (AX, 2)), ((AD, 0),), ((AD, 1), (AD, 3), (AD, 2)))[a]:
            ap(arr, idx).start()

    w_in = (wg_ref, wu_ref, wd_ref)
    LATE = 6
    seen = set()

    def blocks(k, n):
        return wdf.at[pl.ds(0, n)] if k == WL else (wgf, wuf)[k].at[pl.ds(0, n * CB), :]

    def once(k, g, n):
        if (k, g) not in seen:
            seen.add((k, g))
            wait(blocks(k, n), r_v.at[k, g])

    def wpc(k):
        send(w_in[k], wblk(k, x, c), "pc", s_v.at[k], r_v.at[k, OWN])

    def wown(k):
        for fr, to in enumerate(("xp", "xm")):
            if k < WL:
                send(w_in[k], wblk(k, x, c), to, s_v.at[k], r_v.at[k, FIRST])
            else:
                send(wd_ref.at[pl.ds(fr * HB, HB), :], wblk(k, x, c, fr), to, s_v.at[k], r_v.at[k, FIRST])
        if k == WL:
            for fr, to in enumerate(("xp", "xm")):
                send(wd_ref.at[pl.ds((1 - fr) * HB, HB), :], wblk(k, x, c, 1 - fr), to, s_v.at[k], r_v.at[k, LATE])

    def wf(k):
        once(k, FIRST, 1 if k == WL else 2)
        for xx, d, half, to in ((xm, PREV, 0, "xp"), (xp, NEXT, 1, "xm")):
            r = wblk(k, xx, c, half)
            send(r, r, to, s_v.at[k], r_v.at[k, ON])
            if k < WL:
                r = wblk(k, xx, c)
                send(r, r, "pc", s_v.at[k], r_v.at[k, d])

    def wfp():
        once(WL, LATE, 1)
        for xx, d in ((xm, PREV), (xp, NEXT)):
            r = wblk(WL, xx, c)
            send(r, r, "pc", s_v.at[WL], r_v.at[WL, d])

    def wf2(k):
        once(k, ON, 1)
        for half in TWO:
            r = wblk(k, xq, c, half)
            send(r, r, "pc", s_v.at[k], r_v.at[k, OPP])

    def have(k, d, o):
        if o == 1:
            once(k, d, 1)
        elif d == OPP:
            once(k, ON, 1)
        elif d:
            once(k, FIRST, 1 if k == WL else 2)
            if k == WL:
                once(k, LATE, 1)

    xpos = {0: x, 1: xp, 2: xq, 3: xm}
    order = ((0, 0), (0, 1), (3, 0), (1, 0), (3, 1), (1, 1), (2, 0), (2, 1))

    def blk(t):
        d, o = order[t]
        return 2 * xpos[d] + (c if o == 0 else c1)

    def a_slot(t):
        s = t % RING
        return A.at[s // PAIR, s % PAIR]

    def ld_ab(t):
        d, o = order[t]
        s = t % RING
        ii = blk(t)
        out = [pltpu.make_async_copy(xd.at[0, :, pl.ds(pl.multiple_of(ii * CB, CB), CB)], a_slot(t), s_c.at[s, 0])]
        for k in TWO:
            src = w_in[k] if t == 0 else wblk(k, xpos[d], c if o == 0 else c1)
            out.append(pltpu.make_async_copy(src, WX.at[s % PAIR, k, pl.ds((s // PAIR) * CB, CB), :], s_c.at[s, 1]))
        return out

    def sab(t):
        for k in TWO:
            have(k, *order[t])
        for l in ld_ab(t):
            l.start()

    def ab(t):
        s = t % RING
        wait(a_slot(t), s_c.at[s, 0])
        wait(WX.at[s % PAIR, :, pl.ds((s // PAIR) * CB, CB), :], s_c.at[s, 1])

        def body(m, _):
            r = pl.ds(pl.multiple_of(m * QB, QB), QB)
            lhs = A[s // PAIR, s % PAIR, r, :]
            for k in TWO:
                v = jnp.dot(lhs, WX[s % PAIR, k, pl.ds((s // PAIR) * CB, CB), :], preferred_element_type=F32)
                to = XB.at[m // PAIR, m % PAIR] if k == WG else XS.at[m]
                to[...] = v if t == 0 else to[...] + v
            return 0
        lax.fori_loop(0, 4, body, 0)

    def hp():
        def body(q, _):
            m = q // 8
            r = pl.ds(pl.multiple_of((q % 8) * RH, RH), RH)
            a = XB[m // PAIR, m % PAIR, r, :]
            b = XS[m, r, :]
            sig = jax.nn.sigmoid(a)
            sa = a * sig
            XB[m // PAIR, m % PAIR, r, :] = b * sig * (1.0 + a * (1.0 - sig))
            XS[m, r, :] = sa
            B[0, 0, pl.ds(pl.multiple_of(q * RH, RH), RH), :] = (sa * b).astype(BF)
            return 0
        lax.fori_loop(0, RH, body, 0)
        bp[0].start()
        u_put.start()
        v_put.start()

    u_put = pltpu.make_async_copy(XB.at[pl.ds(0, 2)], U, s_one.at[0])
    v_put = pltpu.make_async_copy(XS.at[pl.ds(0, 4)], V, s_one.at[2])

    def ld_g(t):
        d, o = order[t]
        s = t % RING
        ii = blk(t)
        src = wd_ref if t == 0 else wdf.at[ii]
        return [pltpu.make_async_copy(xd.at[1, :, pl.ds(pl.multiple_of(ii * CB, CB), CB)], a_slot(t), s_c.at[s, 0]),
                pltpu.make_async_copy(src, WX.at[s % PAIR, s // PAIR, pl.ds(0, FB), pl.ds(0, CB)], s_c.at[s, 1])]

    def sg(t):
        have(2, *order[t])
        for l in ld_g(t):
            l.start()

    def gg(t):
        if t == 0:
            v_put.wait()
        for l in ld_g(t):
            l.wait()
        s = t % RING

        def body(m, _):
            r = pl.ds(pl.multiple_of(m * QB, QB), QB)
            v = lax.dot_general(A[s // PAIR, s % PAIR, r, :], WX[s % PAIR, s // PAIR, pl.ds(0, FB), pl.ds(0, CB)], NT, preferred_element_type=F32)
            if t == 0:
                XS[m] = v
            else:
                XS[m] += v
            return 0
        lax.fori_loop(0, 4, body, 0)

    def us_load(q, k):
        m = q // PAIR
        r = pl.ds(pl.multiple_of((q % PAIR) * FOUR, FOUR), FOUR)
        src = U.at[m // PAIR, m % PAIR, r, :] if k == 0 else V.at[m, r, :]
        return pltpu.make_async_copy(src, XS.at[4 + q % PAIR, pl.ds(FOUR * k, FOUR), :], s_us.at[q % PAIR])

    def dadb():
        for k in TWO:
            us_load(0, k).start()

        def body(q, _):
            @pl.when(q < 7)
            def _():
                for k in TWO:
                    us_load(q + 1, k).start()
            wait(XS.at[4 + q % PAIR], s_us.at[q % PAIR])

            def inner(e, _):
                g = XS[q // PAIR, pl.ds(pl.multiple_of((q % PAIR) * FOUR + e * RH, RH), RH), :]
                o = pl.ds(pl.multiple_of(q * FOUR + e * RH, RH), RH)
                for k in TWO:
                    B[1 + k, 0, o, :] = (g * XS[4 + q % PAIR, pl.ds(pl.multiple_of(FOUR * k + e * RH, RH), RH), :]).astype(BF)
                return 0
            lax.fori_loop(0, 4, inner, 0)
            return 0
        lax.fori_loop(0, 8, body, 0)
        bp[1].start()
        bp[2].start()

    def chunk(idx):
        return (x + 6 - idx) % RING

    bp = [remote(B.at[k, 0], B.at[k, 1], s_b, r_b.at[k], "pc") for k in range(3)]

    def ap(arr, idx):
        return remote(xd.at[arr, :, pl.ds(pl.multiple_of(TG * chunk(idx) + CB * c1, CB), CB)], AP.at[arr, idx], s_ap, r_ap.at[arr, idx], "pc")

    seq = (0, 1, 3, 2)

    def load_a(k, n):
        arr = 1 - min(k, 1)
        idx = seq[n]
        return (pltpu.make_async_copy(xd.at[arr, :, pl.ds(pl.multiple_of(TG * chunk(idx) + CB * c, CB), CB)], A.at[n % PAIR, 0], s_a.at[n % PAIR]),
                pltpu.make_async_copy(AP.at[arr, idx], A.at[n % PAIR, 1], s_a.at[n % PAIR]))

    def start_a(k, n):
        if k < UP:
            ap(1 - k, seq[n]).wait_recv()
        for l in load_a(k, n):
            l.start()

    def dot_x(k, n, split=False):
        slot = n % PAIR
        wait(A.at[slot], s_a.at[slot])

        def body(m, _):
            cols = pl.ds(pl.multiple_of(m * QB, QB), QB)
            to = (XB.at[0, m], XB.at[1, m], XB.at[2, m], dw.at[k, m])[n]
            to[...] = (lax.dot_general(A[slot, 0, :, cols], B[k, 0], TN, preferred_element_type=F32)
                             + lax.dot_general(A[slot, 1, :, cols], B[k, 1], TN, preferred_element_type=F32))
            return 0

        if split:
            for m in TWO:
                body(m, 0)
                xmsg(k, m).start()
        else:
            lax.fori_loop(0, 2, body, 0)

    def xmsg(k, t):
        src = (XB.at[0, 0], XB.at[0, 1], XB.at[1, 1], XB.at[2, 0], XB.at[1, 0], XB.at[2, 1])[t]
        dst = du.at[t - 4] if k == UP and t >= 4 else XR.at[k, t]
        return remote(src, dst, s_xs.at[min(t // PAIR, 1)], r_xs.at[k, t // PAIR], ("xp", "xm")[t % PAIR])

    def xl(k, n):
        start_a(k, n)

    def x1(k):
        bp[k].wait_recv()
        if k == 0:
            u_put.wait()
        else:
            wait(XB.at[0], s_xs.at[0])
        dot_x(k, 0, True)

    def x2(k):
        if k > 0:
            wait(XB.at[pl.ds(0, 2)], s_xs.at[1])
        dot_x(k, 1)
        start_a(k, 3)
        xmsg(k, 2).start()
        dot_x(k, 2)
        if k == 1:
            start_a(2, 0)
        xmsg(k, 3).start()

    def x2o(k):
        dot_x(k, 3)
        if k == 1:
            start_a(2, 1)

    def xstage(k, t, slot):
        return pltpu.make_async_copy(XR.at[k, t], XS.at[4 + slot], s_one.at[1])

    def x3(k):
        wait(XS.at[pl.ds(4, 2)], r_xs.at[k, 0])
        for t in TWO:
            xstage(k, t, t).start()
        wait(XS.at[pl.ds(4, 2)], s_one.at[1])
        for t in TWO:
            add(XB.at[1 + t, t], XS.at[4 + t], QB)
            xmsg(k, 4 + t).start()

    def xadd(k, ts):
        wait(XS.at[pl.ds(4, 2)], r_xs.at[k, ts[0] // PAIR])
        for h, t in enumerate(ts):
            xstage(k, t, h).start()
        wait(XS.at[pl.ds(4, 2)], s_one.at[1])
        for h, t in enumerate(ts):
            add(dw.at[k, h], XS.at[4 + h], QB)

    def xfa(k):
        xadd(k, (3, 2))

    def xfb(k):
        xadd(k, (4, 5))

    def pair(n, col):
        return ((0, 3), (1, 2))[col][n % PAIR]

    def lw(n):
        if n < 2:
            for col in TWO:
                have(2, pair(n, col), 0)
                have(2, pair(n, col), 1)
        out = []
        for col in TWO:
            d = pair(n, col)
            q = xpos[d]
            if n < 2:
                if d == 0:
                    out.append(pltpu.make_async_copy(wd_ref, WD.at[col, c], s_w.at[n // PAIR]))
                    out.append(pltpu.make_async_copy(wdf.at[2 * x + c1], WD.at[col, c1], s_w.at[n // PAIR]))
                else:
                    out.append(pltpu.make_async_copy(wdf.at[pl.ds(2 * q, 2)], WD.at[col], s_w.at[n // PAIR]))
            else:
                for k in TWO:
                    full = (wgf, wuf)[k]
                    if d == 0:
                        out.append(pltpu.make_async_copy(w_in[k], WX.at[col, k, pl.ds(pl.multiple_of(CB * c, CB), CB), :], s_w.at[n // PAIR]))
                        out.append(pltpu.make_async_copy(full.at[pl.ds(pl.multiple_of(TG * x + CB * c1, CB), CB), :],
                                                         WX.at[col, k, pl.ds(pl.multiple_of(CB * c1, CB), CB), :], s_w.at[n // PAIR]))
                    else:
                        out.append(pltpu.make_async_copy(full.at[pl.ds(pl.multiple_of(TG * q, TG), TG), :], WX.at[col, k], s_w.at[n // PAIR]))
        for o in out:
            o.start()

    def dots_z(n, lo, m):

        def body(q, _):
            col = q // m
            idx = lo + 2 * (q % m)
            p = z + col * (y - z)
            ch = (p + 6 - idx) % RING
            s1 = QB - 192 * col
            s2 = RW + 192 * col
            own = (idx // PAIR) * (1 - idx // 3)
            slot = idx + own * 2 * (n % PAIR)

            def lhs(k):
                return jnp.concatenate([B[k, 0, pl.ds(pl.multiple_of(ch * s1 + g * s2, RW), RW), :] for g in range(4)], axis=0)

            if n < 2:
                l = lhs(0)
                for h in TWO:
                    ZB[col, slot, h] = jnp.dot(l, WD[col, h], preferred_element_type=F32)
            else:
                l = lhs(1)
                u = lhs(2)
                for h in TWO:
                    r = pl.ds(CB * h, CB)
                    ZB[col, slot, h] = (lax.dot_general(l, WX[col, 0, r, :], NT, preferred_element_type=F32)
                                        + lax.dot_general(u, WX[col, 1, r, :], NT, preferred_element_type=F32))
            return 0
        lax.fori_loop(0, 2 * m, body, 0)

    def zmsg(n, col, t):
        src = ((0, 0), (0, 1), (1, 1), (3, 0), (1, 0), (3, 1))[t]
        return remote(ZB.at[col, src[0], src[1]], ZR.at[col, n, t], s_zs.at[min(t // PAIR, 1)], r_zs.at[n, t // PAIR], link[col][t % PAIR])

    def own(n, col, h):
        return ZB.at[col, 2 + 2 * (n % PAIR), h]

    def sub(n, col, h, d):
        s = (pos[col][1] + d) % RING
        return ZB.at[col, 2 + 2 * (n % PAIR), h, pl.ds(pl.multiple_of(s * RW, RW), RW), :]

    def msg2(n, col, t):
        h, d = ((0, 2), (1, 2), (1, 1), (0, 3), (0, 1), (1, 3))[t]
        return remote(sub(n, col, h, d), Z2.at[col, n, t], s_2.at[n % PAIR], r_2.at[n, min(t // PAIR, 1)], link[col][2 + t % PAIR])

    def p1(n):
        wait((WD, WX)[n // PAIR], s_w.at[n // PAIR])
        if n > 0:
            wait(ZB.at[0, pl.ds(0, 2)], s_zs.at[0])
        dots_z(n, 0, 1)
        for t in TWO:
            for col in TWO:
                zmsg(n, col, t).start()

    def p2(n):
        if n > 0:
            wait(ZB.at[0, pl.ds(0, 4)], s_zs.at[1])
        dots_z(n, 1, 2)
        for t in range(2, 4):
            for col in TWO:
                zmsg(n, col, t).start()

    def p2o(n):
        if n > 1:
            wait(Z2.at[0, pl.ds(0, 2)], s_2.at[n % PAIR])
        dots_z(n, 2, 1)

    def zstage(n, col, t, slot):
        return pltpu.make_async_copy(ZR.at[col, n, t], ZS.at[col, slot], s_one.at[3])

    def stage(n, ts):
        wait(ZS, r_zs.at[n, ts[0] // PAIR])
        for h, t in enumerate(ts):
            for col in TWO:
                zstage(n, col, t, h).start()
        wait(ZS, s_one.at[3])

    def p4(n):
        stage(n, (0, 1))
        for t in TWO:
            for col in TWO:
                add(ZB.at[col, (1, 3)[t], t], ZS.at[col, t], QB)
                zmsg(n, col, 4 + t).start()

    def zadd(n, ts):
        stage(n, ts)
        for h in TWO:
            for col in TWO:
                add(own(n, col, h), ZS.at[col, h], QB)

    def fa(n):
        zadd(n, (3, 2))

    def fb(n):
        zadd(n, (4, 5))
        for t in range(4):
            for col in TWO:
                msg2(n, col, t).start()

    def hh(n):
        wait(Z2.at[0, 0, pl.ds(0, 4)], r_2.at[n, 0])
        for t in TWO:
            for col in TWO:
                add(sub(n, col, t, (1, 3)[t]), Z2.at[col, n, t], RW)
                msg2(n, col, 4 + t).start()

    done = []

    def zf(n):
        a = n // PAIR
        if not done:
            for g in (AX, AD, AE):
                wait(some(g, 960), s_g.at[g])
        done.append(n)
        wait(Z2.at[:, 0, pl.ds(0, 4)], r_2.at[n, 1])
        for col in TWO:
            q = xpos[pair(n, col)]
            for h, ts in ((0, (3, 4)), (1, (2, 5))):
                cs = pl.ds(pl.multiple_of(TG * q + CB * h, CB), CB)
                v = sub(n, col, h, 0)[...] + Z2[col, n, ts[0]] + Z2[col, n, ts[1]]
                yo[a, :, cs] = (yo[a, :, cs].astype(F32) + v).astype(BF)

    def enter():
        for d in dev.values():
            pl.semaphore_signal(barrier, inc=1, device_id=d, device_id_type=MESH)
        pl.semaphore_wait(barrier, len(dev))

    own_ld = [pltpu.make_async_copy(r, yo.at[k], s_one.at[4]) for k, r in enumerate((x_ref, dy_ref))]
    for l in own_ld:
        l.start()
    barrier = pltpu.get_barrier_semaphore()
    enter()
    wait(yo, s_one.at[4])
    put = pltpu.make_async_copy(yo, xd.at[:, pl.ds(pl.multiple_of(j * RW, RW), RW), :], s_one.at[5])
    put.start()
    ga(AX)
    gb0(AX)
    ga(AD)
    wpc(WL)
    wpc(WU)
    wpc(WG)
    wown(WG)
    ga2(AX)
    gf(AX, OWN)
    gb31(AX)
    wown(WU)
    ga2(AD)
    gb2(AX)
    wf(WG)
    gf(AX, PREV)
    gf(AX, NEXT)
    gf(AX, OPP)
    ga(AE)
    gb31(AD)
    wf(WU)
    gb0(AD)
    gend(AX)
    sab(B2)
    sab(B1)
    sab(B0)
    ab(B0)
    wown(WL)
    ab(B1)
    gb2(AD)
    sab(B3)
    gf(AD, PREV)
    sab(B4)
    ga2(AE)
    wf2(WG)
    ab(B2)
    gb0(AE)
    wf2(WU)
    gf(AD, OWN)
    ab(B3)
    sab(B6)
    gf(AD, NEXT)
    gf(AD, OPP)
    sab(B5)
    ab(B4)
    sab(B7)
    gb2(AE)
    ab(B5)
    gb31(AE)
    gf(AE, OWN)
    ab(B6)
    wf(WL)
    ab(B7)
    gend(AD)
    hp()
    xl(DOWN, A0)
    gf(AE, PREV)
    wfp()
    gf(AE, NEXT)
    gf(AE, OPP)
    x1(DOWN)
    lw(Y0)
    gend(AE)
    p1(Y0)
    xl(DOWN, A2)
    xl(DOWN, A1)
    wf2(WL)
    p2(Y0)
    x2(DOWN)
    x2o(DOWN)
    sg(B1)
    sg(B0)
    p2o(Y0)
    lw(Y1)
    gg(B0)
    sg(B4)
    sg(B3)
    gg(B1)
    sg(B2)
    p4(Y0)
    gg(B2)
    gg(B3)
    gg(B4)
    sg(B5)
    p1(Y1)
    x3(DOWN)
    sg(B6)
    gg(B5)
    gg(B6)
    sg(B7)
    p2(Y1)
    gg(B7)
    xl(GATE, A0)
    lw(X0)
    dadb()
    xfa(DOWN)
    p2o(Y1)
    xl(GATE, A1)
    x1(GATE)
    p4(Y1)
    fa(Y0)
    p1(X0)
    xl(GATE, A2)
    x2(GATE)
    fb(Y0)
    xfb(DOWN)
    x3(GATE)
    fa(Y1)
    x1(UP)
    fb(Y1)
    hh(Y0)
    x2o(GATE)
    p2(X0)
    zf(Y0)
    xl(UP, A2)
    p4(X0)
    p2o(X0)
    lw(X1)
    hh(Y1)
    p1(X1)
    xfa(GATE)
    x2(UP)
    fa(X0)
    p2(X1)
    p4(X1)
    xfb(GATE)
    x3(UP)
    zf(Y1)
    fb(X0)
    p2o(X1)
    x2o(UP)
    fa(X1)
    fb(X1)
    hh(X0)
    xfa(UP)
    hh(X1)
    zf(X0)
    zf(X1)
    def end():
        for k in (WG, WU, WL):
            wait(blocks(k, 7), s_v.at[k])
        wait(AP, s_ap)
        wait(B.at[:, 0], s_b)
        for q in TWO:
            wait(Z2.at[0, pl.ds(0, 2)], s_2.at[q])
            wait(ZB.at[0, pl.ds(0, 2 + 2 * q)], s_zs.at[q])
        wait(XB.at[0], s_xs.at[0])
        wait(XB.at[pl.ds(0, 2)], s_xs.at[1])
        wait(du, r_xs.at[2, 2])

    end()


def mlp(x, dy, wg, wu, wd):
    sd = jax.ShapeDtypeStruct
    dma = pltpu.SemaphoreType.DMA
    V = pltpu.VMEM
    o = pl.pallas_call(
        mlp_kernel,
        out_shape=(V((3, 2, QB, FB), F32), V((2, RW, DM), BF), V((2, QB, FB), F32),
                   sd((2, TG, DM), BF), sd((DM, FB), BF), sd((DM, FB), BF), sd((8, FB, CB), BF), sd((2, 2, QB, FB), F32), sd((4, QB, FB), F32),
                   sd((3, 6, QB, FB), F32), sd((2, 4, 6, QB, CB), F32), sd((2, 4, TG, CB), BF)),
        in_specs=[HBM] * 5,
        out_specs=(VMEM,) * 3 + (HBM,) * 9,
        scratch_shapes=[
            V((3, 2, TG, FB), BF), V((2, 2, TG, CB), BF), V((3, 2, QB, FB), F32), V((6, QB, FB), F32),
            V((2, 2, FB, CB), BF), V((2, 2, TG, FB), BF), V((2, 5, 2, QB, CB), F32), V((2, 2, QB, CB), F32),
            V((2, 4, 6, RW, CB), F32),
            dma((3,)), dma((3, 7)), dma((3,)), dma((3, 7)), dma, dma((2, 4)), dma, dma((3,)), dma((2,)), dma((3, 3)),
            dma((2,)), dma((4, 3)), dma((2,)), dma((4, 2)), dma((4, 2)), dma((2,)), dma((2,)), dma((2,)), dma((7,)),
        ],
        compiler_params=pltpu.CompilerParams(collective_id=1, has_side_effects=True, vmem_limit_bytes=58600000),
        name="mlp",
    )(x, dy, wg, wu, wd)
    return o[:3]


def place_kernel(dw, yo, du, y, dx, og, ou, od, bu, bt, sem):
    outs = [pltpu.make_async_copy(dw.at[1], og, sem.at[0]), pltpu.make_async_copy(yo.at[0], y, sem.at[1]), pltpu.make_async_copy(yo.at[1], dx, sem.at[2]),
            pltpu.make_async_copy(bu, ou, sem.at[3]), pltpu.make_async_copy(bt, od, sem.at[4])]
    for o in outs[:3]:
        o.start()
    for h in TWO:
        r = pl.ds(QB * h, QB)
        bu[r, :] = dw[2, r, :] + du[h]
    outs[3].start()
    for h in TWO:
        r = pl.ds(QB * h, QB)
        bt[:, r] = dw[0, r, :].T
    outs[4].start()
    for o in outs:
        o.wait()


def place(dw, yo, du):
    sd = jax.ShapeDtypeStruct
    V = pltpu.VMEM
    return pl.pallas_call(
        place_kernel,
        out_shape=(sd((RW, DM), BF), sd((RW, DM), BF), sd((CB, FB), F32), sd((CB, FB), F32), sd((FB, CB), F32)),
        in_specs=[VMEM] * 3,
        out_specs=(HBM,) * 5,
        scratch_shapes=[V((CB, FB), F32), V((FB, CB), F32), pltpu.SemaphoreType.DMA((5,))],
        compiler_params=pltpu.CompilerParams(vmem_limit_bytes=24 * 2**20),
        name="place",
    )(dw.reshape(3, CB, FB), yo, du)


def solution(mesh):
    rows = P(("dp", "tp"), None)
    wsp = P("dp", "tp")
    dsp = P("tp", "dp")

    def local(x, w_gate, w_up, w_down, dy):
        return place(*mlp(x, dy, w_gate, w_up, w_down))

    return jax.shard_map(local, mesh=mesh, in_specs=(rows, wsp, wsp, dsp, rows), out_specs=(rows, rows, wsp, wsp, dsp), check_vma=False)
```

```python
import jax
import jax.numpy as jnp
from jax import lax
from jax.experimental import pallas as pl
from jax.experimental.pallas import tpu as pltpu
from jax.sharding import PartitionSpec as P

MESH = pl.DeviceIdType.MESH
HBM = pl.BlockSpec(memory_space=pltpu.HBM)
VMEM = pl.BlockSpec(memory_space=pltpu.VMEM)
NT = (((1,), (1,)), ((), ()))
TN = (((0,), (0,)), ((), ()))
F32 = jnp.float32
BF = jnp.bfloat16
TWO = range(2)
RING = 4
PAIR = 2
HB = 448
FOUR = 128
DM, TG, FB, CB, QB, RW, RH = 4096, 1024, 896, 512, 256, 64, 32
AX, AD, AE = range(3)
OWN, NEXT, OPP, PREV = range(4)
WG, WU, WL = range(3)
DOWN, GATE, UP = range(3)
Y0, Y1, X0, X1 = range(4)
A0, A1, A2 = range(3)
B0, B1, B2, B3, B4, B5, B6, B7 = range(8)


def mlp_kernel(x_ref, dy_ref, wg_ref, wu_ref, wd_ref, dw, yo, du, xd, wgf, wuf, wdf, U, V, XR, ZR, AP,
               B, A, XB, XS, WD, WX, ZB, ZS, Z2,
               s_g, r_g, s_v, r_v, s_ap, r_ap, s_b, r_b, s_xs, r_xs, s_zs, r_zs, s_2, r_2, s_c, s_a, s_w, s_us, s_one, in_x, in_zy):
    i = lax.axis_index("dp")
    j = lax.axis_index("tp")
    x, c, z, y = i // PAIR, i % PAIR, j // 4, j % RING
    xp, xm, xq, c1 = (x + 1) % RING, (x + 3) % RING, (x + 2) % RING, 1 - c
    dev = {
        "xp": {"dp": 2 * xp + c}, "xm": {"dp": 2 * xm + c}, "pc": {"dp": 2 * x + c1},
        "yp": {"tp": 4 * z + (y + 1) % RING}, "ym": {"tp": 4 * z + (y + 3) % RING},
        "zp": {"tp": 4 * ((z + 1) % RING) + y}, "zm": {"tp": 4 * ((z + 3) % RING) + y},
    }
    pos = ((z, y), (y, z))
    link = (("zp", "zm", "yp", "ym"), ("yp", "ym", "zp", "zm"))

    def remote(src, dst, ss, rs, to):
        return pltpu.make_async_remote_copy(src_ref=src, dst_ref=dst, send_sem=ss, recv_sem=rs, device_id=dev[to], device_id_type=MESH)

    def wait(ref, sem):
        pltpu.make_async_copy(ref, ref, sem).wait()

    def add(dst, src, n):
        def body(r, _):
            s = pl.ds(pl.multiple_of(r * RH, RH), RH)
            dst[s, :] = dst[s, :] + src[s, :]
            return 0
        lax.fori_loop(0, n // RH, body, 0)

    def send(src, dst, to, ss, rs):
        remote(src, dst, ss, rs, to).start()

    def wblk(k, xx, cc, half=None):
        ii = 2 * xx + cc
        if k < 2:
            r = (wgf, wuf)[k]
            if half is None:
                return r.at[pl.ds(pl.multiple_of(ii * CB, CB), CB), :]
            return r.at[pl.ds(pl.multiple_of(ii * CB + half * QB, QB), QB), :]
        if half is None:
            return wdf.at[ii]
        return wdf.at[ii, pl.ds(half * HB, HB), :]

    ahead = xq // PAIR

    def cols(a):
        if a == AX:
            return slice(None)
        h = ahead if a == AD else 1 - ahead
        return pl.ds(pl.multiple_of(h * (DM // PAIR), DM // PAIR), DM // PAIR)

    def rows(a, col, s, p, lo=0, n=RH):
        zz, yy = (p, s) if col == 0 else (s, p)
        return xd.at[min(a, AD), pl.ds(pl.multiple_of((zz * 4 + yy) * RW + col * RH + lo, 16), n), cols(a)]

    def geo(col):
        sec, prim = pos[col]
        sp, sm, pp, pm = link[col]
        return prim, sec, pp, pm, sp, sm

    def some(a, n):
        return xd.at[min(a, AD), pl.ds(0, n), cols(a)]

    FIRST, ON, LAST = range(4, 7)

    def ga(a):
        for col in TWO:
            p, s, pp, pm, sp, sm = geo(col)
            src = yo.at[min(a, AD), pl.ds(col * RH, RH), cols(a)]
            for to in (pp, pm):
                send(src, rows(a, col, p, s), to, s_g.at[a], r_g.at[a, FIRST])

    def gb0(a):
        for col in TWO:
            p, s, pp, pm, sp, sm = geo(col)
            src = yo.at[min(a, AD), pl.ds(col * RH, RH), cols(a)]
            for to in (sp, sm):
                send(src, rows(a, col, p, s), to, s_g.at[a], r_g.at[a, OWN])

    def ga2(a):
        wait(some(a, FOUR), r_g.at[a, FIRST])
        for col in TWO:
            p, s, pp, pm, sp, sm = geo(col)
            for d, lo, to in ((PREV, 0, pp), (NEXT, 16, pm)):
                r = rows(a, col, (p + d) % RING, s, lo, 16)
                send(r, r, to, s_g.at[a], r_g.at[a, ON])

    def gb31(a):
        for col in TWO:
            p, s, pp, pm, sp, sm = geo(col)
            for d in (PREV, NEXT):
                r = rows(a, col, (p + d) % RING, s)
                for to in (sp, sm):
                    send(r, r, to, s_g.at[a], r_g.at[a, d])

    def gb2(a):
        wait(some(a, RW), r_g.at[a, ON])
        for col in TWO:
            p, s, pp, pm, sp, sm = geo(col)
            r = rows(a, col, (p + OPP) % RING, s)
            for to in (sp, sm):
                send(r, r, to, s_g.at[a], r_g.at[a, OPP])

    def gf(a, d):
        wait(some(a, FOUR), r_g.at[a, d])
        for col in TWO:
            p, s, pp, pm, sp, sm = geo(col)
            for e, lo, to in ((PREV, 0, sp), (NEXT, 16, sm)):
                r = rows(a, col, (p + d) % RING, (s + e) % RING, lo, 16)
                send(r, r, to, s_g.at[a], r_g.at[a, LAST])

    def gend(a):
        if a == AX:
            put.wait()
        wait(some(a, QB), r_g.at[a, LAST])
        for arr, idx in (((AX, 0), (AX, 1), (AX, 3), (AX, 2)), ((AD, 0),), ((AD, 1), (AD, 3), (AD, 2)))[a]:
            ap(arr, idx).start()

    w_in = (wg_ref, wu_ref, wd_ref)
    LATE = 6
    seen = set()

    def blocks(k, n):
        return wdf.at[pl.ds(0, n)] if k == WL else (wgf, wuf)[k].at[pl.ds(0, n * CB), :]

    def once(k, g, n):
        if (k, g) not in seen:
            seen.add((k, g))
            wait(blocks(k, n), r_v.at[k, g])

    def wpc(k):
        send(w_in[k], wblk(k, x, c), "pc", s_v.at[k], r_v.at[k, OWN])

    def wown(k):
        for fr, to in enumerate(("xp", "xm")):
            if k < WL:
                send(w_in[k], wblk(k, x, c), to, s_v.at[k], r_v.at[k, FIRST])
            else:
                send(wd_ref.at[pl.ds(fr * HB, HB), :], wblk(k, x, c, fr), to, s_v.at[k], r_v.at[k, FIRST])
        if k == WL:
            for fr, to in enumerate(("xp", "xm")):
                send(wd_ref.at[pl.ds((1 - fr) * HB, HB), :], wblk(k, x, c, 1 - fr), to, s_v.at[k], r_v.at[k, LATE])

    def wf(k):
        once(k, FIRST, 1 if k == WL else 2)
        for xx, d, half, to in ((xm, PREV, 0, "xp"), (xp, NEXT, 1, "xm")):
            r = wblk(k, xx, c, half)
            send(r, r, to, s_v.at[k], r_v.at[k, ON])
            if k < WL:
                r = wblk(k, xx, c)
                send(r, r, "pc", s_v.at[k], r_v.at[k, d])

    def wfp():
        once(WL, LATE, 1)
        for xx, d in ((xm, PREV), (xp, NEXT)):
            r = wblk(WL, xx, c)
            send(r, r, "pc", s_v.at[WL], r_v.at[WL, d])

    def wf2(k):
        once(k, ON, 1)
        for half in TWO:
            r = wblk(k, xq, c, half)
            send(r, r, "pc", s_v.at[k], r_v.at[k, OPP])

    def have(k, d, o):
        if o == 1:
            once(k, d, 1)
        elif d == OPP:
            once(k, ON, 1)
        elif d:
            once(k, FIRST, 1 if k == WL else 2)
            if k == WL:
                once(k, LATE, 1)

    xpos = {0: x, 1: xp, 2: xq, 3: xm}
    order = ((0, 0), (0, 1), (3, 0), (1, 0), (3, 1), (1, 1), (2, 0), (2, 1))

    def blk(t):
        d, o = order[t]
        return 2 * xpos[d] + (c if o == 0 else c1)

    def a_slot(t):
        s = t % RING
        return A.at[s // PAIR, s % PAIR]

    def ld_ab(t):
        d, o = order[t]
        s = t % RING
        ii = blk(t)
        out = [pltpu.make_async_copy(xd.at[0, :, pl.ds(pl.multiple_of(ii * CB, CB), CB)], a_slot(t), s_c.at[s, 0])]
        for k in TWO:
            src = w_in[k] if t == 0 else wblk(k, xpos[d], c if o == 0 else c1)
            out.append(pltpu.make_async_copy(src, WX.at[s % PAIR, k, pl.ds((s // PAIR) * CB, CB), :], s_c.at[s, 1]))
        return out

    def sab(t):
        for k in TWO:
            have(k, *order[t])
        for l in ld_ab(t):
            l.start()

    def ab(t):
        s = t % RING
        wait(a_slot(t), s_c.at[s, 0])
        wait(WX.at[s % PAIR, :, pl.ds((s // PAIR) * CB, CB), :], s_c.at[s, 1])

        def body(m, _):
            r = pl.ds(pl.multiple_of(m * QB, QB), QB)
            lhs = A[s // PAIR, s % PAIR, r, :]
            for k in TWO:
                v = jnp.dot(lhs, WX[s % PAIR, k, pl.ds((s // PAIR) * CB, CB), :], preferred_element_type=F32)
                to = XB.at[m // PAIR, m % PAIR] if k == WG else XS.at[m]
                to[...] = v if t == 0 else to[...] + v
            return 0
        lax.fori_loop(0, 4, body, 0)

    def hp():
        def body(q, _):
            m = q // 8
            r = pl.ds(pl.multiple_of((q % 8) * RH, RH), RH)
            a = XB[m // PAIR, m % PAIR, r, :]
            b = XS[m, r, :]
            sig = jax.nn.sigmoid(a)
            sa = a * sig
            XB[m // PAIR, m % PAIR, r, :] = b * sig * (1.0 + a * (1.0 - sig))
            XS[m, r, :] = sa
            B[0, 0, pl.ds(pl.multiple_of(q * RH, RH), RH), :] = (sa * b).astype(BF)
            return 0
        lax.fori_loop(0, RH, body, 0)
        bp[0].start()
        u_put.start()
        v_put.start()

    u_put = pltpu.make_async_copy(XB.at[pl.ds(0, 2)], U, s_one.at[0])
    v_put = pltpu.make_async_copy(XS.at[pl.ds(0, 4)], V, s_one.at[2])

    def ld_g(t):
        d, o = order[t]
        s = t % RING
        ii = blk(t)
        src = wd_ref if t == 0 else wdf.at[ii]
        return [pltpu.make_async_copy(xd.at[1, :, pl.ds(pl.multiple_of(ii * CB, CB), CB)], a_slot(t), s_c.at[s, 0]),
                pltpu.make_async_copy(src, WX.at[s % PAIR, s // PAIR, pl.ds(0, FB), pl.ds(0, CB)], s_c.at[s, 1])]

    def sg(t):
        have(2, *order[t])
        for l in ld_g(t):
            l.start()

    def gg(t):
        if t == 0:
            v_put.wait()
        for l in ld_g(t):
            l.wait()
        s = t % RING

        def body(m, _):
            r = pl.ds(pl.multiple_of(m * QB, QB), QB)
            v = lax.dot_general(A[s // PAIR, s % PAIR, r, :], WX[s % PAIR, s // PAIR, pl.ds(0, FB), pl.ds(0, CB)], NT, preferred_element_type=F32)
            if t == 0:
                XS[m] = v
            else:
                XS[m] += v
            return 0
        lax.fori_loop(0, 4, body, 0)

    def us_load(q, k):
        m = q // PAIR
        r = pl.ds(pl.multiple_of((q % PAIR) * FOUR, FOUR), FOUR)
        src = U.at[m // PAIR, m % PAIR, r, :] if k == 0 else V.at[m, r, :]
        return pltpu.make_async_copy(src, XS.at[4 + q % PAIR, pl.ds(FOUR * k, FOUR), :], s_us.at[q % PAIR])

    def dadb():
        for k in TWO:
            us_load(0, k).start()

        def body(q, _):
            @pl.when(q < 7)
            def _():
                for k in TWO:
                    us_load(q + 1, k).start()
            wait(XS.at[4 + q % PAIR], s_us.at[q % PAIR])

            def inner(e, _):
                g = XS[q // PAIR, pl.ds(pl.multiple_of((q % PAIR) * FOUR + e * RH, RH), RH), :]
                o = pl.ds(pl.multiple_of(q * FOUR + e * RH, RH), RH)
                for k in TWO:
                    B[1 + k, 0, o, :] = (g * XS[4 + q % PAIR, pl.ds(pl.multiple_of(FOUR * k + e * RH, RH), RH), :]).astype(BF)
                return 0
            lax.fori_loop(0, 4, inner, 0)
            return 0
        lax.fori_loop(0, 8, body, 0)
        bp[1].start()
        bp[2].start()

    def chunk(idx):
        return (x + 6 - idx) % RING

    bp = [remote(B.at[k, 0], B.at[k, 1], s_b, r_b.at[k], "pc") for k in range(3)]

    def ap(arr, idx):
        return remote(xd.at[arr, :, pl.ds(pl.multiple_of(TG * chunk(idx) + CB * c1, CB), CB)], AP.at[arr, idx], s_ap, r_ap.at[arr, idx], "pc")

    seq = (0, 1, 3, 2)

    def load_a(k, n):
        arr = 1 - min(k, 1)
        idx = seq[n]
        return (pltpu.make_async_copy(xd.at[arr, :, pl.ds(pl.multiple_of(TG * chunk(idx) + CB * c, CB), CB)], A.at[n % PAIR, 0], s_a.at[n % PAIR]),
                pltpu.make_async_copy(AP.at[arr, idx], A.at[n % PAIR, 1], s_a.at[n % PAIR]))

    def start_a(k, n):
        if k < UP:
            ap(1 - k, seq[n]).wait_recv()
        for l in load_a(k, n):
            l.start()

    def dot_x(k, n, split=False):
        slot = n % PAIR
        wait(A.at[slot], s_a.at[slot])

        def body(m, _):
            cols = pl.ds(pl.multiple_of(m * QB, QB), QB)
            to = (XB.at[0, m], XB.at[1, m], XB.at[2, m], dw.at[k, m])[n]
            to[...] = (lax.dot_general(A[slot, 0, :, cols], B[k, 0], TN, preferred_element_type=F32)
                             + lax.dot_general(A[slot, 1, :, cols], B[k, 1], TN, preferred_element_type=F32))
            return 0

        if split:
            for m in TWO:
                body(m, 0)
                xmsg(k, m).start()
        else:
            lax.fori_loop(0, 2, body, 0)

    def xmsg(k, t):
        src = (XB.at[0, 0], XB.at[0, 1], XB.at[1, 1], XB.at[2, 0], XB.at[1, 0], XB.at[2, 1])[t]
        dst = du.at[t - 4] if k == UP and t >= 4 else XR.at[k, t]
        return remote(src, dst, s_xs.at[min(t // PAIR, 1)], r_xs.at[k, t // PAIR], ("xp", "xm")[t % PAIR])

    def xl(k, n):
        start_a(k, n)

    def x1(k):
        bp[k].wait_recv()
        if k == 0:
            u_put.wait()
        else:
            wait(XB.at[0], s_xs.at[0])
        dot_x(k, 0, True)

    def x2(k):
        if k > 0:
            wait(XB.at[pl.ds(0, 2)], s_xs.at[1])
        dot_x(k, 1)
        start_a(k, 3)
        xmsg(k, 2).start()
        dot_x(k, 2)
        if k == 1:
            start_a(2, 0)
        xmsg(k, 3).start()

    def x2o(k):
        dot_x(k, 3)
        if k == 1:
            start_a(2, 1)

    def xstage(k, t, slot):
        return pltpu.make_async_copy(XR.at[k, t], XS.at[4 + slot], s_one.at[1])

    def x3(k):
        wait(XS.at[pl.ds(4, 2)], r_xs.at[k, 0])
        for t in TWO:
            xstage(k, t, t).start()
        wait(XS.at[pl.ds(4, 2)], s_one.at[1])
        for t in TWO:
            add(XB.at[1 + t, t], XS.at[4 + t], QB)
            xmsg(k, 4 + t).start()

    def xadd(k, ts):
        wait(XS.at[pl.ds(4, 2)], r_xs.at[k, ts[0] // PAIR])
        for h, t in enumerate(ts):
            xstage(k, t, h).start()
        wait(XS.at[pl.ds(4, 2)], s_one.at[1])
        for h, t in enumerate(ts):
            add(dw.at[k, h], XS.at[4 + h], QB)

    def xfa(k):
        xadd(k, (3, 2))

    def xfb(k):
        xadd(k, (4, 5))

    def pair(n, col):
        return ((0, 3), (1, 2))[col][n % PAIR]

    def lw(n):
        if n < 2:
            for col in TWO:
                have(2, pair(n, col), 0)
                have(2, pair(n, col), 1)
        out = []
        for col in TWO:
            d = pair(n, col)
            q = xpos[d]
            if n < 2:
                if d == 0:
                    out.append(pltpu.make_async_copy(wd_ref, WD.at[col, c], s_w.at[n // PAIR]))
                    out.append(pltpu.make_async_copy(wdf.at[2 * x + c1], WD.at[col, c1], s_w.at[n // PAIR]))
                else:
                    out.append(pltpu.make_async_copy(wdf.at[pl.ds(2 * q, 2)], WD.at[col], s_w.at[n // PAIR]))
            else:
                for k in TWO:
                    full = (wgf, wuf)[k]
                    if d == 0:
                        out.append(pltpu.make_async_copy(w_in[k], WX.at[col, k, pl.ds(pl.multiple_of(CB * c, CB), CB), :], s_w.at[n // PAIR]))
                        out.append(pltpu.make_async_copy(full.at[pl.ds(pl.multiple_of(TG * x + CB * c1, CB), CB), :],
                                                         WX.at[col, k, pl.ds(pl.multiple_of(CB * c1, CB), CB), :], s_w.at[n // PAIR]))
                    else:
                        out.append(pltpu.make_async_copy(full.at[pl.ds(pl.multiple_of(TG * q, TG), TG), :], WX.at[col, k], s_w.at[n // PAIR]))
        for o in out:
            o.start()

    def dots_z(n, lo, m):

        def body(q, _):
            col = q // m
            idx = lo + 2 * (q % m)
            p = z + col * (y - z)
            ch = (p + 6 - idx) % RING
            s1 = QB - 192 * col
            s2 = RW + 192 * col
            own = (idx // PAIR) * (1 - idx // 3)
            slot = idx + own * 2 * (n % PAIR)

            def lhs(k):
                return jnp.concatenate([B[k, 0, pl.ds(pl.multiple_of(ch * s1 + g * s2, RW), RW), :] for g in range(4)], axis=0)

            if n < 2:
                l = lhs(0)
                for h in TWO:
                    ZB[col, slot, h] = jnp.dot(l, WD[col, h], preferred_element_type=F32)
            else:
                l = lhs(1)
                u = lhs(2)
                for h in TWO:
                    r = pl.ds(CB * h, CB)
                    ZB[col, slot, h] = (lax.dot_general(l, WX[col, 0, r, :], NT, preferred_element_type=F32)
                                        + lax.dot_general(u, WX[col, 1, r, :], NT, preferred_element_type=F32))
            return 0
        lax.fori_loop(0, 2 * m, body, 0)

    def zmsg(n, col, t):
        src = ((0, 0), (0, 1), (1, 1), (3, 0), (1, 0), (3, 1))[t]
        return remote(ZB.at[col, src[0], src[1]], ZR.at[col, n, t], s_zs.at[min(t // PAIR, 1)], r_zs.at[n, t // PAIR], link[col][t % PAIR])

    def own(n, col, h):
        return ZB.at[col, 2 + 2 * (n % PAIR), h]

    def sub(n, col, h, d):
        s = (pos[col][1] + d) % RING
        return ZB.at[col, 2 + 2 * (n % PAIR), h, pl.ds(pl.multiple_of(s * RW, RW), RW), :]

    def msg2(n, col, t):
        h, d = ((0, 2), (1, 2), (1, 1), (0, 3), (0, 1), (1, 3))[t]
        return remote(sub(n, col, h, d), Z2.at[col, n, t], s_2.at[n % PAIR], r_2.at[n, min(t // PAIR, 1)], link[col][2 + t % PAIR])

    def p1(n):
        wait((WD, WX)[n // PAIR], s_w.at[n // PAIR])
        if n > 0:
            wait(ZB.at[0, pl.ds(0, 2)], s_zs.at[0])
        dots_z(n, 0, 1)
        for t in TWO:
            for col in TWO:
                zmsg(n, col, t).start()

    def p2(n):
        if n > 0:
            wait(ZB.at[0, pl.ds(0, 4)], s_zs.at[1])
        dots_z(n, 1, 2)
        for t in range(2, 4):
            for col in TWO:
                zmsg(n, col, t).start()

    def p2o(n):
        if n > 1:
            wait(Z2.at[0, pl.ds(0, 2)], s_2.at[n % PAIR])
        dots_z(n, 2, 1)

    def zstage(n, col, t, slot):
        return pltpu.make_async_copy(ZR.at[col, n, t], ZS.at[col, slot], s_one.at[3])

    def stage(n, ts):
        wait(ZS, r_zs.at[n, ts[0] // PAIR])
        for h, t in enumerate(ts):
            for col in TWO:
                zstage(n, col, t, h).start()
        wait(ZS, s_one.at[3])

    def p4(n):
        stage(n, (0, 1))
        for t in TWO:
            for col in TWO:
                add(ZB.at[col, (1, 3)[t], t], ZS.at[col, t], QB)
                zmsg(n, col, 4 + t).start()

    def zadd(n, ts):
        stage(n, ts)
        for h in TWO:
            for col in TWO:
                add(own(n, col, h), ZS.at[col, h], QB)

    def fa(n):
        zadd(n, (3, 2))

    def fb(n):
        zadd(n, (4, 5))
        for t in range(4):
            for col in TWO:
                msg2(n, col, t).start()

    def hh(n):
        wait(Z2.at[0, 0, pl.ds(0, 4)], r_2.at[n, 0])
        for t in TWO:
            for col in TWO:
                add(sub(n, col, t, (1, 3)[t]), Z2.at[col, n, t], RW)
                msg2(n, col, 4 + t).start()

    done = []

    def zf(n):
        a = n // PAIR
        if not done:
            for g in (AX, AD, AE):
                wait(some(g, 960), s_g.at[g])
        done.append(n)
        wait(Z2.at[:, 0, pl.ds(0, 4)], r_2.at[n, 1])
        for col in TWO:
            q = xpos[pair(n, col)]
            for h, ts in ((0, (3, 4)), (1, (2, 5))):
                cs = pl.ds(pl.multiple_of(TG * q + CB * h, CB), CB)
                v = sub(n, col, h, 0)[...] + Z2[col, n, ts[0]] + Z2[col, n, ts[1]]
                yo[a, :, cs] = (yo[a, :, cs].astype(F32) + v).astype(BF)

    odd = (x + c + y + z) % PAIR
    along = ("xp", "xm", "pc")
    across = ("yp", "ym", "zp", "zm")

    def tell(sem, names):
        for d in names:
            pl.semaphore_signal(sem, inc=1, device_id=dev[d], device_id_type=MESH)

    def enter():
        @pl.when(odd == 0)
        def _():
            tell(barrier, across)
            pl.semaphore_wait(barrier, len(along))
            tell(in_x, along)

        @pl.when(odd == 1)
        def _():
            tell(barrier, along)
            pl.semaphore_wait(in_x, len(along))

    def enter_zy():
        @pl.when(odd == 0)
        def _():
            pl.semaphore_wait(in_zy, len(across))

        @pl.when(odd == 1)
        def _():
            pl.semaphore_wait(barrier, len(across))
            tell(in_zy, across)

    own_ld = [pltpu.make_async_copy(r, yo.at[k], s_one.at[4]) for k, r in enumerate((x_ref, dy_ref))]
    for l in own_ld:
        l.start()
    barrier = pltpu.get_barrier_semaphore()
    enter()
    put = pltpu.make_async_copy(yo, xd.at[:, pl.ds(pl.multiple_of(j * RW, RW), RW), :], s_one.at[5])
    wown(WG)
    wown(WU)
    wpc(WG)
    wpc(WU)
    wpc(WL)
    wait(yo, s_one.at[4])
    put.start()
    enter_zy()
    ga(AX)
    gb0(AX)
    ga(AD)
    ga2(AX)
    gf(AX, OWN)
    gb31(AX)
    ga2(AD)
    gb2(AX)
    wf(WG)
    gf(AX, PREV)
    gf(AX, NEXT)
    gf(AX, OPP)
    ga(AE)
    gb31(AD)
    wf(WU)
    gb0(AD)
    gend(AX)
    sab(B2)
    sab(B1)
    sab(B0)
    ab(B0)
    wown(WL)
    ab(B1)
    gb2(AD)
    sab(B3)
    gf(AD, PREV)
    sab(B4)
    ga2(AE)
    wf2(WG)
    ab(B2)
    gb0(AE)
    wf2(WU)
    gf(AD, OWN)
    ab(B3)
    sab(B6)
    gf(AD, NEXT)
    gf(AD, OPP)
    sab(B5)
    ab(B4)
    sab(B7)
    gb2(AE)
    ab(B5)
    gb31(AE)
    gf(AE, OWN)
    ab(B6)
    wf(WL)
    ab(B7)
    gend(AD)
    hp()
    xl(DOWN, A0)
    gf(AE, PREV)
    wfp()
    gf(AE, NEXT)
    gf(AE, OPP)
    x1(DOWN)
    lw(Y0)
    gend(AE)
    p1(Y0)
    xl(DOWN, A2)
    xl(DOWN, A1)
    wf2(WL)
    p2(Y0)
    x2(DOWN)
    x2o(DOWN)
    sg(B1)
    sg(B0)
    p2o(Y0)
    lw(Y1)
    gg(B0)
    sg(B4)
    sg(B3)
    gg(B1)
    sg(B2)
    p4(Y0)
    gg(B2)
    gg(B3)
    gg(B4)
    sg(B5)
    p1(Y1)
    x3(DOWN)
    sg(B6)
    gg(B5)
    gg(B6)
    sg(B7)
    p2(Y1)
    gg(B7)
    xl(GATE, A0)
    lw(X0)
    dadb()
    xfa(DOWN)
    p2o(Y1)
    xl(GATE, A1)
    x1(GATE)
    p4(Y1)
    fa(Y0)
    p1(X0)
    xl(GATE, A2)
    x2(GATE)
    fb(Y0)
    xfb(DOWN)
    x3(GATE)
    fa(Y1)
    x1(UP)
    fb(Y1)
    hh(Y0)
    x2o(GATE)
    p2(X0)
    zf(Y0)
    xl(UP, A2)
    p4(X0)
    p2o(X0)
    lw(X1)
    hh(Y1)
    p1(X1)
    xfa(GATE)
    x2(UP)
    fa(X0)
    p2(X1)
    p4(X1)
    xfb(GATE)
    x3(UP)
    zf(Y1)
    fb(X0)
    p2o(X1)
    x2o(UP)
    fa(X1)
    fb(X1)
    hh(X0)
    xfa(UP)
    hh(X1)
    zf(X0)
    zf(X1)
    def end():
        for k in (WG, WU, WL):
            wait(blocks(k, 7), s_v.at[k])
        wait(AP, s_ap)
        wait(B.at[:, 0], s_b)
        for q in TWO:
            wait(Z2.at[0, pl.ds(0, 2)], s_2.at[q])
            wait(ZB.at[0, pl.ds(0, 2 + 2 * q)], s_zs.at[q])
        wait(XB.at[0], s_xs.at[0])
        wait(XB.at[pl.ds(0, 2)], s_xs.at[1])
        wait(du, r_xs.at[2, 2])

    end()


def mlp(x, dy, wg, wu, wd):
    sd = jax.ShapeDtypeStruct
    dma = pltpu.SemaphoreType.DMA
    V = pltpu.VMEM
    o = pl.pallas_call(
        mlp_kernel,
        out_shape=(V((3, 2, QB, FB), F32), V((2, RW, DM), BF), V((2, QB, FB), F32),
                   sd((2, TG, DM), BF), sd((DM, FB), BF), sd((DM, FB), BF), sd((8, FB, CB), BF), sd((2, 2, QB, FB), F32), sd((4, QB, FB), F32),
                   sd((3, 6, QB, FB), F32), sd((2, 4, 6, QB, CB), F32), sd((2, 4, TG, CB), BF)),
        in_specs=[HBM] * 5,
        out_specs=(VMEM,) * 3 + (HBM,) * 9,
        scratch_shapes=[
            V((3, 2, TG, FB), BF), V((2, 2, TG, CB), BF), V((3, 2, QB, FB), F32), V((6, QB, FB), F32),
            V((2, 2, FB, CB), BF), V((2, 2, TG, FB), BF), V((2, 5, 2, QB, CB), F32), V((2, 2, QB, CB), F32),
            V((2, 4, 6, RW, CB), F32),
            dma((3,)), dma((3, 7)), dma((3,)), dma((3, 7)), dma, dma((2, 4)), dma, dma((3,)), dma((2,)), dma((3, 3)),
            dma((2,)), dma((4, 3)), dma((2,)), dma((4, 2)), dma((4, 2)), dma((2,)), dma((2,)), dma((2,)), dma((7,)),
            pltpu.SemaphoreType.REGULAR, pltpu.SemaphoreType.REGULAR,
        ],
        compiler_params=pltpu.CompilerParams(collective_id=1, has_side_effects=True, vmem_limit_bytes=58600000),
        name="mlp",
    )(x, dy, wg, wu, wd)
    return o[:3]


def place_kernel(dw, yo, du, y, dx, og, ou, od, bu, bt, sem):
    outs = [pltpu.make_async_copy(dw.at[1], og, sem.at[0]), pltpu.make_async_copy(yo.at[0], y, sem.at[1]), pltpu.make_async_copy(yo.at[1], dx, sem.at[2]),
            pltpu.make_async_copy(bu, ou, sem.at[3]), pltpu.make_async_copy(bt, od, sem.at[4])]
    for o in outs[:3]:
        o.start()
    for h in TWO:
        r = pl.ds(QB * h, QB)
        bu[r, :] = dw[2, r, :] + du[h]
    outs[3].start()
    for h in TWO:
        r = pl.ds(QB * h, QB)
        bt[:, r] = dw[0, r, :].T
    outs[4].start()
    for o in outs:
        o.wait()


def place(dw, yo, du):
    sd = jax.ShapeDtypeStruct
    V = pltpu.VMEM
    return pl.pallas_call(
        place_kernel,
        out_shape=(sd((RW, DM), BF), sd((RW, DM), BF), sd((CB, FB), F32), sd((CB, FB), F32), sd((FB, CB), F32)),
        in_specs=[VMEM] * 3,
        out_specs=(HBM,) * 5,
        scratch_shapes=[V((CB, FB), F32), V((FB, CB), F32), pltpu.SemaphoreType.DMA((5,))],
        compiler_params=pltpu.CompilerParams(vmem_limit_bytes=24 * 2**20),
        name="place",
    )(dw.reshape(3, CB, FB), yo, du)


def solution(mesh):
    rows = P(("dp", "tp"), None)
    wsp = P("dp", "tp")
    dsp = P("tp", "dp")

    def local(x, w_gate, w_up, w_down, dy):
        return place(*mlp(x, dy, w_gate, w_up, w_down))

    return jax.shard_map(local, mesh=mesh, in_specs=(rows, wsp, wsp, dsp, rows), out_specs=(rows, rows, wsp, wsp, dsp), check_vma=False)
```

```python
import jax
import jax.numpy as jnp
from jax import lax
from jax.experimental import pallas as pl
from jax.experimental.pallas import tpu as pltpu
from jax.sharding import PartitionSpec as P

MESH = pl.DeviceIdType.MESH
HBM = pl.BlockSpec(memory_space=pltpu.HBM)
VMEM = pl.BlockSpec(memory_space=pltpu.VMEM)
NT = (((1,), (1,)), ((), ()))
TN = (((0,), (0,)), ((), ()))
F32 = jnp.float32
BF = jnp.bfloat16
TWO = range(2)
RING = 4
PAIR = 2
HB = 448
FOUR = 128
DM, TG, FB, CB, QB, RW, RH = 4096, 1024, 896, 512, 256, 64, 32
AX, AD, AE = range(3)
OWN, NEXT, OPP, PREV = range(4)
WG, WU, WL = range(3)
DOWN, GATE, UP = range(3)
Y0, Y1, X0, X1 = range(4)
A0, A1, A2 = range(3)
B0, B1, B2, B3, B4, B5, B6, B7 = range(8)


def mlp_kernel(x_ref, dy_ref, wg_ref, wu_ref, wd_ref, dw, yo, du, xd, wgf, wuf, wdf, U, V, XR, ZR, AP,
               B, A, XB, XS, WD, WX, ZB, ZS, Z2,
               s_g, r_g, s_v, r_v, s_ap, r_ap, s_b, r_b, s_xs, s_zs, s_2, s_c, s_a, s_w, s_us, s_one, in_x, in_zy):
    i = lax.axis_index("dp")
    j = lax.axis_index("tp")
    x, c, z, y = i // PAIR, i % PAIR, j // 4, j % RING
    xp, xm, xq, c1 = (x + 1) % RING, (x + 3) % RING, (x + 2) % RING, 1 - c
    dev = {
        "xp": {"dp": 2 * xp + c}, "xm": {"dp": 2 * xm + c}, "pc": {"dp": 2 * x + c1},
        "yp": {"tp": 4 * z + (y + 1) % RING}, "ym": {"tp": 4 * z + (y + 3) % RING},
        "zp": {"tp": 4 * ((z + 1) % RING) + y}, "zm": {"tp": 4 * ((z + 3) % RING) + y},
    }
    pos = ((z, y), (y, z))
    link = (("zp", "zm", "yp", "ym"), ("yp", "ym", "zp", "zm"))

    def remote(src, dst, ss, rs, to):
        return pltpu.make_async_remote_copy(src_ref=src, dst_ref=dst, send_sem=ss, recv_sem=rs, device_id=dev[to], device_id_type=MESH)

    def wait(ref, sem):
        pltpu.make_async_copy(ref, ref, sem).wait()

    def r_x(k, t):
        return r_v.at[k, 4 + t // PAIR]

    def r_z(i):
        return r_g.at[i // 7, i % 7]

    def add(dst, src, n):
        def body(r, _):
            s = pl.ds(pl.multiple_of(r * RH, RH), RH)
            dst[s, :] = dst[s, :] + src[s, :]
            return 0
        lax.fori_loop(0, n // RH, body, 0)

    def send(src, dst, to, ss, rs):
        remote(src, dst, ss, rs, to).start()

    def wblk(k, xx, cc, half=None):
        ii = 2 * xx + cc
        if k < 2:
            r = (wgf, wuf)[k]
            if half is None:
                return r.at[pl.ds(pl.multiple_of(ii * CB, CB), CB), :]
            return r.at[pl.ds(pl.multiple_of(ii * CB + half * QB, QB), QB), :]
        if half is None:
            return wdf.at[ii]
        return wdf.at[ii, pl.ds(half * HB, HB), :]

    ahead = xq // PAIR

    def cols(a):
        if a == AX:
            return slice(None)
        h = ahead if a == AD else 1 - ahead
        return pl.ds(pl.multiple_of(h * (DM // PAIR), DM // PAIR), DM // PAIR)

    def rows(a, col, s, p, lo=0, n=RH):
        zz, yy = (p, s) if col == 0 else (s, p)
        return xd.at[min(a, AD), pl.ds(pl.multiple_of((zz * 4 + yy) * RW + col * RH + lo, 16), n), cols(a)]

    def geo(col):
        sec, prim = pos[col]
        sp, sm, pp, pm = link[col]
        return prim, sec, pp, pm, sp, sm

    def some(a, n):
        return xd.at[min(a, AD), pl.ds(0, n), cols(a)]

    FIRST, ON, LAST = range(4, 7)

    def ga(a):
        for col in TWO:
            p, s, pp, pm, sp, sm = geo(col)
            src = yo.at[min(a, AD), pl.ds(col * RH, RH), cols(a)]
            for to in (pp, pm):
                send(src, rows(a, col, p, s), to, s_g.at[a], r_g.at[a, FIRST])

    def gb0(a):
        for col in TWO:
            p, s, pp, pm, sp, sm = geo(col)
            src = yo.at[min(a, AD), pl.ds(col * RH, RH), cols(a)]
            for to in (sp, sm):
                send(src, rows(a, col, p, s), to, s_g.at[a], r_g.at[a, OWN])

    def ga2(a):
        wait(some(a, FOUR), r_g.at[a, FIRST])
        for col in TWO:
            p, s, pp, pm, sp, sm = geo(col)
            for d, lo, to in ((PREV, 0, pp), (NEXT, 16, pm)):
                r = rows(a, col, (p + d) % RING, s, lo, 16)
                send(r, r, to, s_g.at[a], r_g.at[a, ON])

    def gb31(a):
        for col in TWO:
            p, s, pp, pm, sp, sm = geo(col)
            for d in (PREV, NEXT):
                r = rows(a, col, (p + d) % RING, s)
                for to in (sp, sm):
                    send(r, r, to, s_g.at[a], r_g.at[a, d])

    def gb2(a):
        wait(some(a, RW), r_g.at[a, ON])
        for col in TWO:
            p, s, pp, pm, sp, sm = geo(col)
            r = rows(a, col, (p + OPP) % RING, s)
            for to in (sp, sm):
                send(r, r, to, s_g.at[a], r_g.at[a, OPP])

    def gf(a, d):
        wait(some(a, FOUR), r_g.at[a, d])
        for col in TWO:
            p, s, pp, pm, sp, sm = geo(col)
            for e, lo, to in ((PREV, 0, sp), (NEXT, 16, sm)):
                r = rows(a, col, (p + d) % RING, (s + e) % RING, lo, 16)
                send(r, r, to, s_g.at[a], r_g.at[a, LAST])

    def gend(a):
        if a == AX:
            put.wait()
        wait(some(a, QB), r_g.at[a, LAST])
        for arr, idx in (((AX, 0), (AX, 1), (AX, 3), (AX, 2)), ((AD, 0),), ((AD, 1), (AD, 3), (AD, 2)))[a]:
            ap(arr, idx).start()

    w_in = (wg_ref, wu_ref, wd_ref)
    LATE = 6
    seen = set()

    def blocks(k, n):
        return wdf.at[pl.ds(0, n)] if k == WL else (wgf, wuf)[k].at[pl.ds(0, n * CB), :]

    def once(k, g, n):
        if (k, g) not in seen:
            seen.add((k, g))
            wait(blocks(k, n), r_v.at[k, g])

    def wpc(k):
        send(w_in[k], wblk(k, x, c), "pc", s_v.at[k], r_v.at[k, OWN])

    def wown(k):
        for fr, to in enumerate(("xp", "xm")):
            if k < WL:
                send(w_in[k], wblk(k, x, c), to, s_v.at[k], r_v.at[k, FIRST])
            else:
                send(wd_ref.at[pl.ds(fr * HB, HB), :], wblk(k, x, c, fr), to, s_v.at[k], r_v.at[k, FIRST])
        if k == WL:
            for fr, to in enumerate(("xp", "xm")):
                send(wd_ref.at[pl.ds((1 - fr) * HB, HB), :], wblk(k, x, c, 1 - fr), to, s_v.at[k], r_v.at[k, LATE])

    def wf(k):
        once(k, FIRST, 1 if k == WL else 2)
        for xx, d, half, to in ((xm, PREV, 0, "xp"), (xp, NEXT, 1, "xm")):
            r = wblk(k, xx, c, half)
            send(r, r, to, s_v.at[k], r_v.at[k, ON])
            if k < WL:
                r = wblk(k, xx, c)
                send(r, r, "pc", s_v.at[k], r_v.at[k, d])

    def wfp():
        once(WL, LATE, 1)
        for xx, d in ((xm, PREV), (xp, NEXT)):
            r = wblk(WL, xx, c)
            send(r, r, "pc", s_v.at[WL], r_v.at[WL, d])

    def wf2(k):
        once(k, ON, 1)
        for half in TWO:
            r = wblk(k, xq, c, half)
            send(r, r, "pc", s_v.at[k], r_v.at[k, OPP])

    def have(k, d, o):
        if o == 1:
            once(k, d, 1)
        elif d == OPP:
            once(k, ON, 1)
        elif d:
            once(k, FIRST, 1 if k == WL else 2)
            if k == WL:
                once(k, LATE, 1)

    xpos = {0: x, 1: xp, 2: xq, 3: xm}
    order = ((0, 0), (0, 1), (3, 0), (1, 0), (3, 1), (1, 1), (2, 0), (2, 1))

    def blk(t):
        d, o = order[t]
        return 2 * xpos[d] + (c if o == 0 else c1)

    def a_slot(t):
        s = t % RING
        return A.at[s // PAIR, s % PAIR]

    def ld_ab(t):
        d, o = order[t]
        s = t % RING
        ii = blk(t)
        out = [pltpu.make_async_copy(xd.at[0, :, pl.ds(pl.multiple_of(ii * CB, CB), CB)], a_slot(t), s_c.at[s])]
        for k in TWO:
            src = w_in[k] if t == 0 else wblk(k, xpos[d], c if o == 0 else c1)
            out.append(pltpu.make_async_copy(src, WX.at[s % PAIR, k, pl.ds((s // PAIR) * CB, CB), :], s_c.at[s]))
        return out

    def sab(t):
        for k in TWO:
            have(k, *order[t])
        for l in ld_ab(t):
            l.start()

    def ab(t):
        s = t % RING
        wait(xd.at[0, pl.ds(0, 352)], s_c.at[s])

        def body(m, _):
            r = pl.ds(pl.multiple_of(m * QB, QB), QB)
            lhs = A[s // PAIR, s % PAIR, r, :]
            for k in TWO:
                v = jnp.dot(lhs, WX[s % PAIR, k, pl.ds((s // PAIR) * CB, CB), :], preferred_element_type=F32)
                to = XB.at[m // PAIR, m % PAIR] if k == WG else XS.at[m]
                to[...] = v if t == 0 else to[...] + v
            return 0
        lax.fori_loop(0, 4, body, 0)

    def hp():
        def body(q, _):
            m = q // 8
            r = pl.ds(pl.multiple_of((q % 8) * RH, RH), RH)
            a = XB[m // PAIR, m % PAIR, r, :]
            b = XS[m, r, :]
            sig = jax.nn.sigmoid(a)
            sa = a * sig
            XB[m // PAIR, m % PAIR, r, :] = b * sig * (1.0 + a * (1.0 - sig))
            XS[m, r, :] = sa
            B[0, 0, pl.ds(pl.multiple_of(q * RH, RH), RH), :] = (sa * b).astype(BF)
            return 0
        lax.fori_loop(0, RH, body, 0)
        bp[0].start()
        u_put.start()
        v_put.start()

    u_put = pltpu.make_async_copy(XB.at[pl.ds(0, 2)], U, s_one.at[0])
    v_put = pltpu.make_async_copy(XS.at[pl.ds(0, 4)], V, s_one.at[2])

    def ld_g(t):
        d, o = order[t]
        s = t % RING
        ii = blk(t)
        src = wd_ref if t == 0 else wdf.at[ii]
        return [pltpu.make_async_copy(xd.at[1, :, pl.ds(pl.multiple_of(ii * CB, CB), CB)], a_slot(t), s_c.at[s]),
                pltpu.make_async_copy(src, WX.at[s % PAIR, s // PAIR, pl.ds(0, FB), pl.ds(0, CB)], s_c.at[s])]

    def sg(t):
        have(2, *order[t])
        for l in ld_g(t):
            l.start()

    def gg(t):
        if t == 0:
            v_put.wait()
        s = t % RING
        wait(xd.at[1, pl.ds(0, 240)], s_c.at[s])

        def body(m, _):
            r = pl.ds(pl.multiple_of(m * QB, QB), QB)
            v = lax.dot_general(A[s // PAIR, s % PAIR, r, :], WX[s % PAIR, s // PAIR, pl.ds(0, FB), pl.ds(0, CB)], NT, preferred_element_type=F32)
            if t == 0:
                XS[m] = v
            else:
                XS[m] += v
            return 0
        lax.fori_loop(0, 4, body, 0)

    def us_load(q, k):
        m = q // PAIR
        r = pl.ds(pl.multiple_of((q % PAIR) * FOUR, FOUR), FOUR)
        src = U.at[m // PAIR, m % PAIR, r, :] if k == 0 else V.at[m, r, :]
        return pltpu.make_async_copy(src, XS.at[4 + q % PAIR, pl.ds(FOUR * k, FOUR), :], s_us.at[q % PAIR])

    def dadb():
        for k in TWO:
            us_load(0, k).start()

        def body(q, _):
            @pl.when(q < 7)
            def _():
                for k in TWO:
                    us_load(q + 1, k).start()
            wait(XS.at[4 + q % PAIR], s_us.at[q % PAIR])

            def inner(e, _):
                g = XS[q // PAIR, pl.ds(pl.multiple_of((q % PAIR) * FOUR + e * RH, RH), RH), :]
                o = pl.ds(pl.multiple_of(q * FOUR + e * RH, RH), RH)
                for k in TWO:
                    B[1 + k, 0, o, :] = (g * XS[4 + q % PAIR, pl.ds(pl.multiple_of(FOUR * k + e * RH, RH), RH), :]).astype(BF)
                return 0
            lax.fori_loop(0, 4, inner, 0)
            return 0
        lax.fori_loop(0, 8, body, 0)
        bp[1].start()
        bp[2].start()

    def chunk(idx):
        return (x + 6 - idx) % RING

    bp = [remote(B.at[k, 0], B.at[k, 1], s_b, r_b.at[k], "pc") for k in range(3)]

    def ap(arr, idx):
        return remote(xd.at[arr, :, pl.ds(pl.multiple_of(TG * chunk(idx) + CB * c1, CB), CB)], AP.at[arr, idx], s_ap, r_ap.at[arr * min(idx + 1, 2)], "pc")

    seq = (0, 1, 3, 2)

    def load_a(k, n):
        arr = 1 - min(k, 1)
        idx = seq[n]
        return (pltpu.make_async_copy(xd.at[arr, :, pl.ds(pl.multiple_of(TG * chunk(idx) + CB * c, CB), CB)], A.at[n % PAIR, 0], s_a.at[n % PAIR]),
                pltpu.make_async_copy(AP.at[arr, idx], A.at[n % PAIR, 1], s_a.at[n % PAIR]))

    served = set()

    def start_a(k, n):
        if k == DOWN and n == 0:
            wait(AP.at[1, 0], r_ap.at[1])
        elif k == DOWN and 2 not in served:
            served.add(2)
            wait(AP.at[1, pl.ds(0, 3)], r_ap.at[2])
        elif k == GATE and 0 not in served:
            served.add(0)
            wait(AP.at[0], r_ap.at[0])
        for l in load_a(k, n):
            l.start()

    def dot_x(k, n, split=False):
        slot = n % PAIR
        wait(A.at[slot], s_a.at[slot])

        def body(m, _):
            cols = pl.ds(pl.multiple_of(m * QB, QB), QB)
            to = (XB.at[0, m], XB.at[1, m], XB.at[2, m], dw.at[k, m])[n]
            to[...] = (lax.dot_general(A[slot, 0, :, cols], B[k, 0], TN, preferred_element_type=F32)
                             + lax.dot_general(A[slot, 1, :, cols], B[k, 1], TN, preferred_element_type=F32))
            return 0

        if split:
            for m in TWO:
                body(m, 0)
                xmsg(k, m).start()
        else:
            lax.fori_loop(0, 2, body, 0)

    def xmsg(k, t):
        src = (XB.at[0, 0], XB.at[0, 1], XB.at[1, 1], XB.at[2, 0], XB.at[1, 0], XB.at[2, 1])[t]
        dst = du.at[t - 4] if k == UP and t >= 4 else XR.at[k, t]
        return remote(src, dst, s_xs.at[min(t // PAIR, 1)], r_x(k, t), ("xp", "xm")[t % PAIR])

    def xl(k, n):
        start_a(k, n)

    def x1(k):
        bp[k].wait_recv()
        if k == 0:
            u_put.wait()
        else:
            wait(XB.at[0], s_xs.at[0])
        dot_x(k, 0, True)

    def x2(k):
        if k > 0:
            wait(XB.at[pl.ds(0, 2)], s_xs.at[1])
        dot_x(k, 1)
        start_a(k, 3)
        xmsg(k, 2).start()
        dot_x(k, 2)
        if k == 1:
            start_a(2, 0)
        xmsg(k, 3).start()

    def x2o(k):
        dot_x(k, 3)
        if k == 1:
            start_a(2, 1)

    def xstage(k, t, slot):
        return pltpu.make_async_copy(XR.at[k, t], XS.at[4 + slot], s_one.at[1])

    def x3(k):
        wait(XS.at[pl.ds(4, 2)], r_x(k, 0))
        for t in TWO:
            xstage(k, t, t).start()
        wait(XS.at[pl.ds(4, 2)], s_one.at[1])
        for t in TWO:
            add(XB.at[1 + t, t], XS.at[4 + t], QB)
            xmsg(k, 4 + t).start()

    def xadd(k, ts):
        wait(XS.at[pl.ds(4, 2)], r_x(k, ts[0]))
        for h, t in enumerate(ts):
            xstage(k, t, h).start()
        wait(XS.at[pl.ds(4, 2)], s_one.at[1])
        for h, t in enumerate(ts):
            add(dw.at[k, h], XS.at[4 + h], QB)

    def xfa(k):
        xadd(k, (3, 2))

    def xfb(k):
        xadd(k, (4, 5))

    def pair(n, col):
        return ((0, 3), (1, 2))[col][n % PAIR]

    def lw(n):
        if n < 2:
            for col in TWO:
                have(2, pair(n, col), 0)
                have(2, pair(n, col), 1)
        out = []
        for col in TWO:
            d = pair(n, col)
            q = xpos[d]
            if n < 2:
                if d == 0:
                    out.append(pltpu.make_async_copy(wd_ref, WD.at[col, c], s_w.at[n // PAIR]))
                    out.append(pltpu.make_async_copy(wdf.at[2 * x + c1], WD.at[col, c1], s_w.at[n // PAIR]))
                else:
                    out.append(pltpu.make_async_copy(wdf.at[pl.ds(2 * q, 2)], WD.at[col], s_w.at[n // PAIR]))
            else:
                for k in TWO:
                    full = (wgf, wuf)[k]
                    if d == 0:
                        out.append(pltpu.make_async_copy(w_in[k], WX.at[col, k, pl.ds(pl.multiple_of(CB * c, CB), CB), :], s_w.at[n // PAIR]))
                        out.append(pltpu.make_async_copy(full.at[pl.ds(pl.multiple_of(TG * x + CB * c1, CB), CB), :],
                                                         WX.at[col, k, pl.ds(pl.multiple_of(CB * c1, CB), CB), :], s_w.at[n // PAIR]))
                    else:
                        out.append(pltpu.make_async_copy(full.at[pl.ds(pl.multiple_of(TG * q, TG), TG), :], WX.at[col, k], s_w.at[n // PAIR]))
        for o in out:
            o.start()

    def dots_z(n, lo, m):

        def body(q, _):
            col = q // m
            idx = lo + 2 * (q % m)
            p = z + col * (y - z)
            ch = (p + 6 - idx) % RING
            s1 = QB - 192 * col
            s2 = RW + 192 * col
            own = (idx // PAIR) * (1 - idx // 3)
            slot = idx + own * 2 * (n % PAIR)

            def lhs(k):
                return jnp.concatenate([B[k, 0, pl.ds(pl.multiple_of(ch * s1 + g * s2, RW), RW), :] for g in range(4)], axis=0)

            if n < 2:
                l = lhs(0)
                for h in TWO:
                    ZB[col, slot, h] = jnp.dot(l, WD[col, h], preferred_element_type=F32)
            else:
                l = lhs(1)
                u = lhs(2)
                for h in TWO:
                    r = pl.ds(CB * h, CB)
                    ZB[col, slot, h] = (lax.dot_general(l, WX[col, 0, r, :], NT, preferred_element_type=F32)
                                        + lax.dot_general(u, WX[col, 1, r, :], NT, preferred_element_type=F32))
            return 0
        lax.fori_loop(0, 2 * m, body, 0)

    def zmsg(n, col, t):
        src = ((0, 0), (0, 1), (1, 1), (3, 0), (1, 0), (3, 1))[t]
        return remote(ZB.at[col, src[0], src[1]], ZR.at[col, n, t], s_zs.at[min(t // PAIR, 1)], r_z(3 * n + t // PAIR), link[col][t % PAIR])

    def own(n, col, h):
        return ZB.at[col, 2 + 2 * (n % PAIR), h]

    def sub(n, col, h, d):
        s = (pos[col][1] + d) % RING
        return ZB.at[col, 2 + 2 * (n % PAIR), h, pl.ds(pl.multiple_of(s * RW, RW), RW), :]

    def msg2(n, col, t):
        h, d = ((0, 2), (1, 2), (1, 1), (0, 3), (0, 1), (1, 3))[t]
        return remote(sub(n, col, h, d), Z2.at[col, n, t], s_2.at[n % PAIR], r_z(12 + PAIR * n + min(t // PAIR, 1)), link[col][2 + t % PAIR])

    def p1(n):
        wait((WD, WX)[n // PAIR], s_w.at[n // PAIR])
        if n > 0:
            wait(ZB.at[0, pl.ds(0, 2)], s_zs.at[0])
        dots_z(n, 0, 1)
        for t in TWO:
            for col in TWO:
                zmsg(n, col, t).start()

    def p2(n):
        if n > 0:
            wait(ZB.at[0, pl.ds(0, 4)], s_zs.at[1])
        dots_z(n, 1, 2)
        for t in range(2, 4):
            for col in TWO:
                zmsg(n, col, t).start()

    def p2o(n):
        if n > 1:
            wait(Z2.at[0, pl.ds(0, 2)], s_2.at[n % PAIR])
        dots_z(n, 2, 1)

    def zstage(n, col, t, slot):
        return pltpu.make_async_copy(ZR.at[col, n, t], ZS.at[col, slot], s_one.at[3])

    def stage(n, ts):
        wait(ZS, r_z(3 * n + ts[0] // PAIR))
        for h, t in enumerate(ts):
            for col in TWO:
                zstage(n, col, t, h).start()
        wait(ZS, s_one.at[3])

    def p4(n):
        stage(n, (0, 1))
        for t in TWO:
            for col in TWO:
                add(ZB.at[col, (1, 3)[t], t], ZS.at[col, t], QB)
                zmsg(n, col, 4 + t).start()

    def zadd(n, ts):
        stage(n, ts)
        for h in TWO:
            for col in TWO:
                add(own(n, col, h), ZS.at[col, h], QB)

    def fa(n):
        zadd(n, (3, 2))

    def fb(n):
        zadd(n, (4, 5))
        for t in range(4):
            for col in TWO:
                msg2(n, col, t).start()

    def hh(n):
        wait(Z2.at[0, 0, pl.ds(0, 4)], r_z(12 + PAIR * n))
        for t in TWO:
            for col in TWO:
                add(sub(n, col, t, (1, 3)[t]), Z2.at[col, n, t], RW)
                msg2(n, col, 4 + t).start()

    done = []

    def zf(n):
        a = n // PAIR
        if not done:
            for g in (AX, AD, AE):
                wait(some(g, 960), s_g.at[g])
        done.append(n)
        wait(Z2.at[:, 0, pl.ds(0, 4)], r_z(13 + PAIR * n))
        for col in TWO:
            q = xpos[pair(n, col)]
            for h, ts in ((0, (3, 4)), (1, (2, 5))):
                cs = pl.ds(pl.multiple_of(TG * q + CB * h, CB), CB)
                v = sub(n, col, h, 0)[...] + Z2[col, n, ts[0]] + Z2[col, n, ts[1]]
                yo[a, :, cs] = (yo[a, :, cs].astype(F32) + v).astype(BF)

    odd = (x + c + y + z) % PAIR
    along = ("xp", "xm", "pc")
    across = ("yp", "ym", "zp", "zm")

    def tell(sem, names):
        for d in names:
            pl.semaphore_signal(sem, inc=1, device_id=dev[d], device_id_type=MESH)

    def enter():
        @pl.when(odd == 0)
        def _():
            tell(barrier, across)
            pl.semaphore_wait(barrier, len(along))
            tell(in_x, along)

        @pl.when(odd == 1)
        def _():
            tell(barrier, along)
            pl.semaphore_wait(in_x, len(along))

    def enter_zy():
        @pl.when(odd == 0)
        def _():
            pl.semaphore_wait(in_zy, len(across))

        @pl.when(odd == 1)
        def _():
            pl.semaphore_wait(barrier, len(across))
            tell(in_zy, across)

    own_ld = [pltpu.make_async_copy(r, yo.at[k], s_one.at[4]) for k, r in enumerate((x_ref, dy_ref))]
    for l in own_ld:
        l.start()
    barrier = pltpu.get_barrier_semaphore()
    enter()
    put = pltpu.make_async_copy(yo, xd.at[:, pl.ds(pl.multiple_of(j * RW, RW), RW), :], s_one.at[5])
    wown(WG)
    wown(WU)
    wpc(WG)
    wpc(WU)
    wpc(WL)
    wait(yo, s_one.at[4])
    put.start()
    enter_zy()
    ga(AX)
    gb0(AX)
    ga(AD)
    ga2(AX)
    gf(AX, OWN)
    gb31(AX)
    ga2(AD)
    gb2(AX)
    wf(WG)
    gf(AX, PREV)
    gf(AX, NEXT)
    gf(AX, OPP)
    ga(AE)
    gb31(AD)
    wf(WU)
    gb0(AD)
    gend(AX)
    sab(B2)
    sab(B1)
    sab(B0)
    ab(B0)
    wown(WL)
    ab(B1)
    gb2(AD)
    sab(B3)
    gf(AD, PREV)
    sab(B4)
    ga2(AE)
    wf2(WG)
    ab(B2)
    gb0(AE)
    wf2(WU)
    gf(AD, OWN)
    ab(B3)
    sab(B6)
    gf(AD, NEXT)
    gf(AD, OPP)
    sab(B5)
    ab(B4)
    sab(B7)
    gb2(AE)
    ab(B5)
    gb31(AE)
    gf(AE, OWN)
    ab(B6)
    wf(WL)
    ab(B7)
    gend(AD)
    hp()
    xl(DOWN, A0)
    gf(AE, PREV)
    wfp()
    gf(AE, NEXT)
    gf(AE, OPP)
    x1(DOWN)
    lw(Y0)
    gend(AE)
    p1(Y0)
    xl(DOWN, A2)
    xl(DOWN, A1)
    wf2(WL)
    p2(Y0)
    x2(DOWN)
    x2o(DOWN)
    sg(B1)
    sg(B0)
    p2o(Y0)
    lw(Y1)
    gg(B0)
    sg(B4)
    sg(B3)
    gg(B1)
    sg(B2)
    p4(Y0)
    gg(B2)
    gg(B3)
    gg(B4)
    sg(B5)
    p1(Y1)
    x3(DOWN)
    sg(B6)
    gg(B5)
    gg(B6)
    sg(B7)
    p2(Y1)
    gg(B7)
    xl(GATE, A0)
    lw(X0)
    dadb()
    xfa(DOWN)
    p2o(Y1)
    xl(GATE, A1)
    x1(GATE)
    p4(Y1)
    fa(Y0)
    p1(X0)
    xl(GATE, A2)
    x2(GATE)
    fb(Y0)
    xfb(DOWN)
    x3(GATE)
    fa(Y1)
    x1(UP)
    fb(Y1)
    hh(Y0)
    x2o(GATE)
    p2(X0)
    zf(Y0)
    xl(UP, A2)
    p4(X0)
    p2o(X0)
    lw(X1)
    hh(Y1)
    p1(X1)
    xfa(GATE)
    x2(UP)
    fa(X0)
    p2(X1)
    p4(X1)
    xfb(GATE)
    x3(UP)
    zf(Y1)
    fb(X0)
    p2o(X1)
    x2o(UP)
    fa(X1)
    fb(X1)
    hh(X0)
    xfa(UP)
    hh(X1)
    zf(X0)
    zf(X1)
    def end():
        for k in (WG, WU, WL):
            wait(blocks(k, 7), s_v.at[k])
        wait(AP, s_ap)
        wait(B.at[:, 0], s_b)
        for q in TWO:
            wait(Z2.at[0, pl.ds(0, 2)], s_2.at[q])
            wait(ZB.at[0, pl.ds(0, 2 + 2 * q)], s_zs.at[q])
        wait(XB.at[0], s_xs.at[0])
        wait(XB.at[pl.ds(0, 2)], s_xs.at[1])
        wait(du, r_x(UP, 4))

    end()


def mlp(x, dy, wg, wu, wd):
    sd = jax.ShapeDtypeStruct
    dma = pltpu.SemaphoreType.DMA
    V = pltpu.VMEM
    o = pl.pallas_call(
        mlp_kernel,
        out_shape=(V((3, 2, QB, FB), F32), V((2, RW, DM), BF), V((2, QB, FB), F32),
                   sd((2, TG, DM), BF), sd((DM, FB), BF), sd((DM, FB), BF), sd((8, FB, CB), BF), sd((2, 2, QB, FB), F32), sd((4, QB, FB), F32),
                   sd((3, 6, QB, FB), F32), sd((2, 4, 6, QB, CB), F32), sd((2, 4, TG, CB), BF)),
        in_specs=[HBM] * 5,
        out_specs=(VMEM,) * 3 + (HBM,) * 9,
        scratch_shapes=[
            V((3, 2, TG, FB), BF), V((2, 2, TG, CB), BF), V((3, 2, QB, FB), F32), V((6, QB, FB), F32),
            V((2, 2, FB, CB), BF), V((2, 2, TG, FB), BF), V((2, 5, 2, QB, CB), F32), V((2, 2, QB, CB), F32),
            V((2, 4, 6, RW, CB), F32),
            dma((3,)), dma((3, 7)), dma((3,)), dma((3, 7)), dma, dma((3,)), dma, dma((3,)), dma((2,)), dma((2,)), dma((2,)),
            dma((4,)), dma((2,)), dma((2,)), dma((2,)), dma((7,)),
            pltpu.SemaphoreType.REGULAR, pltpu.SemaphoreType.REGULAR,
        ],
        compiler_params=pltpu.CompilerParams(collective_id=1, has_side_effects=True, vmem_limit_bytes=58600000),
        name="mlp",
    )(x, dy, wg, wu, wd)
    return o[:3]


def place_kernel(dw, yo, du, y, dx, og, ou, od, bu, bt, sem):
    outs = [pltpu.make_async_copy(dw.at[1], og, sem.at[0]), pltpu.make_async_copy(yo.at[0], y, sem.at[1]), pltpu.make_async_copy(yo.at[1], dx, sem.at[2]),
            pltpu.make_async_copy(bu, ou, sem.at[3]), pltpu.make_async_copy(bt, od, sem.at[4])]
    for o in outs[:3]:
        o.start()
    for h in TWO:
        r = pl.ds(QB * h, QB)
        bu[r, :] = dw[2, r, :] + du[h]
    outs[3].start()
    for h in TWO:
        r = pl.ds(QB * h, QB)
        bt[:, r] = dw[0, r, :].T
    outs[4].start()
    for o in outs:
        o.wait()


def place(dw, yo, du):
    sd = jax.ShapeDtypeStruct
    V = pltpu.VMEM
    return pl.pallas_call(
        place_kernel,
        out_shape=(sd((RW, DM), BF), sd((RW, DM), BF), sd((CB, FB), F32), sd((CB, FB), F32), sd((FB, CB), F32)),
        in_specs=[VMEM] * 3,
        out_specs=(HBM,) * 5,
        scratch_shapes=[V((CB, FB), F32), V((FB, CB), F32), pltpu.SemaphoreType.DMA((5,))],
        compiler_params=pltpu.CompilerParams(vmem_limit_bytes=24 * 2**20),
        name="place",
    )(dw.reshape(3, CB, FB), yo, du)


def solution(mesh):
    rows = P(("dp", "tp"), None)
    wsp = P("dp", "tp")
    dsp = P("tp", "dp")

    def local(x, w_gate, w_up, w_down, dy):
        return place(*mlp(x, dy, w_gate, w_up, w_down))

    return jax.shard_map(local, mesh=mesh, in_specs=(rows, wsp, wsp, dsp, rows), out_specs=(rows, rows, wsp, wsp, dsp), check_vma=False)
```

```python
import jax
import jax.numpy as jnp
from jax import lax
from jax.experimental import pallas as pl
from jax.experimental.pallas import tpu as pltpu
from jax.sharding import PartitionSpec as P

MESH = pl.DeviceIdType.MESH
HBM = pl.BlockSpec(memory_space=pltpu.HBM)
VMEM = pl.BlockSpec(memory_space=pltpu.VMEM)
NT = (((1,), (1,)), ((), ()))
TN = (((0,), (0,)), ((), ()))
F32 = jnp.float32
BF = jnp.bfloat16
TWO = range(2)
RING = 4
PAIR = 2
HB = 448
FOUR = 128
DM, TG, FB, CB, QB, RW, RH = 4096, 1024, 896, 512, 256, 64, 32
AX, AD, AE = range(3)
OWN, NEXT, OPP, PREV = range(4)
WG, WU, WL = range(3)
DOWN, GATE, UP = range(3)
Y0, Y1, X0, X1 = range(4)
A0, A1, A2 = range(3)
B0, B1, B2, B3, B4, B5, B6, B7 = range(8)


def mlp_kernel(x_ref, dy_ref, wg_ref, wu_ref, wd_ref, dw, yo, du, xd, wgf, wuf, wdf, U, V, XR, ZR, AP,
               B, A, XB, XS, WD, WX, ZB, ZS, Z2,
               s_g, r_g, s_v, r_v, s_ap, r_ap, s_b, r_b, s_xs, s_zs, s_2, s_c, s_w, s_us, s_one, in_x, in_zy):
    i = lax.axis_index("dp")
    j = lax.axis_index("tp")
    x, c, z, y = i // PAIR, i % PAIR, j // 4, j % RING
    xp, xm, xq, c1 = (x + 1) % RING, (x + 3) % RING, (x + 2) % RING, 1 - c
    dev = {
        "xp": {"dp": 2 * xp + c}, "xm": {"dp": 2 * xm + c}, "pc": {"dp": 2 * x + c1},
        "yp": {"tp": 4 * z + (y + 1) % RING}, "ym": {"tp": 4 * z + (y + 3) % RING},
        "zp": {"tp": 4 * ((z + 1) % RING) + y}, "zm": {"tp": 4 * ((z + 3) % RING) + y},
    }
    pos = ((z, y), (y, z))
    link = (("zp", "zm", "yp", "ym"), ("yp", "ym", "zp", "zm"))

    def remote(src, dst, ss, rs, to):
        return pltpu.make_async_remote_copy(src_ref=src, dst_ref=dst, send_sem=ss, recv_sem=rs, device_id=dev[to], device_id_type=MESH)

    def wait(ref, sem):
        pltpu.make_async_copy(ref, ref, sem).wait()

    def r_x(k, t):
        return r_v.at[k, 4 + t // PAIR]

    def r_z(i):
        return r_g.at[i // 7, i % 7]

    def add(dst, src, n):
        def body(r, _):
            s = pl.ds(pl.multiple_of(r * RH, RH), RH)
            dst[s, :] = dst[s, :] + src[s, :]
            return 0
        lax.fori_loop(0, n // RH, body, 0)

    def send(src, dst, to, ss, rs):
        remote(src, dst, ss, rs, to).start()

    def wblk(k, xx, cc, half=None):
        ii = 2 * xx + cc
        if k < 2:
            r = (wgf, wuf)[k]
            if half is None:
                return r.at[pl.ds(pl.multiple_of(ii * CB, CB), CB), :]
            return r.at[pl.ds(pl.multiple_of(ii * CB + half * QB, QB), QB), :]
        if half is None:
            return wdf.at[ii]
        return wdf.at[ii, pl.ds(half * HB, HB), :]

    ahead = xq // PAIR

    def cols(a):
        if a == AX:
            return slice(None)
        h = ahead if a == AD else 1 - ahead
        return pl.ds(pl.multiple_of(h * (DM // PAIR), DM // PAIR), DM // PAIR)

    def rows(a, col, s, p, lo=0, n=RH):
        zz, yy = (p, s) if col == 0 else (s, p)
        return xd.at[min(a, AD), pl.ds(pl.multiple_of((zz * 4 + yy) * RW + col * RH + lo, 16), n), cols(a)]

    def geo(col):
        sec, prim = pos[col]
        sp, sm, pp, pm = link[col]
        return prim, sec, pp, pm, sp, sm

    def some(a, n):
        return xd.at[min(a, AD), pl.ds(0, n), cols(a)]

    FIRST, ON, LAST = range(4, 7)

    def ga(a):
        for col in TWO:
            p, s, pp, pm, sp, sm = geo(col)
            src = yo.at[min(a, AD), pl.ds(col * RH, RH), cols(a)]
            for to in (pp, pm):
                send(src, rows(a, col, p, s), to, s_g.at[a], r_g.at[a, FIRST])

    def gb0(a):
        for col in TWO:
            p, s, pp, pm, sp, sm = geo(col)
            src = yo.at[min(a, AD), pl.ds(col * RH, RH), cols(a)]
            for to in (sp, sm):
                send(src, rows(a, col, p, s), to, s_g.at[a], r_g.at[a, OWN])

    def ga2(a):
        wait(some(a, FOUR), r_g.at[a, FIRST])
        for col in TWO:
            p, s, pp, pm, sp, sm = geo(col)
            for d, lo, to in ((PREV, 0, pp), (NEXT, 16, pm)):
                r = rows(a, col, (p + d) % RING, s, lo, 16)
                send(r, r, to, s_g.at[a], r_g.at[a, ON])

    def gb31(a):
        for col in TWO:
            p, s, pp, pm, sp, sm = geo(col)
            for d in (PREV, NEXT):
                r = rows(a, col, (p + d) % RING, s)
                for to in (sp, sm):
                    send(r, r, to, s_g.at[a], r_g.at[a, d])

    def gb2(a):
        wait(some(a, RW), r_g.at[a, ON])
        for col in TWO:
            p, s, pp, pm, sp, sm = geo(col)
            r = rows(a, col, (p + OPP) % RING, s)
            for to in (sp, sm):
                send(r, r, to, s_g.at[a], r_g.at[a, OPP])

    def gf(a, d):
        wait(some(a, FOUR), r_g.at[a, d])
        for col in TWO:
            p, s, pp, pm, sp, sm = geo(col)
            for e, lo, to in ((PREV, 0, sp), (NEXT, 16, sm)):
                r = rows(a, col, (p + d) % RING, (s + e) % RING, lo, 16)
                send(r, r, to, s_g.at[a], r_g.at[a, LAST])

    def gend(a):
        if a == AX:
            put.wait()
        wait(some(a, QB), r_g.at[a, LAST])
        for arr, idx in (((AX, 0), (AX, 1), (AX, 3), (AX, 2)), ((AD, 0),), ((AD, 1), (AD, 3), (AD, 2)))[a]:
            ap(arr, idx).start()

    w_in = (wg_ref, wu_ref, wd_ref)
    LATE = 6
    seen = set()

    def blocks(k, n):
        return wdf.at[pl.ds(0, n)] if k == WL else (wgf, wuf)[k].at[pl.ds(0, n * CB), :]

    def once(k, g, n):
        if (k, g) not in seen:
            seen.add((k, g))
            wait(blocks(k, n), r_v.at[k, g])

    def wpc(k):
        send(w_in[k], wblk(k, x, c), "pc", s_v.at[k], r_v.at[k, OWN])

    def wown(k):
        for fr, to in enumerate(("xp", "xm")):
            if k < WL:
                send(w_in[k], wblk(k, x, c), to, s_v.at[k], r_v.at[k, FIRST])
            else:
                send(wd_ref.at[pl.ds(fr * HB, HB), :], wblk(k, x, c, fr), to, s_v.at[k], r_v.at[k, FIRST])
        if k == WL:
            for fr, to in enumerate(("xp", "xm")):
                send(wd_ref.at[pl.ds((1 - fr) * HB, HB), :], wblk(k, x, c, 1 - fr), to, s_v.at[k], r_v.at[k, LATE])

    def wf(k):
        once(k, FIRST, 1 if k == WL else 2)
        for xx, d, half, to in ((xm, PREV, 0, "xp"), (xp, NEXT, 1, "xm")):
            r = wblk(k, xx, c, half)
            send(r, r, to, s_v.at[k], r_v.at[k, ON])
            if k < WL:
                r = wblk(k, xx, c)
                send(r, r, "pc", s_v.at[k], r_v.at[k, d])

    def wfp():
        once(WL, LATE, 1)
        for xx, d in ((xm, PREV), (xp, NEXT)):
            r = wblk(WL, xx, c)
            send(r, r, "pc", s_v.at[WL], r_v.at[WL, d])

    def wf2(k):
        once(k, ON, 1)
        for half in TWO:
            r = wblk(k, xq, c, half)
            send(r, r, "pc", s_v.at[k], r_v.at[k, OPP])

    def have(k, d, o):
        if o == 1:
            once(k, d, 1)
        elif d == OPP:
            once(k, ON, 1)
        elif d:
            once(k, FIRST, 1 if k == WL else 2)
            if k == WL:
                once(k, LATE, 1)

    xpos = {0: x, 1: xp, 2: xq, 3: xm}
    order = ((0, 0), (0, 1), (3, 0), (1, 0), (3, 1), (1, 1), (2, 0), (2, 1))

    def blk(t):
        d, o = order[t]
        return 2 * xpos[d] + (c if o == 0 else c1)

    def a_slot(t):
        s = t % RING
        return A.at[s // PAIR, s % PAIR]

    def ld_ab(t):
        d, o = order[t]
        s = t % RING
        ii = blk(t)
        out = [pltpu.make_async_copy(xd.at[0, :, pl.ds(pl.multiple_of(ii * CB, CB), CB)], a_slot(t), s_c.at[s])]
        for k in TWO:
            src = w_in[k] if t == 0 else wblk(k, xpos[d], c if o == 0 else c1)
            out.append(pltpu.make_async_copy(src, WX.at[s % PAIR, k, pl.ds((s // PAIR) * CB, CB), :], s_c.at[s]))
        return out

    def sab(t):
        for k in TWO:
            have(k, *order[t])
        for l in ld_ab(t):
            l.start()

    def ab(t):
        s = t % RING
        wait(xd.at[0, pl.ds(0, 352)], s_c.at[s])

        def body(m, _):
            r = pl.ds(pl.multiple_of(m * QB, QB), QB)
            lhs = A[s // PAIR, s % PAIR, r, :]
            for k in TWO:
                v = jnp.dot(lhs, WX[s % PAIR, k, pl.ds((s // PAIR) * CB, CB), :], preferred_element_type=F32)
                to = XB.at[m // PAIR, m % PAIR] if k == WG else XS.at[m]
                to[...] = v if t == 0 else to[...] + v
            return 0
        lax.fori_loop(0, 4, body, 0)

    def hp():
        def body(q, _):
            m = q // 8
            r = pl.ds(pl.multiple_of((q % 8) * RH, RH), RH)
            a = XB[m // PAIR, m % PAIR, r, :]
            b = XS[m, r, :]
            sig = jax.nn.sigmoid(a)
            sa = a * sig
            XB[m // PAIR, m % PAIR, r, :] = b * sig * (1.0 + a * (1.0 - sig))
            XS[m, r, :] = sa
            B[0, 0, pl.ds(pl.multiple_of(q * RH, RH), RH), :] = (sa * b).astype(BF)
            return 0
        lax.fori_loop(0, RH, body, 0)
        bp[0].start()
        u_put.start()
        v_put.start()

    u_put = pltpu.make_async_copy(XB.at[pl.ds(0, 2)], U, s_one.at[0])
    v_put = pltpu.make_async_copy(XS.at[pl.ds(0, 4)], V, s_one.at[1])

    def ld_g(t):
        d, o = order[t]
        s = t % RING
        ii = blk(t)
        src = wd_ref if t == 0 else wdf.at[ii]
        return [pltpu.make_async_copy(xd.at[1, :, pl.ds(pl.multiple_of(ii * CB, CB), CB)], a_slot(t), s_c.at[s]),
                pltpu.make_async_copy(src, WX.at[s % PAIR, s // PAIR, pl.ds(0, FB), pl.ds(0, CB)], s_c.at[s])]

    def sg(t):
        have(2, *order[t])
        for l in ld_g(t):
            l.start()

    def gg(t):
        if t == 0:
            v_put.wait()
        s = t % RING
        wait(xd.at[1, pl.ds(0, 240)], s_c.at[s])

        def body(m, _):
            r = pl.ds(pl.multiple_of(m * QB, QB), QB)
            v = lax.dot_general(A[s // PAIR, s % PAIR, r, :], WX[s % PAIR, s // PAIR, pl.ds(0, FB), pl.ds(0, CB)], NT, preferred_element_type=F32)
            if t == 0:
                XS[m] = v
            else:
                XS[m] += v
            return 0
        lax.fori_loop(0, 4, body, 0)

    def us_load(q, k):
        m = q // PAIR
        r = pl.ds(pl.multiple_of((q % PAIR) * FOUR, FOUR), FOUR)
        src = U.at[m // PAIR, m % PAIR, r, :] if k == 0 else V.at[m, r, :]
        return pltpu.make_async_copy(src, XS.at[4 + q % PAIR, pl.ds(FOUR * k, FOUR), :], s_us.at[q % PAIR])

    def dadb():
        for k in TWO:
            us_load(0, k).start()

        def body(q, _):
            @pl.when(q < 7)
            def _():
                for k in TWO:
                    us_load(q + 1, k).start()
            wait(XS.at[4 + q % PAIR], s_us.at[q % PAIR])

            def inner(e, _):
                g = XS[q // PAIR, pl.ds(pl.multiple_of((q % PAIR) * FOUR + e * RH, RH), RH), :]
                o = pl.ds(pl.multiple_of(q * FOUR + e * RH, RH), RH)
                for k in TWO:
                    B[1 + k, 0, o, :] = (g * XS[4 + q % PAIR, pl.ds(pl.multiple_of(FOUR * k + e * RH, RH), RH), :]).astype(BF)
                return 0
            lax.fori_loop(0, 4, inner, 0)
            return 0
        lax.fori_loop(0, 8, body, 0)
        bp[1].start()
        bp[2].start()

    def chunk(idx):
        return (x + 6 - idx) % RING

    bp = [remote(B.at[k, 0], B.at[k, 1], s_b, r_b.at[k], "pc") for k in range(3)]

    def ap(arr, idx):
        return remote(xd.at[arr, :, pl.ds(pl.multiple_of(TG * chunk(idx) + CB * c1, CB), CB)], AP.at[arr, idx], s_ap, r_ap.at[arr * min(idx + 1, 2)], "pc")

    seq = (0, 1, 3, 2)

    def load_a(k, n):
        arr = 1 - min(k, 1)
        idx = seq[n]
        return (pltpu.make_async_copy(xd.at[arr, :, pl.ds(pl.multiple_of(TG * chunk(idx) + CB * c, CB), CB)], A.at[n % PAIR, 0], s_c.at[n % PAIR]),
                pltpu.make_async_copy(AP.at[arr, idx], A.at[n % PAIR, 1], s_c.at[n % PAIR]))

    served = set()

    def start_a(k, n):
        if k == DOWN and n == 0:
            wait(AP.at[1, 0], r_ap.at[1])
        elif k == DOWN and 2 not in served:
            served.add(2)
            wait(AP.at[1, pl.ds(0, 3)], r_ap.at[2])
        elif k == GATE and 0 not in served:
            served.add(0)
            wait(AP.at[0], r_ap.at[0])
        for l in load_a(k, n):
            l.start()

    def dot_x(k, n, split=False):
        slot = n % PAIR
        wait(A.at[slot], s_c.at[slot])

        def body(m, _):
            cols = pl.ds(pl.multiple_of(m * QB, QB), QB)
            to = (XB.at[0, m], XB.at[1, m], XB.at[2, m], dw.at[k, m])[n]
            to[...] = (lax.dot_general(A[slot, 0, :, cols], B[k, 0], TN, preferred_element_type=F32)
                             + lax.dot_general(A[slot, 1, :, cols], B[k, 1], TN, preferred_element_type=F32))
            return 0

        if split:
            for m in TWO:
                body(m, 0)
                xmsg(k, m).start()
        else:
            lax.fori_loop(0, 2, body, 0)

    def xmsg(k, t):
        src = (XB.at[0, 0], XB.at[0, 1], XB.at[1, 1], XB.at[2, 0], XB.at[1, 0], XB.at[2, 1])[t]
        dst = du.at[t - 4] if k == UP and t >= 4 else XR.at[k, t]
        return remote(src, dst, s_xs.at[min(t // PAIR, 1)], r_x(k, t), ("xp", "xm")[t % PAIR])

    def xl(k, n):
        start_a(k, n)

    def x1(k):
        bp[k].wait_recv()
        if k == 0:
            u_put.wait()
        else:
            wait(XB.at[0], s_xs.at[0])
        dot_x(k, 0, True)

    def x2(k):
        if k > 0:
            wait(XB.at[pl.ds(0, 2)], s_xs.at[1])
        dot_x(k, 1)
        start_a(k, 3)
        xmsg(k, 2).start()
        dot_x(k, 2)
        if k == 1:
            start_a(2, 0)
        xmsg(k, 3).start()

    def x2o(k):
        dot_x(k, 3)
        if k == 1:
            start_a(2, 1)

    def xstage(k, t, slot):
        return pltpu.make_async_copy(XR.at[k, t], XS.at[4 + slot], s_one.at[3])

    def x3(k):
        wait(XS.at[pl.ds(4, 2)], r_x(k, 0))
        for t in TWO:
            xstage(k, t, t).start()
        wait(XS.at[pl.ds(4, 2)], s_one.at[3])
        for t in TWO:
            add(XB.at[1 + t, t], XS.at[4 + t], QB)
            xmsg(k, 4 + t).start()

    def xadd(k, ts):
        wait(XS.at[pl.ds(4, 2)], r_x(k, ts[0]))
        for h, t in enumerate(ts):
            xstage(k, t, h).start()
        wait(XS.at[pl.ds(4, 2)], s_one.at[3])
        for h, t in enumerate(ts):
            add(dw.at[k, h], XS.at[4 + h], QB)

    def xfa(k):
        xadd(k, (3, 2))

    def xfb(k):
        xadd(k, (4, 5))

    def pair(n, col):
        return ((0, 3), (1, 2))[col][n % PAIR]

    def lw(n):
        if n < 2:
            for col in TWO:
                have(2, pair(n, col), 0)
                have(2, pair(n, col), 1)
        out = []
        for col in TWO:
            d = pair(n, col)
            q = xpos[d]
            if n < 2:
                if d == 0:
                    out.append(pltpu.make_async_copy(wd_ref, WD.at[col, c], s_w.at[n // PAIR]))
                    out.append(pltpu.make_async_copy(wdf.at[2 * x + c1], WD.at[col, c1], s_w.at[n // PAIR]))
                else:
                    out.append(pltpu.make_async_copy(wdf.at[pl.ds(2 * q, 2)], WD.at[col], s_w.at[n // PAIR]))
            else:
                for k in TWO:
                    full = (wgf, wuf)[k]
                    if d == 0:
                        out.append(pltpu.make_async_copy(w_in[k], WX.at[col, k, pl.ds(pl.multiple_of(CB * c, CB), CB), :], s_w.at[n // PAIR]))
                        out.append(pltpu.make_async_copy(full.at[pl.ds(pl.multiple_of(TG * x + CB * c1, CB), CB), :],
                                                         WX.at[col, k, pl.ds(pl.multiple_of(CB * c1, CB), CB), :], s_w.at[n // PAIR]))
                    else:
                        out.append(pltpu.make_async_copy(full.at[pl.ds(pl.multiple_of(TG * q, TG), TG), :], WX.at[col, k], s_w.at[n // PAIR]))
        for o in out:
            o.start()

    def dots_z(n, lo, m):

        def body(q, _):
            col = q // m
            idx = lo + 2 * (q % m)
            p = z + col * (y - z)
            ch = (p + 6 - idx) % RING
            s1 = QB - 192 * col
            s2 = RW + 192 * col
            own = (idx // PAIR) * (1 - idx // 3)
            slot = idx + own * 2 * (n % PAIR)

            def lhs(k):
                return jnp.concatenate([B[k, 0, pl.ds(pl.multiple_of(ch * s1 + g * s2, RW), RW), :] for g in range(4)], axis=0)

            if n < 2:
                l = lhs(0)
                for h in TWO:
                    ZB[col, slot, h] = jnp.dot(l, WD[col, h], preferred_element_type=F32)
            else:
                l = lhs(1)
                u = lhs(2)
                for h in TWO:
                    r = pl.ds(CB * h, CB)
                    ZB[col, slot, h] = (lax.dot_general(l, WX[col, 0, r, :], NT, preferred_element_type=F32)
                                        + lax.dot_general(u, WX[col, 1, r, :], NT, preferred_element_type=F32))
            return 0
        lax.fori_loop(0, 2 * m, body, 0)

    def zmsg(n, col, t):
        src = ((0, 0), (0, 1), (1, 1), (3, 0), (1, 0), (3, 1))[t]
        return remote(ZB.at[col, src[0], src[1]], ZR.at[col, n, t], s_zs.at[min(t // PAIR, 1)], r_z(3 * n + t // PAIR), link[col][t % PAIR])

    def own(n, col, h):
        return ZB.at[col, 2 + 2 * (n % PAIR), h]

    def sub(n, col, h, d):
        s = (pos[col][1] + d) % RING
        return ZB.at[col, 2 + 2 * (n % PAIR), h, pl.ds(pl.multiple_of(s * RW, RW), RW), :]

    def msg2(n, col, t):
        h, d = ((0, 2), (1, 2), (1, 1), (0, 3), (0, 1), (1, 3))[t]
        return remote(sub(n, col, h, d), Z2.at[col, n, t], s_2.at[n % PAIR], r_z(12 + PAIR * n + min(t // PAIR, 1)), link[col][2 + t % PAIR])

    def p1(n):
        wait((WD, WX)[n // PAIR], s_w.at[n // PAIR])
        if n > 0:
            wait(ZB.at[0, pl.ds(0, 2)], s_zs.at[0])
        dots_z(n, 0, 1)
        for t in TWO:
            for col in TWO:
                zmsg(n, col, t).start()

    def p2(n):
        if n > 0:
            wait(ZB.at[0, pl.ds(0, 4)], s_zs.at[1])
        dots_z(n, 1, 2)
        for t in range(2, 4):
            for col in TWO:
                zmsg(n, col, t).start()

    def p2o(n):
        if n > 1:
            wait(Z2.at[0, pl.ds(0, 2)], s_2.at[n % PAIR])
        dots_z(n, 2, 1)

    def zstage(n, col, t, slot):
        return pltpu.make_async_copy(ZR.at[col, n, t], ZS.at[col, slot], s_one.at[2])

    def stage(n, ts):
        wait(ZS, r_z(3 * n + ts[0] // PAIR))
        for h, t in enumerate(ts):
            for col in TWO:
                zstage(n, col, t, h).start()
        wait(ZS, s_one.at[2])

    def p4(n):
        stage(n, (0, 1))
        for t in TWO:
            for col in TWO:
                add(ZB.at[col, (1, 3)[t], t], ZS.at[col, t], QB)
                zmsg(n, col, 4 + t).start()

    def zadd(n, ts):
        stage(n, ts)
        for h in TWO:
            for col in TWO:
                add(own(n, col, h), ZS.at[col, h], QB)

    def fa(n):
        zadd(n, (3, 2))

    def fb(n):
        zadd(n, (4, 5))
        for t in range(4):
            for col in TWO:
                msg2(n, col, t).start()

    def hh(n):
        wait(Z2.at[0, 0, pl.ds(0, 4)], r_z(12 + PAIR * n))
        for t in TWO:
            for col in TWO:
                add(sub(n, col, t, (1, 3)[t]), Z2.at[col, n, t], RW)
                msg2(n, col, 4 + t).start()

    done = []

    def zf(n):
        a = n // PAIR
        if not done:
            for g in (AX, AD, AE):
                wait(some(g, 960), s_g.at[g])
        done.append(n)
        wait(Z2.at[:, 0, pl.ds(0, 4)], r_z(13 + PAIR * n))
        for col in TWO:
            q = xpos[pair(n, col)]
            for h, ts in ((0, (3, 4)), (1, (2, 5))):
                cs = pl.ds(pl.multiple_of(TG * q + CB * h, CB), CB)
                v = sub(n, col, h, 0)[...] + Z2[col, n, ts[0]] + Z2[col, n, ts[1]]
                yo[a, :, cs] = (yo[a, :, cs].astype(F32) + v).astype(BF)

    odd = (x + c + y + z) % PAIR
    along = ("xp", "xm", "pc")
    across = ("yp", "ym", "zp", "zm")

    def tell(sem, names):
        for d in names:
            pl.semaphore_signal(sem, inc=1, device_id=dev[d], device_id_type=MESH)

    def enter():
        @pl.when(odd == 0)
        def _():
            tell(barrier, across)
            pl.semaphore_wait(barrier, len(along))
            tell(in_x, along)

        @pl.when(odd == 1)
        def _():
            tell(barrier, along)
            pl.semaphore_wait(in_x, len(along))

    def enter_zy():
        @pl.when(odd == 0)
        def _():
            pl.semaphore_wait(in_zy, len(across))

        @pl.when(odd == 1)
        def _():
            pl.semaphore_wait(barrier, len(across))
            tell(in_zy, across)

    own_ld = [pltpu.make_async_copy(r, yo.at[k], s_one.at[2]) for k, r in enumerate((x_ref, dy_ref))]
    for l in own_ld:
        l.start()
    barrier = pltpu.get_barrier_semaphore()
    enter()
    put = pltpu.make_async_copy(yo, xd.at[:, pl.ds(pl.multiple_of(j * RW, RW), RW), :], s_one.at[3])
    wown(WG)
    wown(WU)
    wpc(WG)
    wpc(WU)
    wpc(WL)
    wait(yo, s_one.at[2])
    put.start()
    enter_zy()
    ga(AX)
    gb0(AX)
    ga(AD)
    ga2(AX)
    gf(AX, OWN)
    gb31(AX)
    ga2(AD)
    gb2(AX)
    wf(WG)
    gf(AX, PREV)
    gf(AX, NEXT)
    gf(AX, OPP)
    ga(AE)
    gb31(AD)
    wf(WU)
    wown(WL)
    gb0(AD)
    gend(AX)
    sab(B2)
    sab(B1)
    sab(B0)
    ab(B0)
    ab(B1)
    gb2(AD)
    sab(B3)
    gf(AD, PREV)
    sab(B4)
    ga2(AE)
    wf2(WG)
    ab(B2)
    gb0(AE)
    wf2(WU)
    gf(AD, OWN)
    ab(B3)
    sab(B6)
    gf(AD, NEXT)
    gf(AD, OPP)
    sab(B5)
    ab(B4)
    sab(B7)
    gb2(AE)
    ab(B5)
    gb31(AE)
    gf(AE, OWN)
    ab(B6)
    wf(WL)
    ab(B7)
    gend(AD)
    hp()
    xl(DOWN, A0)
    gf(AE, PREV)
    wfp()
    gf(AE, NEXT)
    gf(AE, OPP)
    x1(DOWN)
    lw(Y0)
    gend(AE)
    p1(Y0)
    xl(DOWN, A2)
    xl(DOWN, A1)
    wf2(WL)
    p2(Y0)
    x2(DOWN)
    x2o(DOWN)
    sg(B1)
    sg(B0)
    p2o(Y0)
    lw(Y1)
    gg(B0)
    sg(B4)
    sg(B3)
    gg(B1)
    sg(B2)
    p4(Y0)
    gg(B2)
    gg(B3)
    gg(B4)
    sg(B5)
    p1(Y1)
    x3(DOWN)
    sg(B6)
    gg(B5)
    gg(B6)
    sg(B7)
    p2(Y1)
    gg(B7)
    xl(GATE, A0)
    lw(X0)
    dadb()
    xfa(DOWN)
    p2o(Y1)
    xl(GATE, A1)
    x1(GATE)
    p4(Y1)
    fa(Y0)
    p1(X0)
    xl(GATE, A2)
    x2(GATE)
    fb(Y0)
    xfb(DOWN)
    x3(GATE)
    fa(Y1)
    x1(UP)
    fb(Y1)
    hh(Y0)
    x2o(GATE)
    p2(X0)
    zf(Y0)
    xl(UP, A2)
    p4(X0)
    p2o(X0)
    lw(X1)
    hh(Y1)
    p1(X1)
    xfa(GATE)
    x2(UP)
    fa(X0)
    p2(X1)
    p4(X1)
    xfb(GATE)
    x3(UP)
    zf(Y1)
    fb(X0)
    p2o(X1)
    x2o(UP)
    fa(X1)
    fb(X1)
    hh(X0)
    xfa(UP)
    hh(X1)
    zf(X0)
    zf(X1)
    def end():
        for k in (WG, WU, WL):
            wait(blocks(k, 7), s_v.at[k])
        wait(AP, s_ap)
        wait(B.at[:, 0], s_b)
        for q in TWO:
            wait(Z2.at[0, pl.ds(0, 2)], s_2.at[q])
            wait(ZB.at[0, pl.ds(0, 2 + 2 * q)], s_zs.at[q])
        wait(XB.at[0], s_xs.at[0])
        wait(XB.at[pl.ds(0, 2)], s_xs.at[1])
        wait(du, r_x(UP, 4))

    end()


def mlp(x, dy, wg, wu, wd):
    sd = jax.ShapeDtypeStruct
    dma = pltpu.SemaphoreType.DMA
    V = pltpu.VMEM
    o = pl.pallas_call(
        mlp_kernel,
        out_shape=(V((3, 2, QB, FB), F32), V((2, RW, DM), BF), V((2, QB, FB), F32),
                   sd((2, TG, DM), BF), sd((DM, FB), BF), sd((DM, FB), BF), sd((8, FB, CB), BF), sd((2, 2, QB, FB), F32), sd((4, QB, FB), F32),
                   sd((3, 6, QB, FB), F32), sd((2, 4, 6, QB, CB), F32), sd((2, 4, TG, CB), BF)),
        in_specs=[HBM] * 5,
        out_specs=(VMEM,) * 3 + (HBM,) * 9,
        scratch_shapes=[
            V((3, 2, TG, FB), BF), V((2, 2, TG, CB), BF), V((3, 2, QB, FB), F32), V((6, QB, FB), F32),
            V((2, 2, FB, CB), BF), V((2, 2, TG, FB), BF), V((2, 5, 2, QB, CB), F32), V((2, 2, QB, CB), F32),
            V((2, 4, 6, RW, CB), F32),
            dma((3,)), dma((3, 7)), dma((3,)), dma((3, 7)), dma, dma((3,)), dma, dma((3,)), dma((2,)), dma((2,)), dma((2,)),
            dma((4,)), dma((2,)), dma((2,)), dma((4,)),
            pltpu.SemaphoreType.REGULAR, pltpu.SemaphoreType.REGULAR,
        ],
        compiler_params=pltpu.CompilerParams(collective_id=1, has_side_effects=True, vmem_limit_bytes=58600000),
        name="mlp",
    )(x, dy, wg, wu, wd)
    return o[:3]


def place_kernel(dw, yo, du, y, dx, og, ou, od, bu, bt, sem):
    def put(src, dst, k):
        o = pltpu.make_async_copy(src, dst, sem.at[k])
        o.start()
        return o

    outs = [put(dw.at[1], og, 0)]
    for h in TWO:
        r = pl.ds(QB * h, QB)
        bu[r, :] = dw[2, r, :] + du[h]
        outs.append(put(bu.at[r], ou.at[r], 1 + h))
    outs += [put(yo.at[0], y, 3), put(yo.at[1], dx, 4)]
    for h, q in enumerate((pl.ds(0, CB), pl.ds(CB, FB - CB))):
        bt[q, :] = dw[0, :, q].T
        outs.append(put(bt.at[q], od.at[q], 5 + h))
    for o in outs:
        o.wait()


def place(dw, yo, du):
    sd = jax.ShapeDtypeStruct
    V = pltpu.VMEM
    return pl.pallas_call(
        place_kernel,
        out_shape=(sd((RW, DM), BF), sd((RW, DM), BF), sd((CB, FB), F32), sd((CB, FB), F32), sd((FB, CB), F32)),
        in_specs=[VMEM] * 3,
        out_specs=(HBM,) * 5,
        scratch_shapes=[V((CB, FB), F32), V((FB, CB), F32), pltpu.SemaphoreType.DMA((7,))],
        compiler_params=pltpu.CompilerParams(vmem_limit_bytes=24 * 2**20),
        name="place",
    )(dw.reshape(3, CB, FB), yo, du)


def solution(mesh):
    rows = P(("dp", "tp"), None)
    wsp = P("dp", "tp")
    dsp = P("tp", "dp")

    def local(x, w_gate, w_up, w_down, dy):
        return place(*mlp(x, dy, w_gate, w_up, w_down))

    return jax.shard_map(local, mesh=mesh, in_specs=(rows, wsp, wsp, dsp, rows), out_specs=(rows, rows, wsp, wsp, dsp), check_vma=False)
```

```python
import jax
import jax.numpy as jnp
from jax import lax
from jax.experimental import pallas as pl
from jax.experimental.pallas import tpu as pltpu
from jax.sharding import PartitionSpec as P

MESH = pl.DeviceIdType.MESH
HBM = pl.BlockSpec(memory_space=pltpu.HBM)
VMEM = pl.BlockSpec(memory_space=pltpu.VMEM)
NT = (((1,), (1,)), ((), ()))
TN = (((0,), (0,)), ((), ()))
F32 = jnp.float32
BF = jnp.bfloat16
TWO = range(2)
RING = 4
PAIR = 2
HB = 448
FOUR = 128
DM, TG, FB, CB, QB, RW, RH = 4096, 1024, 896, 512, 256, 64, 32
AX, AD, AE = range(3)
OWN, NEXT, OPP, PREV = range(4)
WG, WU, WL = range(3)
DOWN, GATE, UP = range(3)
Y0, Y1, X0, X1 = range(4)
A0, A1, A2 = range(3)
B0, B1, B2, B3, B4, B5, B6, B7 = range(8)


def mlp_kernel(x_ref, dy_ref, wg_ref, wu_ref, wd_ref, dw, yo, du, xd, wgf, wuf, wdf, U, V, XR, ZR, AP,
               B, A, XB, XS, WD, WX, ZB, ZS, Z2,
               s_g, r_g, s_v, r_v, s_ap, r_ap, s_b, r_b, s_xs, s_zs, s_2, s_c, s_w, s_one, in_x, in_zy):
    i = lax.axis_index("dp")
    j = lax.axis_index("tp")
    x, c, z, y = i // PAIR, i % PAIR, j // 4, j % RING
    xp, xm, xq, c1 = (x + 1) % RING, (x + 3) % RING, (x + 2) % RING, 1 - c
    dev = {
        "xp": {"dp": 2 * xp + c}, "xm": {"dp": 2 * xm + c}, "pc": {"dp": 2 * x + c1},
        "yp": {"tp": 4 * z + (y + 1) % RING}, "ym": {"tp": 4 * z + (y + 3) % RING},
        "zp": {"tp": 4 * ((z + 1) % RING) + y}, "zm": {"tp": 4 * ((z + 3) % RING) + y},
    }
    pos = ((z, y), (y, z))
    link = (("zp", "zm", "yp", "ym"), ("yp", "ym", "zp", "zm"))

    def remote(src, dst, ss, rs, to):
        return pltpu.make_async_remote_copy(src_ref=src, dst_ref=dst, send_sem=ss, recv_sem=rs, device_id=dev[to], device_id_type=MESH)

    def wait(ref, sem):
        pltpu.make_async_copy(ref, ref, sem).wait()

    def r_x(k, t):
        return r_v.at[k, 4 + t // PAIR]

    def r_z(i):
        return r_g.at[i // 7, i % 7]

    def add(dst, src, n):
        def body(r, _):
            s = pl.ds(pl.multiple_of(r * RH, RH), RH)
            dst[s, :] = dst[s, :] + src[s, :]
            return 0
        lax.fori_loop(0, n // RH, body, 0)

    def send(src, dst, to, ss, rs):
        remote(src, dst, ss, rs, to).start()

    def wblk(k, xx, cc, half=None):
        ii = 2 * xx + cc
        if k < 2:
            r = (wgf, wuf)[k]
            if half is None:
                return r.at[pl.ds(pl.multiple_of(ii * CB, CB), CB), :]
            return r.at[pl.ds(pl.multiple_of(ii * CB + half * QB, QB), QB), :]
        if half is None:
            return wdf.at[ii]
        return wdf.at[ii, pl.ds(half * HB, HB), :]

    ahead = xq // PAIR

    def cols(a):
        if a == AX:
            return slice(None)
        h = ahead if a == AD else 1 - ahead
        return pl.ds(pl.multiple_of(h * (DM // PAIR), DM // PAIR), DM // PAIR)

    def rows(a, col, s, p, lo=0, n=RH):
        zz, yy = (p, s) if col == 0 else (s, p)
        return xd.at[min(a, AD), pl.ds(pl.multiple_of((zz * 4 + yy) * RW + col * RH + lo, 16), n), cols(a)]

    def geo(col):
        sec, prim = pos[col]
        sp, sm, pp, pm = link[col]
        return prim, sec, pp, pm, sp, sm

    def some(a, n):
        return xd.at[min(a, AD), pl.ds(0, n), cols(a)]

    FIRST, ON, LAST = range(4, 7)

    def ga(a):
        for col in TWO:
            p, s, pp, pm, sp, sm = geo(col)
            src = yo.at[min(a, AD), pl.ds(col * RH, RH), cols(a)]
            for to in (pp, pm):
                send(src, rows(a, col, p, s), to, s_g.at[a], r_g.at[a, FIRST])

    def gb0(a):
        for col in TWO:
            p, s, pp, pm, sp, sm = geo(col)
            src = yo.at[min(a, AD), pl.ds(col * RH, RH), cols(a)]
            for to in (sp, sm):
                send(src, rows(a, col, p, s), to, s_g.at[a], r_g.at[a, OWN])

    def ga2(a):
        wait(some(a, FOUR), r_g.at[a, FIRST])
        for col in TWO:
            p, s, pp, pm, sp, sm = geo(col)
            for d, lo, to in ((PREV, 0, pp), (NEXT, 16, pm)):
                r = rows(a, col, (p + d) % RING, s, lo, 16)
                send(r, r, to, s_g.at[a], r_g.at[a, ON])

    def gb31(a):
        for col in TWO:
            p, s, pp, pm, sp, sm = geo(col)
            for d in (PREV, NEXT):
                r = rows(a, col, (p + d) % RING, s)
                for to in (sp, sm):
                    send(r, r, to, s_g.at[a], r_g.at[a, d])

    def gb2(a):
        wait(some(a, RW), r_g.at[a, ON])
        for col in TWO:
            p, s, pp, pm, sp, sm = geo(col)
            r = rows(a, col, (p + OPP) % RING, s)
            for to in (sp, sm):
                send(r, r, to, s_g.at[a], r_g.at[a, OPP])

    def gf(a, d):
        wait(some(a, FOUR), r_g.at[a, d])
        for col in TWO:
            p, s, pp, pm, sp, sm = geo(col)
            for e, lo, to in ((PREV, 0, sp), (NEXT, 16, sm)):
                r = rows(a, col, (p + d) % RING, (s + e) % RING, lo, 16)
                send(r, r, to, s_g.at[a], r_g.at[a, LAST])

    def gend(a):
        if a == AX:
            put.wait()
        wait(some(a, QB), r_g.at[a, LAST])
        for arr, idx in (((AX, 0), (AX, 1), (AX, 3), (AX, 2)), ((AD, 0),), ((AD, 1), (AD, 3), (AD, 2)))[a]:
            ap(arr, idx).start()

    w_in = (wg_ref, wu_ref, wd_ref)
    LATE = 6
    seen = set()

    def blocks(k, n):
        return wdf.at[pl.ds(0, n)] if k == WL else (wgf, wuf)[k].at[pl.ds(0, n * CB), :]

    def once(k, g, n):
        if (k, g) not in seen:
            seen.add((k, g))
            wait(blocks(k, n), r_v.at[k, g])

    def wpc(k):
        send(w_in[k], wblk(k, x, c), "pc", s_v.at[k], r_v.at[k, OWN])

    def wown(k):
        for fr, to in enumerate(("xp", "xm")):
            if k < WL:
                send(w_in[k], wblk(k, x, c), to, s_v.at[k], r_v.at[k, FIRST])
            else:
                send(wd_ref.at[pl.ds(fr * HB, HB), :], wblk(k, x, c, fr), to, s_v.at[k], r_v.at[k, FIRST])
        if k == WL:
            for fr, to in enumerate(("xp", "xm")):
                send(wd_ref.at[pl.ds((1 - fr) * HB, HB), :], wblk(k, x, c, 1 - fr), to, s_v.at[k], r_v.at[k, LATE])

    def wf(k):
        once(k, FIRST, 1 if k == WL else 2)
        for xx, d, half, to in ((xm, PREV, 0, "xp"), (xp, NEXT, 1, "xm")):
            r = wblk(k, xx, c, half)
            send(r, r, to, s_v.at[k], r_v.at[k, ON])
            if k < WL:
                r = wblk(k, xx, c)
                send(r, r, "pc", s_v.at[k], r_v.at[k, d])

    def wfp():
        once(WL, LATE, 1)
        for xx, d in ((xm, PREV), (xp, NEXT)):
            r = wblk(WL, xx, c)
            send(r, r, "pc", s_v.at[WL], r_v.at[WL, d])

    def wf2(k):
        once(k, ON, 1)
        for half in TWO:
            r = wblk(k, xq, c, half)
            send(r, r, "pc", s_v.at[k], r_v.at[k, OPP])

    def have(k, d, o):
        if o == 1:
            once(k, d, 1)
        elif d == OPP:
            once(k, ON, 1)
        elif d:
            once(k, FIRST, 1 if k == WL else 2)
            if k == WL:
                once(k, LATE, 1)

    xpos = {0: x, 1: xp, 2: xq, 3: xm}
    order = ((0, 0), (0, 1), (3, 0), (1, 0), (3, 1), (1, 1), (2, 0), (2, 1))

    def blk(t):
        d, o = order[t]
        return 2 * xpos[d] + (c if o == 0 else c1)

    def a_slot(t):
        s = t % RING
        return A.at[s // PAIR, s % PAIR]

    def ld_ab(t):
        d, o = order[t]
        s = t % RING
        ii = blk(t)
        out = [pltpu.make_async_copy(xd.at[0, :, pl.ds(pl.multiple_of(ii * CB, CB), CB)], a_slot(t), s_c.at[s])]
        for k in TWO:
            src = w_in[k] if t == 0 else wblk(k, xpos[d], c if o == 0 else c1)
            out.append(pltpu.make_async_copy(src, WX.at[s % PAIR, k, pl.ds((s // PAIR) * CB, CB), :], s_c.at[s]))
        return out

    def sab(t):
        for k in TWO:
            have(k, *order[t])
        for l in ld_ab(t):
            l.start()

    def ab(t):
        s = t % RING
        wait(xd.at[0, pl.ds(0, 352)], s_c.at[s])

        def body(m, _):
            r = pl.ds(pl.multiple_of(m * QB, QB), QB)
            lhs = A[s // PAIR, s % PAIR, r, :]
            for k in TWO:
                v = jnp.dot(lhs, WX[s % PAIR, k, pl.ds((s // PAIR) * CB, CB), :], preferred_element_type=F32)
                to = XB.at[m // PAIR, m % PAIR] if k == WG else XS.at[m]
                to[...] = v if t == 0 else to[...] + v
            return 0
        lax.fori_loop(0, 4, body, 0)

    def hp():
        def body(q, _):
            m = q // 8
            r = pl.ds(pl.multiple_of((q % 8) * RH, RH), RH)
            a = XB[m // PAIR, m % PAIR, r, :]
            b = XS[m, r, :]
            sig = jax.nn.sigmoid(a)
            sa = a * sig
            XB[m // PAIR, m % PAIR, r, :] = b * sig * (1.0 + a * (1.0 - sig))
            XS[m, r, :] = sa
            B[0, 0, pl.ds(pl.multiple_of(q * RH, RH), RH), :] = (sa * b).astype(BF)
            return 0
        lax.fori_loop(0, RH, body, 0)
        bp[0].start()
        u_put.start()
        v_put.start()

    u_put = pltpu.make_async_copy(XB.at[pl.ds(0, 2)], U, s_one.at[0])
    v_put = pltpu.make_async_copy(XS.at[pl.ds(0, 4)], V, s_one.at[1])

    def ld_g(t):
        d, o = order[t]
        s = t % RING
        ii = blk(t)
        src = wd_ref if t == 0 else wdf.at[ii]
        return [pltpu.make_async_copy(xd.at[1, :, pl.ds(pl.multiple_of(ii * CB, CB), CB)], a_slot(t), s_c.at[s]),
                pltpu.make_async_copy(src, WX.at[s % PAIR, s // PAIR, pl.ds(0, FB), pl.ds(0, CB)], s_c.at[s])]

    def sg(t):
        have(2, *order[t])
        for l in ld_g(t):
            l.start()

    def gg(t):
        if t == 0:
            v_put.wait()
        s = t % RING
        wait(xd.at[1, pl.ds(0, 240)], s_c.at[s])

        def body(m, _):
            r = pl.ds(pl.multiple_of(m * QB, QB), QB)
            v = lax.dot_general(A[s // PAIR, s % PAIR, r, :], WX[s % PAIR, s // PAIR, pl.ds(0, FB), pl.ds(0, CB)], NT, preferred_element_type=F32)
            if t == 0:
                XS[m] = v
            else:
                XS[m] += v
            return 0
        lax.fori_loop(0, 4, body, 0)

    def us_load(q, k):
        m = q // PAIR
        r = pl.ds(pl.multiple_of((q % PAIR) * FOUR, FOUR), FOUR)
        src = U.at[m // PAIR, m % PAIR, r, :] if k == 0 else V.at[m, r, :]
        return pltpu.make_async_copy(src, XS.at[4 + q % PAIR, pl.ds(FOUR * k, FOUR), :], s_c.at[2 + q % PAIR])

    def dadb():
        for k in TWO:
            us_load(0, k).start()

        def body(q, _):
            @pl.when(q < 7)
            def _():
                for k in TWO:
                    us_load(q + 1, k).start()
            wait(XS.at[4 + q % PAIR], s_c.at[2 + q % PAIR])

            def inner(e, _):
                g = XS[q // PAIR, pl.ds(pl.multiple_of((q % PAIR) * FOUR + e * RH, RH), RH), :]
                o = pl.ds(pl.multiple_of(q * FOUR + e * RH, RH), RH)
                for k in TWO:
                    B[1 + k, 0, o, :] = (g * XS[4 + q % PAIR, pl.ds(pl.multiple_of(FOUR * k + e * RH, RH), RH), :]).astype(BF)
                return 0
            lax.fori_loop(0, 4, inner, 0)
            return 0
        lax.fori_loop(0, 8, body, 0)
        bp[1].start()
        bp[2].start()

    def chunk(idx):
        return (x + 6 - idx) % RING

    bp = [remote(B.at[k, 0], B.at[k, 1], s_b, r_b.at[k], "pc") for k in range(3)]

    def ap(arr, idx):
        return remote(xd.at[arr, :, pl.ds(pl.multiple_of(TG * chunk(idx) + CB * c1, CB), CB)], AP.at[arr, idx], s_ap, r_ap.at[arr * min(idx + 1, 2)], "pc")

    seq = (0, 1, 3, 2)

    def load_a(k, n):
        arr = 1 - min(k, 1)
        idx = seq[n]
        return (pltpu.make_async_copy(xd.at[arr, :, pl.ds(pl.multiple_of(TG * chunk(idx) + CB * c, CB), CB)], A.at[n % PAIR, 0], s_c.at[n % PAIR]),
                pltpu.make_async_copy(AP.at[arr, idx], A.at[n % PAIR, 1], s_c.at[n % PAIR]))

    served = set()

    def start_a(k, n):
        if k == DOWN and n == 0:
            wait(AP.at[1, 0], r_ap.at[1])
        elif k == DOWN and 2 not in served:
            served.add(2)
            wait(AP.at[1, pl.ds(0, 3)], r_ap.at[2])
        elif k == GATE and 0 not in served:
            served.add(0)
            wait(AP.at[0], r_ap.at[0])
        for l in load_a(k, n):
            l.start()

    def dot_x(k, n, split=False):
        slot = n % PAIR
        wait(A.at[slot], s_c.at[slot])

        def body(m, _):
            cols = pl.ds(pl.multiple_of(m * QB, QB), QB)
            to = (XB.at[0, m], XB.at[1, m], XB.at[2, m], dw.at[k, m])[n]
            to[...] = (lax.dot_general(A[slot, 0, :, cols], B[k, 0], TN, preferred_element_type=F32)
                             + lax.dot_general(A[slot, 1, :, cols], B[k, 1], TN, preferred_element_type=F32))
            return 0

        if split:
            for m in TWO:
                body(m, 0)
                xmsg(k, m).start()
        else:
            lax.fori_loop(0, 2, body, 0)

    def xmsg(k, t):
        src = (XB.at[0, 0], XB.at[0, 1], XB.at[1, 1], XB.at[2, 0], XB.at[1, 0], XB.at[2, 1])[t]
        dst = du.at[t - 4] if k == UP and t >= 4 else XR.at[k, t]
        return remote(src, dst, s_xs.at[min(t // PAIR, 1)], r_x(k, t), ("xp", "xm")[t % PAIR])

    def xl(k, n):
        start_a(k, n)

    def x1(k):
        bp[k].wait_recv()
        if k == 0:
            u_put.wait()
        else:
            wait(XB.at[0], s_xs.at[0])
        dot_x(k, 0, True)

    def x2(k):
        if k > 0:
            wait(XB.at[pl.ds(0, 2)], s_xs.at[1])
        dot_x(k, 1)
        start_a(k, 3)
        xmsg(k, 2).start()
        dot_x(k, 2)
        if k == 1:
            start_a(2, 0)
        xmsg(k, 3).start()

    def x2o(k):
        dot_x(k, 3)
        if k == 1:
            start_a(2, 1)

    def xstage(k, t, slot):
        return pltpu.make_async_copy(XR.at[k, t], XS.at[4 + slot], s_one.at[3])

    def x3(k):
        wait(XS.at[pl.ds(4, 2)], r_x(k, 0))
        for t in TWO:
            xstage(k, t, t).start()
        wait(XS.at[pl.ds(4, 2)], s_one.at[3])
        for t in TWO:
            add(XB.at[1 + t, t], XS.at[4 + t], QB)
            xmsg(k, 4 + t).start()

    def xadd(k, ts):
        wait(XS.at[pl.ds(4, 2)], r_x(k, ts[0]))
        for h, t in enumerate(ts):
            xstage(k, t, h).start()
        wait(XS.at[pl.ds(4, 2)], s_one.at[3])
        for h, t in enumerate(ts):
            add(dw.at[k, h], XS.at[4 + h], QB)

    def xfa(k):
        xadd(k, (3, 2))

    def xfb(k):
        xadd(k, (4, 5))

    def pair(n, col):
        return ((0, 3), (1, 2))[col][n % PAIR]

    def lw(n):
        if n < 2:
            for col in TWO:
                have(2, pair(n, col), 0)
                have(2, pair(n, col), 1)
        out = []
        for col in TWO:
            d = pair(n, col)
            q = xpos[d]
            if n < 2:
                if d == 0:
                    out.append(pltpu.make_async_copy(wd_ref, WD.at[col, c], s_w.at[n // PAIR]))
                    out.append(pltpu.make_async_copy(wdf.at[2 * x + c1], WD.at[col, c1], s_w.at[n // PAIR]))
                else:
                    out.append(pltpu.make_async_copy(wdf.at[pl.ds(2 * q, 2)], WD.at[col], s_w.at[n // PAIR]))
            else:
                for k in TWO:
                    full = (wgf, wuf)[k]
                    if d == 0:
                        out.append(pltpu.make_async_copy(w_in[k], WX.at[col, k, pl.ds(pl.multiple_of(CB * c, CB), CB), :], s_w.at[n // PAIR]))
                        out.append(pltpu.make_async_copy(full.at[pl.ds(pl.multiple_of(TG * x + CB * c1, CB), CB), :],
                                                         WX.at[col, k, pl.ds(pl.multiple_of(CB * c1, CB), CB), :], s_w.at[n // PAIR]))
                    else:
                        out.append(pltpu.make_async_copy(full.at[pl.ds(pl.multiple_of(TG * q, TG), TG), :], WX.at[col, k], s_w.at[n // PAIR]))
        for o in out:
            o.start()

    def dots_z(n, lo, m):

        def body(q, _):
            col = q // m
            idx = lo + 2 * (q % m)
            p = z + col * (y - z)
            ch = (p + 6 - idx) % RING
            s1 = QB - 192 * col
            s2 = RW + 192 * col
            own = (idx // PAIR) * (1 - idx // 3)
            slot = idx + own * 2 * (n % PAIR)

            def lhs(k):
                return jnp.concatenate([B[k, 0, pl.ds(pl.multiple_of(ch * s1 + g * s2, RW), RW), :] for g in range(4)], axis=0)

            if n < 2:
                l = lhs(0)
                for h in TWO:
                    ZB[col, slot, h] = jnp.dot(l, WD[col, h], preferred_element_type=F32)
            else:
                l = lhs(1)
                u = lhs(2)
                for h in TWO:
                    r = pl.ds(CB * h, CB)
                    ZB[col, slot, h] = (lax.dot_general(l, WX[col, 0, r, :], NT, preferred_element_type=F32)
                                        + lax.dot_general(u, WX[col, 1, r, :], NT, preferred_element_type=F32))
            return 0
        lax.fori_loop(0, 2 * m, body, 0)

    def zmsg(n, col, t):
        src = ((0, 0), (0, 1), (1, 1), (3, 0), (1, 0), (3, 1))[t]
        return remote(ZB.at[col, src[0], src[1]], ZR.at[col, n, t], s_zs.at[min(t // PAIR, 1)], r_z(3 * n + t // PAIR), link[col][t % PAIR])

    def own(n, col, h):
        return ZB.at[col, 2 + 2 * (n % PAIR), h]

    def sub(n, col, h, d):
        s = (pos[col][1] + d) % RING
        return ZB.at[col, 2 + 2 * (n % PAIR), h, pl.ds(pl.multiple_of(s * RW, RW), RW), :]

    def msg2(n, col, t):
        h, d = ((0, 2), (1, 2), (1, 1), (0, 3), (0, 1), (1, 3))[t]
        return remote(sub(n, col, h, d), Z2.at[col, n, t], s_2.at[n % PAIR], r_z(12 + PAIR * n + min(t // PAIR, 1)), link[col][2 + t % PAIR])

    def p1(n):
        wait((WD, WX)[n // PAIR], s_w.at[n // PAIR])
        if n > 0:
            wait(ZB.at[0, pl.ds(0, 2)], s_zs.at[0])
        dots_z(n, 0, 1)
        for t in TWO:
            for col in TWO:
                zmsg(n, col, t).start()

    def p2(n):
        if n > 0:
            wait(ZB.at[0, pl.ds(0, 4)], s_zs.at[1])
        dots_z(n, 1, 2)
        for t in range(2, 4):
            for col in TWO:
                zmsg(n, col, t).start()

    def p2o(n):
        if n > 1:
            wait(Z2.at[0, pl.ds(0, 2)], s_2.at[n % PAIR])
        dots_z(n, 2, 1)

    def zstage(n, col, t, slot):
        return pltpu.make_async_copy(ZR.at[col, n, t], ZS.at[col, slot], s_one.at[2])

    def stage(n, ts):
        wait(ZS, r_z(3 * n + ts[0] // PAIR))
        for h, t in enumerate(ts):
            for col in TWO:
                zstage(n, col, t, h).start()
        wait(ZS, s_one.at[2])

    def p4(n):
        stage(n, (0, 1))
        for t in TWO:
            for col in TWO:
                add(ZB.at[col, (1, 3)[t], t], ZS.at[col, t], QB)
                zmsg(n, col, 4 + t).start()

    def zadd(n, ts):
        stage(n, ts)
        for h in TWO:
            for col in TWO:
                add(own(n, col, h), ZS.at[col, h], QB)

    def fa(n):
        zadd(n, (3, 2))

    def fb(n):
        zadd(n, (4, 5))
        for t in range(4):
            for col in TWO:
                msg2(n, col, t).start()

    def hh(n):
        wait(Z2.at[0, 0, pl.ds(0, 4)], r_z(12 + PAIR * n))
        for t in TWO:
            for col in TWO:
                add(sub(n, col, t, (1, 3)[t]), Z2.at[col, n, t], RW)
                msg2(n, col, 4 + t).start()

    done = []

    def zf(n):
        a = n // PAIR
        if not done:
            for g in (AX, AD, AE):
                wait(some(g, 960), s_g.at[g])
        done.append(n)
        wait(Z2.at[:, 0, pl.ds(0, 4)], r_z(13 + PAIR * n))
        for col in TWO:
            q = xpos[pair(n, col)]
            for h, ts in ((0, (3, 4)), (1, (2, 5))):
                cs = pl.ds(pl.multiple_of(TG * q + CB * h, CB), CB)
                v = sub(n, col, h, 0)[...] + Z2[col, n, ts[0]] + Z2[col, n, ts[1]]
                yo[a, :, cs] = (yo[a, :, cs].astype(F32) + v).astype(BF)

    odd = (x + c + y + z) % PAIR
    along = ("xp", "xm", "pc")
    across = ("yp", "ym", "zp", "zm")

    def tell(sem, names):
        for d in names:
            pl.semaphore_signal(sem, inc=1, device_id=dev[d], device_id_type=MESH)

    def enter():
        @pl.when(odd == 0)
        def _():
            tell(barrier, across)
            pl.semaphore_wait(barrier, len(along))
            tell(in_x, along)

        @pl.when(odd == 1)
        def _():
            tell(barrier, along)
            pl.semaphore_wait(in_x, len(along))

    def enter_zy():
        @pl.when(odd == 0)
        def _():
            pl.semaphore_wait(in_zy, len(across))

        @pl.when(odd == 1)
        def _():
            pl.semaphore_wait(barrier, len(across))
            tell(in_zy, across)

    own_ld = [pltpu.make_async_copy(r, yo.at[k], s_one.at[2]) for k, r in enumerate((x_ref, dy_ref))]
    for l in own_ld:
        l.start()
    barrier = pltpu.get_barrier_semaphore()
    enter()
    put = pltpu.make_async_copy(yo, xd.at[:, pl.ds(pl.multiple_of(j * RW, RW), RW), :], s_one.at[3])
    wown(WG)
    wown(WU)
    wpc(WG)
    wpc(WU)
    wpc(WL)
    wait(yo, s_one.at[2])
    put.start()
    enter_zy()
    ga(AX)
    gb0(AX)
    ga(AD)
    ga2(AX)
    gf(AX, OWN)
    gb31(AX)
    ga2(AD)
    gb2(AX)
    wf(WG)
    gf(AX, PREV)
    gf(AX, NEXT)
    gf(AX, OPP)
    ga(AE)
    gb31(AD)
    wf(WU)
    wown(WL)
    gb0(AD)
    gend(AX)
    sab(B2)
    sab(B1)
    sab(B0)
    ab(B0)
    ab(B1)
    gb2(AD)
    sab(B3)
    gf(AD, PREV)
    sab(B4)
    ga2(AE)
    wf2(WG)
    ab(B2)
    gb0(AE)
    wf2(WU)
    gf(AD, OWN)
    ab(B3)
    sab(B6)
    gf(AD, NEXT)
    gf(AD, OPP)
    sab(B5)
    ab(B4)
    sab(B7)
    gb2(AE)
    ab(B5)
    gb31(AE)
    gf(AE, OWN)
    ab(B6)
    wf(WL)
    ab(B7)
    gend(AD)
    hp()
    xl(DOWN, A0)
    gf(AE, PREV)
    wfp()
    gf(AE, NEXT)
    gf(AE, OPP)
    x1(DOWN)
    lw(Y0)
    gend(AE)
    p1(Y0)
    xl(DOWN, A2)
    xl(DOWN, A1)
    wf2(WL)
    p2(Y0)
    x2(DOWN)
    x2o(DOWN)
    sg(B1)
    sg(B0)
    p2o(Y0)
    lw(Y1)
    gg(B0)
    sg(B4)
    sg(B3)
    gg(B1)
    sg(B2)
    p4(Y0)
    gg(B2)
    gg(B3)
    gg(B4)
    sg(B5)
    p1(Y1)
    x3(DOWN)
    sg(B6)
    gg(B5)
    gg(B6)
    sg(B7)
    p2(Y1)
    gg(B7)
    xl(GATE, A0)
    lw(X0)
    dadb()
    xfa(DOWN)
    p2o(Y1)
    xl(GATE, A1)
    x1(GATE)
    p4(Y1)
    fa(Y0)
    p1(X0)
    xl(GATE, A2)
    x2(GATE)
    fb(Y0)
    xfb(DOWN)
    x3(GATE)
    fa(Y1)
    x1(UP)
    fb(Y1)
    hh(Y0)
    x2o(GATE)
    p2(X0)
    zf(Y0)
    xl(UP, A2)
    p4(X0)
    p2o(X0)
    lw(X1)
    hh(Y1)
    p1(X1)
    xfa(GATE)
    x2(UP)
    fa(X0)
    p2(X1)
    p4(X1)
    xfb(GATE)
    x3(UP)
    zf(Y1)
    fb(X0)
    p2o(X1)
    x2o(UP)
    fa(X1)
    fb(X1)
    hh(X0)
    xfa(UP)
    hh(X1)
    zf(X0)
    zf(X1)
    def end():
        for k in (WG, WU, WL):
            wait(blocks(k, 7), s_v.at[k])
        wait(AP, s_ap)
        wait(B.at[:, 0], s_b)
        for q in TWO:
            wait(Z2.at[0, pl.ds(0, 2)], s_2.at[q])
            wait(ZB.at[0, pl.ds(0, 2 + 2 * q)], s_zs.at[q])
        wait(XB.at[0], s_xs.at[0])
        wait(XB.at[pl.ds(0, 2)], s_xs.at[1])
        wait(du, r_x(UP, 4))

    end()


def mlp(x, dy, wg, wu, wd):
    sd = jax.ShapeDtypeStruct
    dma = pltpu.SemaphoreType.DMA
    V = pltpu.VMEM
    o = pl.pallas_call(
        mlp_kernel,
        out_shape=(V((3, 2, QB, FB), F32), V((2, RW, DM), BF), V((2, QB, FB), F32),
                   sd((2, TG, DM), BF), sd((DM, FB), BF), sd((DM, FB), BF), sd((8, FB, CB), BF), sd((2, 2, QB, FB), F32), sd((4, QB, FB), F32),
                   sd((3, 6, QB, FB), F32), sd((2, 4, 6, QB, CB), F32), sd((2, 4, TG, CB), BF)),
        in_specs=[HBM] * 5,
        out_specs=(VMEM,) * 3 + (HBM,) * 9,
        scratch_shapes=[
            V((3, 2, TG, FB), BF), V((2, 2, TG, CB), BF), V((3, 2, QB, FB), F32), V((6, QB, FB), F32),
            V((2, 2, FB, CB), BF), V((2, 2, TG, FB), BF), V((2, 5, 2, QB, CB), F32), V((2, 2, QB, CB), F32),
            V((2, 4, 6, RW, CB), F32),
            dma((3,)), dma((3, 7)), dma((3,)), dma((3, 7)), dma, dma((3,)), dma, dma((3,)), dma((2,)), dma((2,)), dma((2,)),
            dma((4,)), dma((2,)), dma((4,)),
            pltpu.SemaphoreType.REGULAR, pltpu.SemaphoreType.REGULAR,
        ],
        compiler_params=pltpu.CompilerParams(collective_id=1, has_side_effects=True, vmem_limit_bytes=58600000),
        name="mlp",
    )(x, dy, wg, wu, wd)
    return o[:3]


def place_kernel(dw, yo, du, y, dx, og, ou, od, bu, bt, sem):
    def put(src, dst, k):
        o = pltpu.make_async_copy(src, dst, sem.at[k])
        o.start()
        return o

    outs = [put(dw.at[1], og, 0)]
    for h in TWO:
        r = pl.ds(QB * h, QB)
        bu[r, :] = dw[2, r, :] + du[h]
        outs.append(put(bu.at[r], ou.at[r], 1 + h))
    outs += [put(yo.at[0], y, 3), put(yo.at[1], dx, 4)]
    for h, q in enumerate((pl.ds(0, CB), pl.ds(CB, FB - CB))):
        bt[q, :] = dw[0, :, q].T
        outs.append(put(bt.at[q], od.at[q], 5 + h))
    for o in outs:
        o.wait()


def place(dw, yo, du):
    sd = jax.ShapeDtypeStruct
    V = pltpu.VMEM
    return pl.pallas_call(
        place_kernel,
        out_shape=(sd((RW, DM), BF), sd((RW, DM), BF), sd((CB, FB), F32), sd((CB, FB), F32), sd((FB, CB), F32)),
        in_specs=[VMEM] * 3,
        out_specs=(HBM,) * 5,
        scratch_shapes=[V((CB, FB), F32), V((FB, CB), F32), pltpu.SemaphoreType.DMA((7,))],
        compiler_params=pltpu.CompilerParams(vmem_limit_bytes=24 * 2**20),
        name="place",
    )(dw.reshape(3, CB, FB), yo, du)


def solution(mesh):
    rows = P(("dp", "tp"), None)
    wsp = P("dp", "tp")
    dsp = P("tp", "dp")

    def local(x, w_gate, w_up, w_down, dy):
        return place(*mlp(x, dy, w_gate, w_up, w_down))

    return jax.shard_map(local, mesh=mesh, in_specs=(rows, wsp, wsp, dsp, rows), out_specs=(rows, rows, wsp, wsp, dsp), check_vma=False)
```
